32 devices in a mesh: dp: 4 (over y, z), seq: 8 (over x, core).
Axes of the slice: x: 4, y: 2, z: 2, core: 2. Of those that a mesh axis runs over, the one named last changes fastest.
The devices are a block of a 4x4x8 slice.
Arguments:
- enc_out: bfloat16 [256, 16, 512], P('dp', 'seq'), parts along dimension 0
- pred_out: bfloat16 [256, 64, 512], P('dp'), parts along dimension 0
- w_enc: bfloat16 [512, 512], replicated
- w_pred: bfloat16 [512, 512], replicated
- w_out: bfloat16 [512, 500], replicated
- labels: int32 [256, 63], P('dp'), parts along dimension 0
- frame_len: int32 [256], P('dp'), parts along dimension 0
- label_len: int32 [256], P('dp'), parts along dimension 0
Outputs:
- output 1: float32 [256], P('dp'), parts along dimension 0
- output 2: bfloat16 [256, 16, 512], P('dp', 'seq'), parts along dimension 0
- output 3: float32 [2048, 512], P('dp'), parts along dimension 0
- output 4: float32 [2048, 512], P('dp'), parts along dimension 0
- output 5: float32 [2048, 500], P('dp'), parts along dimension 0
There are 4 independent parts. The reference program is written for one: setup_inputs(seed, part) draws one part's arguments, and reference() takes and returns one part's arrays. A program takes and returns all parts, laid end to end along the dimension named above; an argument that names none is the same for every part.
All inputs are finite; a program needn't handle non-finite values.
Results may differ from the reference program's by a relative error of at most 0.0142388.
Values are sent between devices in bfloat16 or wider.
A program may use at most 768 MiB of HBM per device.

```python
import jax
import jax.numpy as jnp
from jax import lax

NUM_UTT = 64
NUM_FRAMES = 16
LABEL_POS = 64
ENC_DIM = 512
PRED_DIM = 512
JOINT_DIM = 512
VOCAB_SIZE = 500
FRAME_BLOCK = 2
NUM_LABELS = LABEL_POS - 1
NUM_BLOCKS = NUM_FRAMES // FRAME_BLOCK
NEG_FILL = -1.0e30


def setup_inputs(seed: int = 0, part: int = 0) -> dict:
    shared_key, part_base = jax.random.split(jax.random.key(seed))
    part_key = jax.random.fold_in(part_base, part)
    k_enc, k_pred, k_lab, k_frames, k_lens = jax.random.split(part_key, 5)
    k_wenc, k_wpred, k_wout = jax.random.split(shared_key, 3)
    enc_out = jax.random.normal(k_enc, (NUM_UTT, NUM_FRAMES, ENC_DIM), jnp.float32).astype(jnp.bfloat16)
    pred_out = jax.random.normal(k_pred, (NUM_UTT, LABEL_POS, PRED_DIM), jnp.float32).astype(jnp.bfloat16)
    w_enc = (jax.random.normal(k_wenc, (ENC_DIM, JOINT_DIM), jnp.float32) * ENC_DIM ** -0.5).astype(jnp.bfloat16)
    w_pred = (jax.random.normal(k_wpred, (PRED_DIM, JOINT_DIM), jnp.float32) * PRED_DIM ** -0.5).astype(jnp.bfloat16)
    w_out = (jax.random.normal(k_wout, (JOINT_DIM, VOCAB_SIZE), jnp.float32) * (1.5 * JOINT_DIM ** -0.5)).astype(jnp.bfloat16)
    labels = jax.random.randint(k_lab, (NUM_UTT, NUM_LABELS), 1, VOCAB_SIZE, jnp.int32)
    frame_len = jax.random.randint(k_frames, (NUM_UTT,), NUM_FRAMES // 4 + 1, NUM_FRAMES + 1, jnp.int32).at[0].set(NUM_FRAMES)
    label_len = jax.random.randint(k_lens, (NUM_UTT,), 1, NUM_LABELS + 1, jnp.int32).at[NUM_UTT - 1].set(NUM_LABELS)
    return {'enc_out': enc_out, 'pred_out': pred_out, 'w_enc': w_enc, 'w_pred': w_pred, 'w_out': w_out, 'labels': labels, 'frame_len': frame_len, 'label_len': label_len}


def joint_block(enc_blk, act_g, w_enc, w_out):
    n_utt, n_blk, _ = enc_blk.shape
    act_f = jnp.dot(enc_blk.reshape(n_utt * n_blk, ENC_DIM), w_enc, preferred_element_type=jnp.float32).astype(jnp.bfloat16).reshape(n_utt, n_blk, JOINT_DIM)
    hidden = jnp.tanh(act_f[:, :, None, :].astype(jnp.float32) + act_g[:, None, :, :].astype(jnp.float32)).astype(jnp.bfloat16)
    logits = jnp.dot(hidden.reshape(n_utt * n_blk * LABEL_POS, JOINT_DIM), w_out, preferred_element_type=jnp.float32).reshape(n_utt, n_blk, LABEL_POS, VOCAB_SIZE)
    return hidden, jax.nn.log_softmax(logits, axis=-1)


def label_prefix(frame_lab):
    zero_col = jnp.zeros_like(frame_lab[:, :1])
    return jnp.concatenate([zero_col, jnp.cumsum(frame_lab, axis=1)], axis=1)


def reference(enc_out, pred_out, w_enc, w_pred, w_out, labels, frame_len, label_len):
    act_g = jnp.dot(pred_out.reshape(NUM_UTT * LABEL_POS, PRED_DIM), w_pred, preferred_element_type=jnp.float32).astype(jnp.bfloat16).reshape(NUM_UTT, LABEL_POS, JOINT_DIM)
    lab_ids = jnp.concatenate([labels, jnp.full((NUM_UTT, 1), -1, jnp.int32)], axis=1)
    lab_index = jnp.broadcast_to(labels[:, None, :, None], (NUM_UTT, FRAME_BLOCK, NUM_LABELS, 1))
    enc_blocks = enc_out.reshape(NUM_UTT, NUM_BLOCKS, FRAME_BLOCK, ENC_DIM).transpose(1, 0, 2, 3)

    def lattice_scores(enc_blk):
        _, log_probs = joint_block(enc_blk, act_g, w_enc, w_out)
        lab_lp = jnp.take_along_axis(log_probs[:, :, :NUM_LABELS, :], lab_index, axis=3)[..., 0]
        return log_probs[..., 0], lab_lp

    blank_blocks, lab_blocks = lax.map(lattice_scores, enc_blocks)
    blank_lp = blank_blocks.transpose(1, 0, 2, 3).reshape(NUM_UTT, NUM_FRAMES, LABEL_POS)
    lab_lp = lab_blocks.transpose(1, 0, 2, 3).reshape(NUM_UTT, NUM_FRAMES, NUM_LABELS)

    pos_ids = jnp.arange(LABEL_POS)[None, :]
    neg_rows = jnp.full((NUM_UTT, LABEL_POS), NEG_FILL, jnp.float32)
    init_x = jnp.where(pos_ids == 0, 0.0, neg_rows)
    boundary = jnp.where(pos_ids == label_len[:, None], 0.0, neg_rows)

    def alpha_step(x_prev, frame_in):
        frame_blank, frame_lab = frame_in
        lab_sum = label_prefix(frame_lab)
        alpha_t = lab_sum + lax.cumlogsumexp(x_prev - lab_sum, axis=1)
        return alpha_t + frame_blank, alpha_t

    _, alphas = lax.scan(alpha_step, init_x, (blank_lp.transpose(1, 0, 2), lab_lp.transpose(1, 0, 2)))
    alphas = alphas.transpose(1, 0, 2)

    def beta_step(next_row, frame_in):
        frame_blank, frame_lab, frame_id = frame_in
        lab_sum = label_prefix(frame_lab)
        beta_row = lax.cumlogsumexp(next_row + frame_blank + lab_sum, axis=1, reverse=True) - lab_sum
        beta_row = jnp.where((frame_id >= frame_len)[:, None], boundary, beta_row)
        return beta_row, (beta_row, next_row)

    first_row, (betas, beta_next) = lax.scan(beta_step, boundary, (blank_lp.transpose(1, 0, 2), lab_lp.transpose(1, 0, 2), jnp.arange(NUM_FRAMES)), reverse=True)
    betas = betas.transpose(1, 0, 2)
    beta_next = beta_next.transpose(1, 0, 2)
    log_prob = first_row[:, 0]

    beta_up = jnp.concatenate([betas[:, :, 1:], jnp.full((NUM_UTT, NUM_FRAMES, 1), NEG_FILL, jnp.float32)], axis=2)
    lab_full = jnp.concatenate([lab_lp, jnp.zeros((NUM_UTT, NUM_FRAMES, 1), jnp.float32)], axis=2)
    frame_ok = (jnp.arange(NUM_FRAMES)[None, :] < frame_len[:, None])[:, :, None]
    norm_shift = log_prob[:, None, None]
    occ_blank = jnp.where(frame_ok, jnp.exp(jnp.minimum(alphas + blank_lp + beta_next - norm_shift, 0.0)), 0.0)
    occ_lab = jnp.where(frame_ok, jnp.exp(jnp.minimum(alphas + lab_full + beta_up - norm_shift, 0.0)), 0.0)

    def to_blocks(arr):
        return arr.reshape(NUM_UTT, NUM_BLOCKS, FRAME_BLOCK, LABEL_POS).transpose(1, 0, 2, 3)

    vocab_ids = jnp.arange(VOCAB_SIZE)

    def grad_step(acc_carry, blk_in):
        gw_enc, gw_out, d_act_g = acc_carry
        enc_blk, occ_b, occ_l = blk_in
        hidden, log_probs = joint_block(enc_blk, act_g, w_enc, w_out)
        d_logits = (jnp.exp(log_probs) * (occ_b + occ_l)[..., None] - jnp.where(vocab_ids == 0, occ_b[..., None], 0.0) - jnp.where(vocab_ids == lab_ids[:, None, :, None], occ_l[..., None], 0.0)).astype(jnp.bfloat16)
        flat_dz = d_logits.reshape(NUM_UTT * FRAME_BLOCK * LABEL_POS, VOCAB_SIZE)
        flat_h = hidden.reshape(NUM_UTT * FRAME_BLOCK * LABEL_POS, JOINT_DIM)
        d_hidden = jnp.dot(flat_dz, w_out.T, preferred_element_type=jnp.float32)
        d_pre = (d_hidden * (1.0 - jnp.square(flat_h.astype(jnp.float32)))).astype(jnp.bfloat16).reshape(NUM_UTT, FRAME_BLOCK, LABEL_POS, JOINT_DIM)
        d_act_f = jnp.sum(d_pre.astype(jnp.float32), axis=2).astype(jnp.bfloat16).reshape(NUM_UTT * FRAME_BLOCK, JOINT_DIM)
        grad_blk = jnp.dot(d_act_f, w_enc.T, preferred_element_type=jnp.float32).astype(jnp.bfloat16).reshape(NUM_UTT, FRAME_BLOCK, ENC_DIM)
        gw_enc = gw_enc + jnp.dot(enc_blk.reshape(NUM_UTT * FRAME_BLOCK, ENC_DIM).T, d_act_f, preferred_element_type=jnp.float32)
        gw_out = gw_out + jnp.dot(flat_h.T, flat_dz, preferred_element_type=jnp.float32)
        d_act_g = d_act_g + jnp.sum(d_pre.astype(jnp.float32), axis=1)
        return (gw_enc, gw_out, d_act_g), grad_blk

    acc_init = (jnp.zeros((ENC_DIM, JOINT_DIM), jnp.float32), jnp.zeros((JOINT_DIM, VOCAB_SIZE), jnp.float32), jnp.zeros((NUM_UTT, LABEL_POS, JOINT_DIM), jnp.float32))
    (gw_enc, gw_out, d_act_g), grad_blocks = lax.scan(grad_step, acc_init, (enc_blocks, to_blocks(occ_blank), to_blocks(occ_lab)))
    grad_enc = grad_blocks.transpose(1, 0, 2, 3).reshape(NUM_UTT, NUM_FRAMES, ENC_DIM)
    gw_pred = jnp.einsum('buh,buj->hj', pred_out.astype(jnp.float32), d_act_g.astype(jnp.float32))
    return -log_prob, grad_enc, gw_enc, gw_pred, gw_out
```

```python
import functools

import jax
import jax.numpy as jnp
from jax import lax
from jax.experimental import pallas as pl
from jax.experimental.pallas import tpu as pltpu
from jax.sharding import PartitionSpec as P

NEG_FILL = -1.0e30
CHUNK = 16
LANES = 128
TILE_CHUNKS = 16
TILE = CHUNK * TILE_CHUNKS
F32 = jnp.float32
BF16 = jnp.bfloat16


def logadd(x, y):
    return jnp.maximum(x, y) + jnp.log(1.0 + jnp.exp(-jnp.abs(x - y)))


def dot_nn(x, y):
    return jnp.dot(x, y, preferred_element_type=F32)


def dot_tn(x, y):
    return lax.dot_general(x, y, (((0,), (0,)), ((), ())), preferred_element_type=F32)


def dot_nt(x, y):
    return lax.dot_general(x, y, (((1,), (1,)), ((), ())), preferred_element_type=F32)


def local_kernel(n_utt, n_frames, n_pos, vocab,
                 seq_ref, tlen_ref, ulen_ref,
                 enc_hbm, pred_hbm, wenc_hbm, wpred_hbm, wout_hbm, labels_ref,
                 loss_ref, genc_ref, gwe_ref, gwp_ref, gwo_ref,
                 f_v, g_v, we_v, wp_v, wo_v, wt_v, act_f, act_g, lab_v, lab_scr,
                 hid, ex, sums, sk_b, sk_l, al, xb_s, xl_s, occ_b, occ_l, dz_v, dh_v,
                 dc, da8, lrow, arow, sbase, gbase, utt_of, sems):
    me = seq_ref[0]
    n_diag = n_frames + n_pos - 1
    skew_rows = (n_frames + n_pos) * n_frames
    n_rows = n_utt * n_pos
    vocab_pad = wo_v.shape[1]
    n_grp = vocab_pad // LANES

    copies = [
        pltpu.make_async_copy(enc_hbm, f_v, sems.at[0]),
        pltpu.make_async_copy(pred_hbm.at[pl.ds(pl.multiple_of(me * n_rows, n_rows), n_rows), :], g_v, sems.at[1]),
        pltpu.make_async_copy(wenc_hbm, we_v, sems.at[2]),
        pltpu.make_async_copy(wpred_hbm, wp_v, sems.at[3]),
        pltpu.make_async_copy(wout_hbm, wo_v, sems.at[4]),
    ]
    for cp in copies:
        cp.start()

    def add_utt(b, pos):
        t_len = tlen_ref[me * n_utt + b]
        n_chunk = (ulen_ref[me * n_utt + b] + CHUNK) // CHUNK

        def add_frame(t, pos):
            def add_chunk(q, pos):
                lrow[pos] = b * n_pos + q * CHUNK
                arow[pos] = b * n_frames + t
                skew = (n_frames + 1) * t + n_frames * CHUNK * q
                sbase[pos] = b * skew_rows + skew
                gbase[pos] = skew
                utt_of[pos] = b
                return pos + 1
            return lax.fori_loop(0, n_chunk, add_chunk, pos)
        return lax.fori_loop(0, t_len, add_frame, pos)

    n_chunks = lax.fori_loop(0, n_utt, add_utt, 0)
    n_tiles = (n_chunks + TILE_CHUNKS - 1) // TILE_CHUNKS

    def add_dummy(pos, carry):
        lrow[pos] = n_rows
        arow[pos] = n_utt * n_frames
        sbase[pos] = n_utt * skew_rows
        gbase[pos] = skew_rows
        utt_of[pos] = 0
        return carry
    lax.fori_loop(n_chunks, n_tiles * TILE_CHUNKS, add_dummy, 0)

    dc[...] = jnp.zeros_like(dc)
    da8[...] = jnp.zeros_like(da8)
    gwo_ref[...] = jnp.zeros_like(gwo_ref)
    occ_b[pl.ds(skew_rows, 256), :] = jnp.zeros((256, LANES), F32)
    occ_l[pl.ds(skew_rows, 256), :] = jnp.zeros((256, LANES), F32)
    act_f[pl.ds(n_utt * n_frames, 8), :] = jnp.zeros((8, act_f.shape[1]), F32)
    act_g[pl.ds(n_rows, CHUNK), :] = jnp.zeros((CHUNK, act_g.shape[1]), BF16)
    lab_v[pl.ds(n_rows, CHUNK), :] = jnp.full((CHUNK, LANES), -1, jnp.int32)

    lab_scr[...] = jnp.full_like(lab_scr, -1.0)
    lab_scr[:, :n_pos - 1] = labels_ref[pl.ds(pl.multiple_of(me * n_utt, n_utt), n_utt), :].astype(F32)
    lab_t = jnp.transpose(lab_scr[...])
    for b in range(n_utt):
        lab_v[pl.ds(b * n_pos, n_pos), :] = jnp.broadcast_to(lab_t[:n_pos, b:b + 1], (n_pos, LANES)).astype(jnp.int32)

    for cp in copies:
        cp.wait()
    act_f[pl.ds(0, n_utt * n_frames), :] = dot_nn(f_v[...], we_v[...]).astype(BF16).astype(F32)
    act_g[pl.ds(0, n_rows), :] = dot_nn(g_v[...], wp_v[...]).astype(BF16)
    wt_v[...] = jnp.transpose(wo_v[...])

    lane = lax.broadcasted_iota(jnp.int32, (CHUNK, LANES), 1)
    last_ok = lane < vocab - (n_grp - 1) * LANES

    def fwd_tile(i, carry):
        r0 = pl.multiple_of(i * TILE, TILE)
        for k in range(TILE_CHUNKS):
            lr = pl.multiple_of(lrow[i * TILE_CHUNKS + k], CHUNK)
            ar = arow[i * TILE_CHUNKS + k]
            pre = act_g[pl.ds(lr, CHUNK), :].astype(F32) + act_f[pl.ds(ar, 1), :]
            hid[pl.ds(r0 + k * CHUNK, CHUNK), :] = jnp.tanh(pre).astype(BF16)
        ex[pl.ds(r0, TILE), :] = dot_nn(hid[pl.ds(r0, TILE), :], wo_v[...])
        for k in range(TILE_CHUNKS):
            rows = pl.ds(r0 + k * CHUNK, CHUNK)
            lr = pl.multiple_of(lrow[i * TILE_CHUNKS + k], CHUNK)
            sb = sbase[i * TILE_CHUNKS + k]
            ids = lab_v[pl.ds(lr, CHUNK), :]
            zs = [ex[rows, j * LANES:(j + 1) * LANES] for j in range(n_grp)]
            zs[-1] = jnp.where(last_ok, zs[-1], NEG_FILL)
            top = functools.reduce(jnp.maximum, zs)
            top = jnp.max(top, axis=1, keepdims=True)
            picked = functools.reduce(jnp.add, [jnp.where(lane + j * LANES == ids, zs[j], 0.0) for j in range(n_grp)])
            picked = jnp.sum(picked, axis=1, keepdims=True)
            es = [jnp.exp(z - top) for z in zs]
            for j in range(n_grp):
                ex[rows, j * LANES:(j + 1) * LANES] = es[j]
            tot = jnp.sum(functools.reduce(jnp.add, es), axis=1, keepdims=True)
            tot_b = jnp.broadcast_to(tot, (CHUNK, LANES))
            sums[rows, :] = tot_b
            log_norm = top + jnp.log(tot_b)
            sk_b[pl.ds(sb, CHUNK, stride=n_frames), :] = zs[0][:, 0:1] - log_norm
            sk_l[pl.ds(sb, CHUNK, stride=n_frames), :] = picked - log_norm
        return carry
    lax.fori_loop(0, n_tiles, fwd_tile, 0)

    lane_s = lax.broadcasted_iota(jnp.int32, (n_frames, LANES), 1)
    sub_s = lax.broadcasted_iota(jnp.int32, (n_frames, LANES), 0)
    t_lens = jnp.zeros((n_frames, LANES), jnp.int32)
    u_lens = jnp.zeros((n_frames, LANES), jnp.int32)
    for b in range(n_utt):
        t_lens = jnp.where(lane_s == b, tlen_ref[me * n_utt + b], t_lens)
        u_lens = jnp.where(lane_s == b, ulen_ref[me * n_utt + b], u_lens)
    live_t = sub_s < t_lens
    last_t = sub_s == t_lens - 1

    def diag(d):
        base = pl.multiple_of(d * n_frames, n_frames)
        bl = sk_b[pl.ds(base, n_frames), :]
        lb = sk_l[pl.ds(base, n_frames), :]
        for b in range(1, n_utt):
            off = pl.multiple_of(base + b * skew_rows, n_frames)
            bl = jnp.where(lane_s == b, sk_b[pl.ds(off, n_frames), :], bl)
            lb = jnp.where(lane_s == b, sk_l[pl.ds(off, n_frames), :], lb)
        u = d - sub_s
        live = live_t & (u >= 0)
        bl = jnp.where(live & (u <= u_lens), bl, NEG_FILL)
        lb = jnp.where(live & (u < u_lens), lb, NEG_FILL)
        return base, bl, lb, last_t & (u == u_lens)

    def lattice_step(i, carry):
        a, be = carry
        base, bl, lb, _ = diag(i)
        al[pl.ds(base, n_frames), :] = a
        moved = jnp.where(sub_s == 0, NEG_FILL, pltpu.roll(a + bl, 1, 0))
        a = logadd(moved, a + lb)
        base, bl, lb, end = diag(n_diag - 1 - i)
        up = jnp.where(sub_s == n_frames - 1, NEG_FILL, pltpu.roll(be, n_frames - 1, 0))
        x_b = jnp.where(end, bl, up + bl)
        x_l = be + lb
        xb_s[pl.ds(base, n_frames), :] = x_b
        xl_s[pl.ds(base, n_frames), :] = x_l
        return a, logadd(x_b, x_l)

    neg = jnp.full((n_frames, LANES), NEG_FILL, F32)
    _, be0 = lax.fori_loop(0, n_diag, lattice_step, (jnp.where(sub_s == 0, 0.0, neg), neg))
    log_prob = be0[0:1, :]
    loss_ref[...] = jnp.broadcast_to(-log_prob, loss_ref.shape)

    n_live = n_diag * n_frames
    for r in range(0, n_live, 64):
        rows = pl.ds(r, min(64, n_live - r))
        a = al[rows, :] - log_prob
        occ_b[rows, :] = jnp.exp(jnp.minimum(a + xb_s[rows, :], 0.0))
        occ_l[rows, :] = jnp.exp(jnp.minimum(a + xl_s[rows, :], 0.0))

    def bwd_tile(i, carry):
        r0 = pl.multiple_of(i * TILE, TILE)
        for k in range(TILE_CHUNKS):
            rows = pl.ds(r0 + k * CHUNK, CHUNK)
            lr = pl.multiple_of(lrow[i * TILE_CHUNKS + k], CHUNK)
            gb0 = gbase[i * TILE_CHUNKS + k]
            mine = lane == utt_of[i * TILE_CHUNKS + k]
            ids = lab_v[pl.ds(lr, CHUNK), :]
            ob = jnp.sum(jnp.where(mine, occ_b[pl.ds(gb0, CHUNK, stride=n_frames), :], 0.0), axis=1, keepdims=True)
            ol = jnp.sum(jnp.where(mine, occ_l[pl.ds(gb0, CHUNK, stride=n_frames), :], 0.0), axis=1, keepdims=True)
            scale = (ob + ol) / sums[rows, :]
            for j in range(n_grp):
                dz = ex[rows, j * LANES:(j + 1) * LANES] * scale
                if j == 0:
                    dz = dz - jnp.where(lane == 0, ob, 0.0)
                dz = dz - jnp.where(lane + j * LANES == ids, ol, 0.0)
                dz_v[k * CHUNK:(k + 1) * CHUNK, j * LANES:(j + 1) * LANES] = dz.astype(BF16)
        dh_v[...] = dot_nn(dz_v[...], wt_v[...])
        gwo_ref[...] += dot_tn(hid[pl.ds(r0, TILE), :], dz_v[...])
        for k in range(TILE_CHUNKS):
            rows = pl.ds(r0 + k * CHUNK, CHUNK)
            lr = pl.multiple_of(lrow[i * TILE_CHUNKS + k], CHUNK)
            ar = pl.multiple_of(arow[i * TILE_CHUNKS + k] * 8, 8)
            h = hid[rows, :].astype(F32)
            dp = (dh_v[k * CHUNK:(k + 1) * CHUNK, :] * (1.0 - h * h)).astype(BF16).astype(F32)
            dc[pl.ds(lr, CHUNK), :] += dp
            da8[pl.ds(ar, 8), :] += dp[:8, :] + dp[8:, :]
        return carry
    lax.fori_loop(0, n_tiles, bwd_tile, 0)

    n_af = n_utt * n_frames
    d_act_f = jnp.sum(da8[pl.ds(0, n_af * 8), :].reshape(n_af, 8, da8.shape[1]), axis=1).astype(BF16)
    genc_ref[...] = dot_nt(d_act_f, we_v[...]).astype(BF16)
    gwe_ref[...] = dot_tn(f_v[...], d_act_f)
    gwp_ref[...] = dot_tn(g_v[...], dc[pl.ds(0, n_rows), :].astype(BF16))


def local_grads(seq_idx, enc_rows, pred_out, w_enc, w_pred, w_out, labels, frame_len, label_len, n_utt, n_frames, vocab):
    n_pos = labels.shape[1] + 1
    enc_dim, joint = w_enc.shape
    vocab_pad = w_out.shape[1]
    n_rows = n_utt * n_pos
    n_af = n_utt * n_frames
    max_rows = n_utt * n_frames * n_pos
    skew_rows = (n_frames + n_pos) * n_frames
    n_chunks = max_rows // CHUNK + TILE_CHUNKS
    any_spec = pl.BlockSpec(memory_space=pl.ANY)
    vmem = pl.BlockSpec(memory_space=pltpu.VMEM)
    grid_spec = pltpu.PrefetchScalarGridSpec(
        num_scalar_prefetch=3, grid=(),
        in_specs=[any_spec] * 5 + [vmem],
        out_specs=[vmem] * 5,
        scratch_shapes=[
            pltpu.VMEM((n_af, enc_dim), BF16),
            pltpu.VMEM((n_rows, w_pred.shape[0]), BF16),
            pltpu.VMEM(w_enc.shape, BF16),
            pltpu.VMEM(w_pred.shape, BF16),
            pltpu.VMEM(w_out.shape, BF16),
            pltpu.VMEM((vocab_pad, joint), BF16),
            pltpu.VMEM((n_af + 8, joint), F32),
            pltpu.VMEM((n_rows + CHUNK, joint), BF16),
            pltpu.VMEM((n_rows + CHUNK, LANES), jnp.int32),
            pltpu.VMEM((n_utt, LANES), F32),
            pltpu.VMEM((max_rows, joint), BF16),
            pltpu.VMEM((max_rows, vocab_pad), F32),
            pltpu.VMEM((max_rows, LANES), F32),
            pltpu.VMEM((n_utt * skew_rows + 256, LANES), F32),
            pltpu.VMEM((n_utt * skew_rows + 256, LANES), F32),
            pltpu.VMEM((skew_rows, LANES), F32),
            pltpu.VMEM((skew_rows, LANES), F32),
            pltpu.VMEM((skew_rows, LANES), F32),
            pltpu.VMEM((skew_rows + 256, LANES), F32),
            pltpu.VMEM((skew_rows + 256, LANES), F32),
            pltpu.VMEM((TILE, vocab_pad), BF16),
            pltpu.VMEM((TILE, joint), F32),
            pltpu.VMEM((n_rows + CHUNK, joint), F32),
            pltpu.VMEM((n_af * 8 + 8, joint), F32),
            pltpu.SMEM((n_chunks,), jnp.int32),
            pltpu.SMEM((n_chunks,), jnp.int32),
            pltpu.SMEM((n_chunks,), jnp.int32),
            pltpu.SMEM((n_chunks,), jnp.int32),
            pltpu.SMEM((n_chunks,), jnp.int32),
            pltpu.SemaphoreType.DMA((5,)),
        ])
    return pl.pallas_call(
        functools.partial(local_kernel, n_utt, n_frames, n_pos, vocab),
        grid_spec=grid_spec,
        out_shape=[
            jax.ShapeDtypeStruct((8, LANES), F32),
            jax.ShapeDtypeStruct((n_af, enc_dim), BF16),
            jax.ShapeDtypeStruct((enc_dim, joint), F32),
            jax.ShapeDtypeStruct((w_pred.shape[0], joint), F32),
            jax.ShapeDtypeStruct((joint, vocab_pad), F32),
        ],
        compiler_params=pltpu.CompilerParams(vmem_limit_bytes=62 << 20),
        name="rnnt_local",
    )(seq_idx, frame_len, label_len, enc_rows, pred_out, w_enc, w_pred, w_out, labels)


def solution(mesh):
    seq_size = mesh.shape['seq']

    def local_fn(enc_out, pred_out, w_enc, w_pred, w_out, labels, frame_len, label_len):
        seq_idx = lax.axis_index('seq')
        n_all, n_loc, enc_dim = enc_out.shape
        n_utt = n_all // seq_size
        n_frames = n_loc * seq_size
        vocab = w_out.shape[1]
        vocab_pad = pl.cdiv(vocab, LANES) * LANES
        w_out_p = jnp.pad(w_out, ((0, 0), (0, vocab_pad - vocab)))
        enc_mine = lax.all_to_all(enc_out.reshape(seq_size, n_utt, n_loc, enc_dim), 'seq', 0, 0)
        enc_rows = jnp.swapaxes(enc_mine, 0, 1).reshape(n_utt * n_frames, enc_dim)
        loss, genc, gwe, gwp, gwo = local_grads(
            jnp.reshape(seq_idx, (1,)).astype(jnp.int32), enc_rows, pred_out.reshape(-1, pred_out.shape[2]), w_enc, w_pred, w_out_p,
            labels, frame_len, label_len, n_utt, n_frames, vocab)
        genc = jnp.swapaxes(genc.reshape(n_utt, seq_size, n_loc, enc_dim), 0, 1)
        grad_enc = lax.all_to_all(genc, 'seq', 0, 0).reshape(n_all, n_loc, enc_dim)
        gwe, gwp, gwo = lax.psum((gwe, gwp, gwo), 'seq')
        loss = lax.all_gather(loss[0, :n_utt], 'seq').reshape(n_all)
        return loss, grad_enc, gwe, gwp, gwo[:, :vocab]

    in_specs = (P('dp', 'seq', None), P('dp', None, None), P(None, None), P(None, None), P(None, None), P('dp', None), P('dp'), P('dp'))
    out_specs = (P('dp'), P('dp', 'seq', None), P('dp', None), P('dp', None), P('dp', None))
    return jax.shard_map(local_fn, mesh=mesh, in_specs=in_specs, out_specs=out_specs, check_vma=False)
```

```python
import functools

import jax
import jax.numpy as jnp
from jax import lax
from jax.experimental import pallas as pl
from jax.experimental.pallas import tpu as pltpu
from jax.sharding import PartitionSpec as P

NEG_FILL = -1.0e30
CHUNK = 16
LANES = 128
TILE_CHUNKS = 16
TILE = CHUNK * TILE_CHUNKS
F32 = jnp.float32
BF16 = jnp.bfloat16


def logadd(x, y):
    return jnp.maximum(x, y) + jnp.log(1.0 + jnp.exp(-jnp.abs(x - y)))


def dot_nn(x, y):
    return jnp.dot(x, y, preferred_element_type=F32)


def dot_tn(x, y):
    return lax.dot_general(x, y, (((0,), (0,)), ((), ())), preferred_element_type=F32)


def dot_nt(x, y):
    return lax.dot_general(x, y, (((1,), (1,)), ((), ())), preferred_element_type=F32)


def local_kernel(n_utt, n_frames, n_loc, n_pos, vocab,
                 seq_ref, tlen_ref, ulen_ref,
                 enc_hbm, pred_hbm, wenc_hbm, wpred_hbm, wout_t_hbm, labels_ref,
                 loss_ref, genc_ref, gwe_ref, gwp_ref, gwo_ref,
                 f_v, g_v, we_v, wp_v, wraw_v, wo_v, wt_v, act_f, act_g, lab_v, lab_scr,
                 hid, ex, sums, sk_b, sk_l, al, xb_s, xl_s, occ_b, occ_l, dz_v, dh_v,
                 acc_o, dc, da8, lrow, arow, sbase, gbase, utt_of, sems):
    me = seq_ref[0]
    n_diag = n_frames + n_pos - 1
    skew_rows = (n_frames + n_pos) * n_frames
    n_rows = n_utt * n_pos
    vocab_pad = wt_v.shape[0]
    n_grp = vocab_pad // LANES

    copies = [
        pltpu.make_async_copy(enc_hbm, f_v, sems.at[0]),
        pltpu.make_async_copy(pred_hbm.at[pl.ds(pl.multiple_of(me * n_rows, n_rows), n_rows), :], g_v, sems.at[1]),
        pltpu.make_async_copy(wenc_hbm, we_v, sems.at[2]),
        pltpu.make_async_copy(wpred_hbm, wp_v, sems.at[3]),
        pltpu.make_async_copy(wout_t_hbm, wraw_v, sems.at[4]),
    ]
    for cp in copies:
        cp.start()

    def add_utt(b, pos):
        t_len = tlen_ref[me * n_utt + b]
        n_chunk = (ulen_ref[me * n_utt + b] + CHUNK) // CHUNK

        def add_frame(t, pos):
            def add_chunk(q, pos):
                lrow[pos] = b * n_pos + q * CHUNK
                arow[pos] = t // n_loc * (n_utt * n_loc) + b * n_loc + t % n_loc
                skew = (n_frames + 1) * t + n_frames * CHUNK * q
                sbase[pos] = b * skew_rows + skew
                gbase[pos] = skew
                utt_of[pos] = b
                return pos + 1
            return lax.fori_loop(0, n_chunk, add_chunk, pos)
        return lax.fori_loop(0, t_len, add_frame, pos)

    n_chunks = lax.fori_loop(0, n_utt, add_utt, 0)
    n_tiles = (n_chunks + TILE_CHUNKS - 1) // TILE_CHUNKS

    def add_dummy(pos, carry):
        lrow[pos] = n_rows
        arow[pos] = n_utt * n_frames
        sbase[pos] = n_utt * skew_rows
        gbase[pos] = skew_rows
        utt_of[pos] = 0
        return carry
    lax.fori_loop(n_chunks, n_tiles * TILE_CHUNKS, add_dummy, 0)

    dc[...] = jnp.zeros_like(dc)
    da8[...] = jnp.zeros_like(da8)
    acc_o[...] = jnp.zeros_like(acc_o)
    occ_b[pl.ds(skew_rows, 256), :] = jnp.zeros((256, LANES), F32)
    occ_l[pl.ds(skew_rows, 256), :] = jnp.zeros((256, LANES), F32)
    act_f[pl.ds(n_utt * n_frames, 8), :] = jnp.zeros((8, act_f.shape[1]), F32)
    act_g[pl.ds(n_rows, CHUNK), :] = jnp.zeros((CHUNK, act_g.shape[1]), BF16)
    lab_v[pl.ds(n_rows, CHUNK), :] = jnp.full((CHUNK, LANES), -1, jnp.int32)

    lab_scr[...] = jnp.full_like(lab_scr, -1.0)
    lab_scr[:, :n_pos - 1] = labels_ref[pl.ds(pl.multiple_of(me * n_utt, n_utt), n_utt), :].astype(F32)
    lab_t = jnp.transpose(lab_scr[...])
    for b in range(n_utt):
        lab_v[pl.ds(b * n_pos, n_pos), :] = jnp.broadcast_to(lab_t[:n_pos, b:b + 1], (n_pos, LANES)).astype(jnp.int32)

    for cp in copies:
        cp.wait()
    act_f[pl.ds(0, n_utt * n_frames), :] = dot_nn(f_v[...], we_v[...]).astype(BF16).astype(F32)
    act_g[pl.ds(0, n_rows), :] = dot_nn(g_v[...], wp_v[...]).astype(BF16)
    wt_v[vocab:, :] = jnp.zeros((vocab_pad - vocab, wt_v.shape[1]), BF16)
    wt_v[:vocab, :] = wraw_v[...]
    wo_v[...] = jnp.transpose(wt_v[...])

    lane = lax.broadcasted_iota(jnp.int32, (CHUNK, LANES), 1)
    last_ok = lane < vocab - (n_grp - 1) * LANES

    def fwd_tile(i, carry):
        r0 = pl.multiple_of(i * TILE, TILE)
        for k in range(TILE_CHUNKS):
            lr = pl.multiple_of(lrow[i * TILE_CHUNKS + k], CHUNK)
            ar = arow[i * TILE_CHUNKS + k]
            pre = act_g[pl.ds(lr, CHUNK), :].astype(F32) + act_f[pl.ds(ar, 1), :]
            hid[pl.ds(r0 + k * CHUNK, CHUNK), :] = jnp.tanh(pre).astype(BF16)
        ex[pl.ds(r0, TILE), :] = dot_nn(hid[pl.ds(r0, TILE), :], wo_v[...])
        for k in range(TILE_CHUNKS):
            rows = pl.ds(r0 + k * CHUNK, CHUNK)
            lr = pl.multiple_of(lrow[i * TILE_CHUNKS + k], CHUNK)
            sb = sbase[i * TILE_CHUNKS + k]
            ids = lab_v[pl.ds(lr, CHUNK), :]
            zs = [ex[rows, j * LANES:(j + 1) * LANES] for j in range(n_grp)]
            zs[-1] = jnp.where(last_ok, zs[-1], NEG_FILL)
            top = functools.reduce(jnp.maximum, zs)
            top = jnp.max(top, axis=1, keepdims=True)
            picked = functools.reduce(jnp.add, [jnp.where(lane + j * LANES == ids, zs[j], 0.0) for j in range(n_grp)])
            picked = jnp.sum(picked, axis=1, keepdims=True)
            es = [jnp.exp(z - top) for z in zs]
            for j in range(n_grp):
                ex[rows, j * LANES:(j + 1) * LANES] = es[j]
            tot = jnp.sum(functools.reduce(jnp.add, es), axis=1, keepdims=True)
            tot_b = jnp.broadcast_to(tot, (CHUNK, LANES))
            sums[rows, :] = tot_b
            log_norm = top + jnp.log(tot_b)
            sk_b[pl.ds(sb, CHUNK, stride=n_frames), :] = zs[0][:, 0:1] - log_norm
            sk_l[pl.ds(sb, CHUNK, stride=n_frames), :] = picked - log_norm
        return carry
    lax.fori_loop(0, n_tiles, fwd_tile, 0)

    lane_s = lax.broadcasted_iota(jnp.int32, (n_frames, LANES), 1)
    sub_s = lax.broadcasted_iota(jnp.int32, (n_frames, LANES), 0)
    t_lens = jnp.zeros((n_frames, LANES), jnp.int32)
    u_lens = jnp.zeros((n_frames, LANES), jnp.int32)
    for b in range(n_utt):
        t_lens = jnp.where(lane_s == b, tlen_ref[me * n_utt + b], t_lens)
        u_lens = jnp.where(lane_s == b, ulen_ref[me * n_utt + b], u_lens)
    live_t = sub_s < t_lens
    last_t = sub_s == t_lens - 1

    def diag(d):
        base = pl.multiple_of(d * n_frames, n_frames)
        bl = sk_b[pl.ds(base, n_frames), :]
        lb = sk_l[pl.ds(base, n_frames), :]
        for b in range(1, n_utt):
            off = pl.multiple_of(base + b * skew_rows, n_frames)
            bl = jnp.where(lane_s == b, sk_b[pl.ds(off, n_frames), :], bl)
            lb = jnp.where(lane_s == b, sk_l[pl.ds(off, n_frames), :], lb)
        u = d - sub_s
        live = live_t & (u >= 0)
        bl = jnp.where(live & (u <= u_lens), bl, NEG_FILL)
        lb = jnp.where(live & (u < u_lens), lb, NEG_FILL)
        return base, bl, lb, last_t & (u == u_lens)

    def lattice_step(i, carry):
        a, be = carry
        base, bl, lb, _ = diag(i)
        al[pl.ds(base, n_frames), :] = a
        moved = jnp.where(sub_s == 0, NEG_FILL, pltpu.roll(a + bl, 1, 0))
        a = logadd(moved, a + lb)
        base, bl, lb, end = diag(n_diag - 1 - i)
        up = jnp.where(sub_s == n_frames - 1, NEG_FILL, pltpu.roll(be, n_frames - 1, 0))
        x_b = jnp.where(end, bl, up + bl)
        x_l = be + lb
        xb_s[pl.ds(base, n_frames), :] = x_b
        xl_s[pl.ds(base, n_frames), :] = x_l
        return a, logadd(x_b, x_l)

    neg = jnp.full((n_frames, LANES), NEG_FILL, F32)
    _, be0 = lax.fori_loop(0, n_diag, lattice_step, (jnp.where(sub_s == 0, 0.0, neg), neg))
    log_prob = be0[0:1, :]
    loss_ref[...] = jnp.broadcast_to(-log_prob, loss_ref.shape)

    n_live = n_diag * n_frames
    for r in range(0, n_live, 64):
        rows = pl.ds(r, min(64, n_live - r))
        a = al[rows, :] - log_prob
        occ_b[rows, :] = jnp.exp(jnp.minimum(a + xb_s[rows, :], 0.0))
        occ_l[rows, :] = jnp.exp(jnp.minimum(a + xl_s[rows, :], 0.0))

    def bwd_tile(i, carry):
        r0 = pl.multiple_of(i * TILE, TILE)
        for k in range(TILE_CHUNKS):
            rows = pl.ds(r0 + k * CHUNK, CHUNK)
            lr = pl.multiple_of(lrow[i * TILE_CHUNKS + k], CHUNK)
            gb0 = gbase[i * TILE_CHUNKS + k]
            mine = lane == utt_of[i * TILE_CHUNKS + k]
            ids = lab_v[pl.ds(lr, CHUNK), :]
            ob = jnp.sum(jnp.where(mine, occ_b[pl.ds(gb0, CHUNK, stride=n_frames), :], 0.0), axis=1, keepdims=True)
            ol = jnp.sum(jnp.where(mine, occ_l[pl.ds(gb0, CHUNK, stride=n_frames), :], 0.0), axis=1, keepdims=True)
            scale = (ob + ol) / sums[rows, :]
            for j in range(n_grp):
                dz = ex[rows, j * LANES:(j + 1) * LANES] * scale
                if j == 0:
                    dz = dz - jnp.where(lane == 0, ob, 0.0)
                dz = dz - jnp.where(lane + j * LANES == ids, ol, 0.0)
                dz_v[k * CHUNK:(k + 1) * CHUNK, j * LANES:(j + 1) * LANES] = dz.astype(BF16)
        dh_v[...] = dot_nn(dz_v[...], wt_v[...])
        acc_o[...] += dot_tn(dz_v[...], hid[pl.ds(r0, TILE), :])
        for k in range(TILE_CHUNKS):
            rows = pl.ds(r0 + k * CHUNK, CHUNK)
            lr = pl.multiple_of(lrow[i * TILE_CHUNKS + k], CHUNK)
            ar = pl.multiple_of(arow[i * TILE_CHUNKS + k] * 8, 8)
            h = hid[rows, :].astype(F32)
            dp = (dh_v[k * CHUNK:(k + 1) * CHUNK, :] * (1.0 - h * h)).astype(BF16).astype(F32)
            dc[pl.ds(lr, CHUNK), :] += dp
            da8[pl.ds(ar, 8), :] += dp[:8, :] + dp[8:, :]
        return carry
    lax.fori_loop(0, n_tiles, bwd_tile, 0)

    n_af = n_utt * n_frames
    d_act_f = jnp.sum(da8[pl.ds(0, n_af * 8), :].reshape(n_af, 8, da8.shape[1]), axis=1).astype(BF16)
    genc_ref[...] = dot_nt(d_act_f, we_v[...]).astype(BF16)
    gwe_ref[...] = dot_tn(f_v[...], d_act_f)
    gwo_ref[...] = acc_o[...]
    gwp_ref[...] = dot_tn(g_v[...], dc[pl.ds(0, n_rows), :].astype(BF16))


def local_grads(seq_idx, enc_rows, pred_out, w_enc, w_pred, w_out_t, labels, frame_len, label_len, n_utt, n_frames, n_loc, vocab):
    n_pos = labels.shape[1] + 1
    enc_dim, joint = w_enc.shape
    vocab_pad = pl.cdiv(vocab, LANES) * LANES
    n_rows = n_utt * n_pos
    n_af = n_utt * n_frames
    max_rows = n_utt * n_frames * n_pos
    skew_rows = (n_frames + n_pos) * n_frames
    n_chunks = max_rows // CHUNK + TILE_CHUNKS
    any_spec = pl.BlockSpec(memory_space=pl.ANY)
    vmem = pl.BlockSpec(memory_space=pltpu.VMEM)
    grid_spec = pltpu.PrefetchScalarGridSpec(
        num_scalar_prefetch=3, grid=(),
        in_specs=[any_spec] * 5 + [vmem],
        out_specs=[vmem] * 5,
        scratch_shapes=[
            pltpu.VMEM((n_af, enc_dim), BF16),
            pltpu.VMEM((n_rows, w_pred.shape[0]), BF16),
            pltpu.VMEM(w_enc.shape, BF16),
            pltpu.VMEM(w_pred.shape, BF16),
            pltpu.VMEM(w_out_t.shape, BF16),
            pltpu.VMEM((joint, vocab_pad), BF16),
            pltpu.VMEM((vocab_pad, joint), BF16),
            pltpu.VMEM((n_af + 8, joint), F32),
            pltpu.VMEM((n_rows + CHUNK, joint), BF16),
            pltpu.VMEM((n_rows + CHUNK, LANES), jnp.int32),
            pltpu.VMEM((n_utt, LANES), F32),
            pltpu.VMEM((max_rows, joint), BF16),
            pltpu.VMEM((max_rows, vocab_pad), F32),
            pltpu.VMEM((max_rows, LANES), F32),
            pltpu.VMEM((n_utt * skew_rows + 256, LANES), F32),
            pltpu.VMEM((n_utt * skew_rows + 256, LANES), F32),
            pltpu.VMEM((skew_rows, LANES), F32),
            pltpu.VMEM((skew_rows, LANES), F32),
            pltpu.VMEM((skew_rows, LANES), F32),
            pltpu.VMEM((skew_rows + 256, LANES), F32),
            pltpu.VMEM((skew_rows + 256, LANES), F32),
            pltpu.VMEM((TILE, vocab_pad), BF16),
            pltpu.VMEM((TILE, joint), F32),
            pltpu.VMEM((vocab_pad, joint), F32),
            pltpu.VMEM((n_rows + CHUNK, joint), F32),
            pltpu.VMEM((n_af * 8 + 8, joint), F32),
            pltpu.SMEM((n_chunks,), jnp.int32),
            pltpu.SMEM((n_chunks,), jnp.int32),
            pltpu.SMEM((n_chunks,), jnp.int32),
            pltpu.SMEM((n_chunks,), jnp.int32),
            pltpu.SMEM((n_chunks,), jnp.int32),
            pltpu.SemaphoreType.DMA((5,)),
        ])
    return pl.pallas_call(
        functools.partial(local_kernel, n_utt, n_frames, n_loc, n_pos, vocab),
        grid_spec=grid_spec,
        out_shape=[
            jax.ShapeDtypeStruct((8, LANES), F32),
            jax.ShapeDtypeStruct((n_af, enc_dim), BF16),
            jax.ShapeDtypeStruct((enc_dim, joint), F32),
            jax.ShapeDtypeStruct((w_pred.shape[0], joint), F32),
            jax.ShapeDtypeStruct((vocab_pad, joint), F32),
        ],
        compiler_params=pltpu.CompilerParams(vmem_limit_bytes=62 << 20),
        name="rnnt_local",
    )(seq_idx, frame_len, label_len, enc_rows, pred_out, w_enc, w_pred, w_out_t, labels)


def greet(seq_size, me):
    barrier = pltpu.get_barrier_semaphore()
    for j in range(1, seq_size):
        pl.semaphore_signal(barrier, inc=1, device_id={'seq': lax.rem(me + j, seq_size)}, device_id_type=pl.DeviceIdType.MESH)
    pl.semaphore_wait(barrier, seq_size - 1)


def spread_kernel(seq_size, rows, enc_ref, out_ref, send, recv):
    me = lax.axis_index('seq')
    greet(seq_size, me)
    mine = pl.ds(pl.multiple_of(me * rows, rows), rows)
    copies = []
    for j in range(1, seq_size):
        peer = lax.rem(me + j, seq_size)
        copies.append(pltpu.make_async_remote_copy(
            src_ref=enc_ref.at[pl.ds(pl.multiple_of(peer * rows, rows), rows), :], dst_ref=out_ref.at[mine, :],
            send_sem=send.at[j - 1], recv_sem=recv.at[j - 1], device_id={'seq': peer}, device_id_type=pl.DeviceIdType.MESH))
        copies[-1].start()
    out_ref[mine, :] = enc_ref[mine, :]
    for copy in copies:
        copy.wait()


def spread_frames(enc_rows, seq_size):
    rows = enc_rows.shape[0] // seq_size
    vmem = pl.BlockSpec(memory_space=pltpu.VMEM)
    return pl.pallas_call(
        functools.partial(spread_kernel, seq_size, rows),
        out_shape=jax.ShapeDtypeStruct(enc_rows.shape, enc_rows.dtype),
        in_specs=[vmem], out_specs=vmem,
        scratch_shapes=[pltpu.SemaphoreType.DMA((seq_size - 1,)), pltpu.SemaphoreType.DMA((seq_size - 1,))],
        compiler_params=pltpu.CompilerParams(collective_id=0, has_side_effects=True),
        name="spread_frames",
    )(enc_rows)


def reduce_kernel(seq_size, n_mat, genc_ref, loss_ref, *refs):
    gw = refs[:n_mat]
    genc_out, loss_out = refs[n_mat:n_mat + 2]
    out = refs[n_mat + 2:2 * n_mat + 2]
    rest = refs[2 * n_mat + 2:]
    sib_buf, own, ring_buf = rest[:n_mat], rest[n_mat:2 * n_mat], rest[2 * n_mat:3 * n_mat]
    (sib_send, sib_recv, rs_send, rs_recv, ag_send, ag_recv, dd_send, dd_recv,
     ge_send, ge_recv, lo_send, lo_recv) = rest[3 * n_mat:]
    me = lax.axis_index('seq')
    n_chip = seq_size // 2
    chip, core = lax.div(me, 2), lax.rem(me, 2)
    sibling = chip * 2 + 1 - core
    nexts = (lax.rem(chip + 1, n_chip) * 2 + core, lax.rem(chip + n_chip - 1, n_chip) * 2 + core)
    half = gw[0].shape[0] // 2
    piece = half // (2 * n_chip)

    def remote(src, dst, send, recv, peer):
        copy = pltpu.make_async_remote_copy(src_ref=src, dst_ref=dst, send_sem=send, recv_sem=recv,
                                            device_id={'seq': peer}, device_id_type=pl.DeviceIdType.MESH)
        copy.start()
        return copy

    def at(way, hops):
        c = lax.rem(chip + n_chip - hops, n_chip) if way == 0 else lax.rem(chip + hops, n_chip)
        return pl.multiple_of((c * 2 + way) * piece, piece)

    greet(seq_size, me)
    pending = []
    sib = []
    for m in range(n_mat):
        sib.append(remote(gw[m].at[pl.ds(pl.multiple_of((1 - core) * half, half), half), :], sib_buf[m], sib_send.at[m], sib_recv.at[m], sibling))
    rows = genc_ref.shape[0] // seq_size
    mine = pl.ds(pl.multiple_of(me * rows, rows), rows)
    small = []
    for j in range(1, seq_size):
        peer = lax.rem(me + j, seq_size)
        small.append(remote(genc_ref.at[pl.ds(pl.multiple_of(peer * rows, rows), rows), :], genc_out.at[mine, :], ge_send.at[j - 1], ge_recv.at[j - 1], peer))
        small.append(remote(loss_ref, loss_out.at[me], lo_send.at[j - 1], lo_recv.at[j - 1], peer))
    genc_out[mine, :] = genc_ref[mine, :]
    loss_out[pl.ds(me, 1)] = loss_ref[...][None]

    ring = {}
    for m in range(n_mat):
        sib[m].wait_recv()
        own[m][...] = gw[m][pl.ds(pl.multiple_of(core * half, half), half), :] + sib_buf[m][...]
        for way in range(2):
            ring[m, way, 0] = remote(own[m].at[pl.ds(at(way, 1), piece), :], ring_buf[m].at[way, 0], rs_send.at[m, way, 0], rs_recv.at[m, way, 0], nexts[way])
    for s in range(1, n_chip - 1):
        for m in range(n_mat):
            for way in range(2):
                ring[m, way, s - 1].wait_recv()
                ring_buf[m][way, s - 1] = ring_buf[m][way, s - 1] + own[m][pl.ds(at(way, s + 1), piece), :]
                ring[m, way, s] = remote(ring_buf[m].at[way, s - 1], ring_buf[m].at[way, s], rs_send.at[m, way, s], rs_recv.at[m, way, s], nexts[way])

    def place(way, hops):
        return pl.ds(pl.multiple_of(core * half + at(way, hops), piece), piece)

    last = n_chip - 2
    gather = {}
    for m in range(n_mat):
        for way in range(2):
            ring[m, way, last].wait_recv()
            here = place(way, 0)
            out[m][here, :] = ring_buf[m][way, last] + own[m][pl.ds(at(way, 0), piece), :]
            gather[m, way, 0] = remote(out[m].at[here, :], out[m].at[here, :], ag_send.at[m, way, 0], ag_recv.at[m, way, 0], nexts[way])
            pending.append(remote(out[m].at[here, :], out[m].at[here, :], dd_send.at[m, way, 0], dd_recv.at[m, way, 0], sibling))
    for s in range(1, n_chip):
        for m in range(n_mat):
            for way in range(2):
                gather[m, way, s - 1].wait_recv()
                here = place(way, s)
                if s < n_chip - 1:
                    gather[m, way, s] = remote(out[m].at[here, :], out[m].at[here, :], ag_send.at[m, way, s], ag_recv.at[m, way, s], nexts[way])
                pending.append(remote(out[m].at[here, :], out[m].at[here, :], dd_send.at[m, way, s], dd_recv.at[m, way, s], sibling))
    for copy in pending + small:
        copy.wait()
    for copy in list(ring.values()) + list(gather.values()) + sib:
        copy.wait_send()


def reduce_all(genc, loss, grads, seq_size):
    n_mat = len(grads)
    n_chip = seq_size // 2
    half = grads[0].shape[0] // 2
    piece = half // (2 * n_chip)
    vmem = pl.BlockSpec(memory_space=pltpu.VMEM)
    dma = pltpu.SemaphoreType.DMA
    steps = n_chip - 1
    return pl.pallas_call(
        functools.partial(reduce_kernel, seq_size, n_mat),
        out_shape=[jax.ShapeDtypeStruct(genc.shape, genc.dtype), jax.ShapeDtypeStruct((seq_size,) + loss.shape, F32)]
        + [jax.ShapeDtypeStruct(g.shape, F32) for g in grads],
        in_specs=[vmem] * (2 + n_mat), out_specs=[vmem] * (2 + n_mat),
        scratch_shapes=[pltpu.VMEM((half, g.shape[1]), F32) for g in grads] * 2
        + [pltpu.VMEM((2, steps, piece, g.shape[1]), F32) for g in grads]
        + [dma((n_mat,))] * 2 + [dma((n_mat, 2, steps))] * 4 + [dma((n_mat, 2, n_chip))] * 2 + [dma((seq_size - 1,))] * 4,
        compiler_params=pltpu.CompilerParams(collective_id=1, has_side_effects=True),
        name="reduce_all",
    )(genc, loss, *grads)


def solution(mesh):
    seq_size = mesh.shape['seq']

    def local_fn(enc_out, pred_out, w_enc, w_pred, w_out, labels, frame_len, label_len):
        seq_idx = lax.axis_index('seq')
        n_all, n_loc, enc_dim = enc_out.shape
        n_utt = n_all // seq_size
        n_frames = n_loc * seq_size
        vocab = w_out.shape[1]
        enc_rows = spread_frames(enc_out.reshape(n_all * n_loc, enc_dim), seq_size)
        loss, genc, *grads = local_grads(
            jnp.reshape(seq_idx, (1,)).astype(jnp.int32), enc_rows, pred_out.reshape(-1, pred_out.shape[2]), w_enc, w_pred, w_out.T,
            labels, frame_len, label_len, n_utt, n_frames, n_loc, vocab)
        genc, loss, gwe, gwp, gwo_t = reduce_all(genc, loss, grads, seq_size)
        return loss[:, 0, :n_utt].reshape(n_all), genc.reshape(n_all, n_loc, enc_dim), gwe, gwp, gwo_t[:vocab].T

    in_specs = (P('dp', 'seq', None), P('dp', None, None), P(None, None), P(None, None), P(None, None), P('dp', None), P('dp'), P('dp'))
    out_specs = (P('dp'), P('dp', 'seq', None), P('dp', None), P('dp', None), P('dp', None))
    return jax.shard_map(local_fn, mesh=mesh, in_specs=in_specs, out_specs=out_specs, check_vma=False)
```

```python
import functools

import jax
import jax.numpy as jnp
from jax import lax
from jax.experimental import pallas as pl
from jax.experimental.pallas import tpu as pltpu
from jax.sharding import PartitionSpec as P

NEG_FILL = -1.0e30
CHUNK = 16
LANES = 128
TILE_CHUNKS = 16
TILE = CHUNK * TILE_CHUNKS
SUBS = 2
BODY_CHUNKS = SUBS * TILE_CHUNKS
SAFE_LOGIT = 60.0
F32 = jnp.float32
BF16 = jnp.bfloat16


def logadd(x, y):
    return jnp.maximum(x, y) + jnp.log(1.0 + jnp.exp(-jnp.abs(x - y)))


def dot_nn(x, y):
    return jnp.dot(x, y, preferred_element_type=F32)


def dot_tn(x, y):
    return lax.dot_general(x, y, (((0,), (0,)), ((), ())), preferred_element_type=F32)


def dot_nt(x, y):
    return lax.dot_general(x, y, (((1,), (1,)), ((), ())), preferred_element_type=F32)


def local_kernel(n_utt, n_frames, n_loc, n_pos, vocab,
                 seq_ref, tlen_ref, ulen_ref,
                 enc_hbm, pred_hbm, wenc_hbm, wpred_hbm, wout_t_hbm, labels_ref,
                 loss_ref, da_ref, gwp_ref, gwo_ref,
                 f_v, g_v, we_v, wp_v, wraw_v, wo_v, wt_v, act_f, act_g, lab_v, lab_scr,
                 hid, ex, sums, sk_b, sk_l, cb_s, cl_s, ce_s, al, xb_s, xl_s, occ_b, occ_l, dz_0, dz_1, z_0, z_1,
                 acc_o, dc, da8, lrow, arow, sbase, gbase, utt_of, sems):
    me = seq_ref[0]
    dz_v, z_v = (dz_0, dz_1), (z_0, z_1)
    n_diag = n_frames + n_pos - 1
    pitch = n_frames + 1
    skew_rows = (n_frames + n_pos) * pitch
    n_rows = n_utt * n_pos
    vocab_pad = wt_v.shape[0]
    n_grp = vocab_pad // LANES
    pad_rows = occ_b.shape[0] - skew_rows

    copies = [
        pltpu.make_async_copy(enc_hbm, f_v, sems.at[0]),
        pltpu.make_async_copy(pred_hbm.at[pl.ds(pl.multiple_of(me * n_rows, n_rows), n_rows), :], g_v, sems.at[1]),
        pltpu.make_async_copy(wenc_hbm, we_v, sems.at[2]),
        pltpu.make_async_copy(wpred_hbm, wp_v, sems.at[3]),
        pltpu.make_async_copy(wout_t_hbm, wraw_v, sems.at[4]),
    ]
    for cp in copies:
        cp.start()

    def add_utt(b, pos):
        t_len = tlen_ref[me * n_utt + b]
        n_chunk = (ulen_ref[me * n_utt + b] + CHUNK) // CHUNK

        def add_frame(t, pos):
            def add_chunk(q, pos):
                lrow[pos] = b * n_pos + q * CHUNK
                arow[pos] = t // n_loc * (n_utt * n_loc) + b * n_loc + t % n_loc
                skew = (pitch + 1) * t + pitch * CHUNK * q
                sbase[pos] = b * skew_rows + skew
                gbase[pos] = skew
                utt_of[pos] = b
                return pos + 1
            return lax.fori_loop(0, n_chunk, add_chunk, pos)
        return lax.fori_loop(0, t_len, add_frame, pos)

    n_chunks = lax.fori_loop(0, n_utt, add_utt, 0)
    n_tiles = (n_chunks + BODY_CHUNKS - 1) // BODY_CHUNKS

    def add_dummy(pos, carry):
        lrow[pos] = n_rows
        arow[pos] = n_utt * n_frames
        sbase[pos] = n_utt * skew_rows
        gbase[pos] = skew_rows
        utt_of[pos] = 0
        return carry
    lax.fori_loop(n_chunks, n_tiles * BODY_CHUNKS, add_dummy, 0)

    dc[...] = jnp.zeros_like(dc)
    da8[...] = jnp.zeros_like(da8)
    acc_o[...] = jnp.zeros_like(acc_o)
    occ_b[pl.ds(skew_rows, pad_rows), :] = jnp.zeros((pad_rows, LANES), F32)
    occ_l[pl.ds(skew_rows, pad_rows), :] = jnp.zeros((pad_rows, LANES), F32)
    act_f[pl.ds(n_utt * n_frames, 8), :] = jnp.zeros((8, act_f.shape[1]), F32)
    act_g[pl.ds(n_rows, CHUNK), :] = jnp.zeros((CHUNK, act_g.shape[1]), BF16)
    lab_v[pl.ds(n_rows, CHUNK), :] = jnp.full((CHUNK, LANES), -1, jnp.int32)

    lab_scr[...] = jnp.full_like(lab_scr, -1.0)
    lab_scr[:, :n_pos - 1] = labels_ref[pl.ds(pl.multiple_of(me * n_utt, n_utt), n_utt), :].astype(F32)
    lab_t = jnp.transpose(lab_scr[...])
    for b in range(n_utt):
        lab_v[pl.ds(b * n_pos, n_pos), :] = jnp.broadcast_to(lab_t[:n_pos, b:b + 1], (n_pos, LANES)).astype(jnp.int32)

    for cp in copies:
        cp.wait()
    act_f[pl.ds(0, n_utt * n_frames), :] = dot_nn(f_v[...], we_v[...]).astype(BF16).astype(F32)
    act_g[pl.ds(0, n_rows), :] = dot_nn(g_v[...], wp_v[...]).astype(BF16)
    wt_v[vocab:, :] = jnp.zeros((vocab_pad - vocab, wt_v.shape[1]), BF16)
    wt_v[:vocab, :] = wraw_v[...]
    wo_v[...] = jnp.transpose(wt_v[...])

    lane = lax.broadcasted_iota(jnp.int32, (CHUNK, LANES), 1)
    last_ok = lane < vocab - (n_grp - 1) * LANES

    def fwd_body(shifted, i, carry):
        r0 = pl.multiple_of(i * (SUBS * TILE), SUBS * TILE)
        c0 = i * BODY_CHUNKS
        for k in range(BODY_CHUNKS):
            lr = pl.multiple_of(lrow[c0 + k], CHUNK)
            pre = act_g[pl.ds(lr, CHUNK), :].astype(F32) + act_f[pl.ds(arow[c0 + k], 1), :]
            hid[pl.ds(r0 + k * CHUNK, CHUNK), :] = jnp.tanh(pre).astype(BF16)
        for sub in range(SUBS):
            z_v[sub][...] = dot_nn(hid[pl.ds(r0 + sub * TILE, TILE), :], wo_v[...])
        for k in range(BODY_CHUNKS):
            z_ref = z_v[k // TILE_CHUNKS]
            rows = pl.ds(r0 + k * CHUNK, CHUNK)
            z_rows = pl.ds(k % TILE_CHUNKS * CHUNK, CHUNK)
            ids = lab_v[pl.ds(pl.multiple_of(lrow[c0 + k], CHUNK), CHUNK), :]
            sb = sbase[c0 + k]
            zs = [z_ref[z_rows, j * LANES:(j + 1) * LANES] for j in range(n_grp)]
            picked = functools.reduce(jnp.add, [jnp.where(lane + j * LANES == ids, zs[j], 0.0) for j in range(n_grp)])
            picked = jnp.sum(picked, axis=1, keepdims=True)
            if shifted:
                top = functools.reduce(jnp.maximum, zs[:-1] + [jnp.where(last_ok, zs[-1], NEG_FILL)])
                top = jnp.max(top, axis=1, keepdims=True)
                es = [jnp.exp(z - top) for z in zs]
            else:
                es = [jnp.exp(z) for z in zs]
            es[-1] = jnp.where(last_ok, es[-1], 0.0)
            for j in range(n_grp):
                ex[rows, j * LANES:(j + 1) * LANES] = es[j]
            tot = jnp.sum(functools.reduce(jnp.add, es), axis=1, keepdims=True)
            tot_b = jnp.broadcast_to(tot, (CHUNK, LANES))
            sums[rows, :] = tot_b
            log_norm = jnp.log(tot_b)
            if shifted:
                log_norm = log_norm + top
            sk_b[pl.ds(sb, CHUNK, stride=pitch), :] = zs[0][:, 0:1] - log_norm
            sk_l[pl.ds(sb, CHUNK, stride=pitch), :] = picked - log_norm
        return carry

    bound = jnp.max(jnp.sum(jnp.abs(wo_v[...].astype(F32)), axis=0))

    @pl.when(bound < SAFE_LOGIT)
    def _():
        lax.fori_loop(0, n_tiles, functools.partial(fwd_body, False), 0)

    @pl.when(jnp.logical_not(bound < SAFE_LOGIT))
    def _():
        lax.fori_loop(0, n_tiles, functools.partial(fwd_body, True), 0)

    lane_s = lax.broadcasted_iota(jnp.int32, (n_frames, LANES), 1)
    sub_s = lax.broadcasted_iota(jnp.int32, (n_frames, LANES), 0)
    t_lens = jnp.zeros((n_frames, LANES), jnp.int32)
    u_lens = jnp.zeros((n_frames, LANES), jnp.int32)
    for b in range(n_utt):
        t_lens = jnp.where(lane_s == b, tlen_ref[me * n_utt + b], t_lens)
        u_lens = jnp.where(lane_s == b, ulen_ref[me * n_utt + b], u_lens)
    live_t = sub_s < t_lens
    last_t = sub_s == t_lens - 1

    def merge_diag(d):
        base = d * pitch
        bl = sk_b[pl.ds(base, n_frames), :]
        lb = sk_l[pl.ds(base, n_frames), :]
        for b in range(1, n_utt):
            off = base + b * skew_rows
            bl = jnp.where(lane_s == b, sk_b[pl.ds(off, n_frames), :], bl)
            lb = jnp.where(lane_s == b, sk_l[pl.ds(off, n_frames), :], lb)
        u = d - sub_s
        live = live_t & (u >= 0)
        here = pl.ds(pl.multiple_of(d * n_frames, n_frames), n_frames)
        cb_s[here, :] = jnp.where(live & (u <= u_lens), bl, NEG_FILL)
        cl_s[here, :] = jnp.where(live & (u < u_lens), lb, NEG_FILL)
        ce_s[here, :] = jnp.where(last_t & (u == u_lens), 1.0, 0.0)

    def merge_step(i, carry):
        for k in range(4):
            merge_diag(i * 4 + k)
        return carry
    lax.fori_loop(0, (n_frames + n_pos) // 4, merge_step, 0)

    def lattice_step(i, carry):
        a, be = carry
        fwd = pl.ds(pl.multiple_of(i * n_frames, n_frames), n_frames)
        bwd = pl.ds(pl.multiple_of((n_diag - 1 - i) * n_frames, n_frames), n_frames)
        back = (n_diag - 1 - i) * pitch
        al[pl.ds(i * pitch, n_frames), :] = a
        moved = jnp.where(sub_s == 0, NEG_FILL, pltpu.roll(a + cb_s[fwd, :], 1, 0))
        a = logadd(moved, a + cl_s[fwd, :])
        up = jnp.where(sub_s == n_frames - 1, NEG_FILL, pltpu.roll(be, n_frames - 1, 0))
        bl = cb_s[bwd, :]
        x_b = jnp.where(ce_s[bwd, :] > 0.0, bl, up + bl)
        x_l = be + cl_s[bwd, :]
        xb_s[pl.ds(back, n_frames), :] = x_b
        xl_s[pl.ds(back, n_frames), :] = x_l
        return a, logadd(x_b, x_l)

    def lattice_pair(i, carry):
        return lattice_step(2 * i + 1, lattice_step(2 * i, carry))

    neg = jnp.full((n_frames, LANES), NEG_FILL, F32)
    state = lax.fori_loop(0, n_diag // 2, lattice_pair, (jnp.where(sub_s == 0, 0.0, neg), neg))
    for i in range(n_diag // 2 * 2, n_diag):
        state = lattice_step(i, state)
    be0 = state[1]
    log_prob = be0[0:1, :]
    loss_ref[...] = jnp.broadcast_to(-log_prob, loss_ref.shape)

    n_live = n_diag * pitch
    for r in range(0, n_live, 64):
        rows = pl.ds(r, min(64, n_live - r))
        a = al[rows, :] - log_prob
        occ_b[rows, :] = jnp.exp(jnp.minimum(a + xb_s[rows, :], 0.0))
        occ_l[rows, :] = jnp.exp(jnp.minimum(a + xl_s[rows, :], 0.0))

    def bwd_tile(i, carry):
        r0 = pl.multiple_of(i * (SUBS * TILE), SUBS * TILE)
        c0 = i * BODY_CHUNKS
        for sub in range(SUBS):
            for kk in range(TILE_CHUNKS):
                k = sub * TILE_CHUNKS + kk
                rows = pl.ds(r0 + k * CHUNK, CHUNK)
                gb0 = gbase[c0 + k]
                mine = lane == utt_of[c0 + k]
                ids = lab_v[pl.ds(pl.multiple_of(lrow[c0 + k], CHUNK), CHUNK), :]
                ob = jnp.sum(jnp.where(mine, occ_b[pl.ds(gb0, CHUNK, stride=pitch), :], 0.0), axis=1, keepdims=True)
                ol = jnp.sum(jnp.where(mine, occ_l[pl.ds(gb0, CHUNK, stride=pitch), :], 0.0), axis=1, keepdims=True)
                scale = (ob + ol) / sums[rows, :]
                for j in range(n_grp):
                    dz = ex[rows, j * LANES:(j + 1) * LANES] * scale
                    if j == 0:
                        dz = dz - jnp.where(lane == 0, ob, 0.0)
                    dz = dz - jnp.where(lane + j * LANES == ids, ol, 0.0)
                    dz_v[sub][kk * CHUNK:(kk + 1) * CHUNK, j * LANES:(j + 1) * LANES] = dz.astype(BF16)
        for sub in range(SUBS):
            z_v[sub][...] = dot_nn(dz_v[sub][...], wt_v[...])
        for sub in range(SUBS):
            for kk in range(TILE_CHUNKS):
                k = sub * TILE_CHUNKS + kk
                lr = pl.multiple_of(lrow[c0 + k], CHUNK)
                ar = pl.multiple_of(arow[c0 + k] * 8, 8)
                h = hid[pl.ds(r0 + k * CHUNK, CHUNK), :].astype(F32)
                dp = (z_v[sub][kk * CHUNK:(kk + 1) * CHUNK, :] * (1.0 - h * h)).astype(BF16).astype(F32)
                dc[pl.ds(lr, CHUNK), :] += dp
                da8[pl.ds(ar, 8), :] += dp[:8, :] + dp[8:, :]
        dz_all = jnp.concatenate([dz_v[sub][...] for sub in range(SUBS)], axis=0)
        acc_o[...] += dot_tn(dz_all, hid[pl.ds(r0, SUBS * TILE), :])
        return carry
    lax.fori_loop(0, n_tiles, bwd_tile, 0)

    n_af = n_utt * n_frames
    d_act_f = jnp.sum(da8[pl.ds(0, n_af * 8), :].reshape(n_af, 8, da8.shape[1]), axis=1).astype(BF16)
    da_ref[...] = d_act_f
    gwo_ref[...] = acc_o[...]
    gwp_ref[...] = dot_tn(g_v[...], dc[pl.ds(0, n_rows), :].astype(BF16))


def local_grads(seq_idx, enc_rows, pred_out, w_enc, w_pred, w_out_t, labels, frame_len, label_len, n_utt, n_frames, n_loc, vocab):
    n_pos = labels.shape[1] + 1
    enc_dim, joint = w_enc.shape
    vocab_pad = pl.cdiv(vocab, LANES) * LANES
    n_rows = n_utt * n_pos
    n_af = n_utt * n_frames
    max_rows = n_utt * n_frames * n_pos
    skew_rows = (n_frames + n_pos) * (n_frames + 1)
    n_chunks = max_rows // CHUNK + BODY_CHUNKS
    any_spec = pl.BlockSpec(memory_space=pl.ANY)
    vmem = pl.BlockSpec(memory_space=pltpu.VMEM)
    grid_spec = pltpu.PrefetchScalarGridSpec(
        num_scalar_prefetch=3, grid=(),
        in_specs=[any_spec] * 5 + [vmem],
        out_specs=[vmem] * 4,
        scratch_shapes=[
            pltpu.VMEM((n_af, enc_dim), BF16),
            pltpu.VMEM((n_rows, w_pred.shape[0]), BF16),
            pltpu.VMEM(w_enc.shape, BF16),
            pltpu.VMEM(w_pred.shape, BF16),
            pltpu.VMEM(w_out_t.shape, BF16),
            pltpu.VMEM((joint, vocab_pad), BF16),
            pltpu.VMEM((vocab_pad, joint), BF16),
            pltpu.VMEM((n_af + 8, joint), F32),
            pltpu.VMEM((n_rows + CHUNK, joint), BF16),
            pltpu.VMEM((n_rows + CHUNK, LANES), jnp.int32),
            pltpu.VMEM((n_utt, LANES), F32),
            pltpu.VMEM((max_rows, joint), BF16),
            pltpu.VMEM((max_rows, vocab_pad), F32),
            pltpu.VMEM((max_rows, LANES), F32),
            pltpu.VMEM((n_utt * skew_rows + CHUNK * (n_frames + 1), LANES), F32),
            pltpu.VMEM((n_utt * skew_rows + CHUNK * (n_frames + 1), LANES), F32),
            pltpu.VMEM(((n_frames + n_pos) * n_frames, LANES), F32),
            pltpu.VMEM(((n_frames + n_pos) * n_frames, LANES), F32),
            pltpu.VMEM(((n_frames + n_pos) * n_frames, LANES), F32),
            pltpu.VMEM((skew_rows, LANES), F32),
            pltpu.VMEM((skew_rows, LANES), F32),
            pltpu.VMEM((skew_rows, LANES), F32),
            pltpu.VMEM((skew_rows + CHUNK * (n_frames + 1), LANES), F32),
            pltpu.VMEM((skew_rows + CHUNK * (n_frames + 1), LANES), F32),
            pltpu.VMEM((TILE, vocab_pad), BF16),
            pltpu.VMEM((TILE, vocab_pad), BF16),
            pltpu.VMEM((TILE, max(joint, vocab_pad)), F32),
            pltpu.VMEM((TILE, max(joint, vocab_pad)), F32),
            pltpu.VMEM((vocab_pad, joint), F32),
            pltpu.VMEM((n_rows + CHUNK, joint), F32),
            pltpu.VMEM((n_af * 8 + 8, joint), F32),
            pltpu.SMEM((n_chunks,), jnp.int32),
            pltpu.SMEM((n_chunks,), jnp.int32),
            pltpu.SMEM((n_chunks,), jnp.int32),
            pltpu.SMEM((n_chunks,), jnp.int32),
            pltpu.SMEM((n_chunks,), jnp.int32),
            pltpu.SemaphoreType.DMA((5,)),
        ])
    return pl.pallas_call(
        functools.partial(local_kernel, n_utt, n_frames, n_loc, n_pos, vocab),
        grid_spec=grid_spec,
        out_shape=[
            jax.ShapeDtypeStruct((8, LANES), F32),
            jax.ShapeDtypeStruct((n_af, joint), BF16),
            jax.ShapeDtypeStruct((w_pred.shape[0], joint), F32),
            jax.ShapeDtypeStruct((vocab_pad, joint), F32),
        ],
        compiler_params=pltpu.CompilerParams(vmem_limit_bytes=62 << 20),
        cost_estimate=pl.CostEstimate(flops=6 * max_rows * joint * vocab_pad, bytes_accessed=4 * max_rows * joint, transcendentals=2 * max_rows * joint),
        name="rnnt_local",
    )(seq_idx, frame_len, label_len, enc_rows, pred_out, w_enc, w_pred, w_out_t, labels)


def greet(seq_size, me):
    barrier = pltpu.get_barrier_semaphore()
    for j in range(1, seq_size):
        pl.semaphore_signal(barrier, inc=1, device_id={'seq': lax.rem(me + j, seq_size)}, device_id_type=pl.DeviceIdType.MESH)
    pl.semaphore_wait(barrier, seq_size - 1)


def spread_kernel(seq_size, rows, enc_ref, out_ref, send, recv):
    me = lax.axis_index('seq')
    greet(seq_size, me)
    mine = pl.ds(pl.multiple_of(me * rows, rows), rows)
    copies = []
    for j in range(1, seq_size):
        peer = lax.rem(me + j, seq_size)
        copies.append(pltpu.make_async_remote_copy(
            src_ref=enc_ref.at[pl.ds(pl.multiple_of(peer * rows, rows), rows), :], dst_ref=out_ref.at[mine, :],
            send_sem=send.at[j - 1], recv_sem=recv.at[j - 1], device_id={'seq': peer}, device_id_type=pl.DeviceIdType.MESH))
        copies[-1].start()
    out_ref[mine, :] = enc_ref[mine, :]
    for copy in copies:
        copy.wait()


def spread_frames(enc_rows, seq_size):
    rows = enc_rows.shape[0] // seq_size
    vmem = pl.BlockSpec(memory_space=pltpu.VMEM)
    return pl.pallas_call(
        functools.partial(spread_kernel, seq_size, rows),
        out_shape=jax.ShapeDtypeStruct(enc_rows.shape, enc_rows.dtype),
        in_specs=[vmem], out_specs=vmem,
        scratch_shapes=[pltpu.SemaphoreType.DMA((seq_size - 1,)), pltpu.SemaphoreType.DMA((seq_size - 1,))],
        compiler_params=pltpu.CompilerParams(collective_id=0, has_side_effects=True),
        name="spread_frames",
    )(enc_rows)


def reduce_kernel(seq_size, n_mat, da_ref, loss_ref, *refs):
    gw = refs[:n_mat]
    da_all, loss_out = refs[n_mat:n_mat + 2]
    out = refs[n_mat + 2:2 * n_mat + 2]
    rest = refs[2 * n_mat + 2:]
    sib_buf, own, ring_buf = rest[:n_mat], rest[n_mat:2 * n_mat], rest[2 * n_mat:3 * n_mat]
    (load_sem, sib_send, sib_recv, rs_send, rs_recv, ag_send, ag_recv, dd_send, dd_recv,
     da_send, da_recv, ds_send, ds_recv, lo_send, lo_recv) = rest[3 * n_mat:]
    me = lax.axis_index('seq')
    n_chip = seq_size // 2
    chip, core = lax.div(me, 2), lax.rem(me, 2)
    sibling = chip * 2 + 1 - core
    nexts = (lax.rem(chip + 1, n_chip) * 2 + core, lax.rem(chip + n_chip - 1, n_chip) * 2 + core)
    half = gw[0].shape[0] // 2
    piece = half // (2 * n_chip)

    def remote(src, dst, send, recv, peer):
        copy = pltpu.make_async_remote_copy(src_ref=src, dst_ref=dst, send_sem=send, recv_sem=recv,
                                            device_id={'seq': peer}, device_id_type=pl.DeviceIdType.MESH)
        copy.start()
        return copy

    def behind(way, hops):
        return lax.rem(chip + n_chip - hops, n_chip) if way == 0 else lax.rem(chip + hops, n_chip)

    def at(way, hops):
        return pl.multiple_of((behind(way, hops) * 2 + way) * piece, piece)

    loads = []
    for m in range(n_mat):
        loads.append(pltpu.make_async_copy(gw[m].at[pl.ds(pl.multiple_of(core * half, half), half), :], own[m], load_sem.at[m]))
        loads[-1].start()
    greet(seq_size, me)

    rows = da_ref.shape[0] // 2
    hop1 = {}
    for part in range(2):
        for way in range(2):
            r = pl.ds((way if part == 0 else 1 - way) * rows, rows)
            hop1[way, part] = remote(da_ref.at[r, :], da_all.at[me, r, :], da_send.at[way, part], da_recv.at[way, part], nexts[way])
    sib = []
    for m in range(n_mat):
        sib.append(remote(gw[m].at[pl.ds(pl.multiple_of((1 - core) * half, half), half), :], sib_buf[m], sib_send.at[m], sib_recv.at[m], sibling))
    relays = [remote(da_ref, da_all.at[me], ds_send.at[0], ds_recv.at[0], sibling)]
    small = []
    for j in range(1, seq_size):
        small.append(remote(loss_ref, loss_out.at[me], lo_send.at[j - 1], lo_recv.at[j - 1], lax.rem(me + j, seq_size)))
    loss_out[pl.ds(me, 1)] = loss_ref[...][None]
    da_all[pl.ds(me, 1)] = da_ref[...][None]

    ring = {}
    for m in range(n_mat):
        loads[m].wait()
        sib[m].wait_recv()
        own[m][...] = own[m][...] + sib_buf[m][...]
        for way in range(2):
            ring[m, way, 0] = remote(own[m].at[pl.ds(at(way, 1), piece), :], ring_buf[m].at[way, 0], rs_send.at[m, way, 0], rs_recv.at[m, way, 0], nexts[way])

    def block(way, hops, r):
        return da_all.at[behind(way, hops) * 2 + core, r, :]

    hop2 = {}
    for way in range(2):
        r = pl.ds(way * rows, rows)
        hop1[way, 0].wait_recv()
        hop2[way] = remote(block(way, 1, r), block(way, 1, r), da_send.at[way, 2], da_recv.at[way, 2], nexts[way])
        relays.append(remote(block(way, 1, r), block(way, 1, r), ds_send.at[1 + way], ds_recv.at[1 + way], sibling))
    for way in range(2):
        r = pl.ds((1 - way) * rows, rows)
        hop1[way, 1].wait_recv()
        relays.append(remote(block(way, 1, r), block(way, 1, r), ds_send.at[3 + way], ds_recv.at[3 + way], sibling))

    for s in range(1, n_chip - 1):
        for m in range(n_mat):
            for way in range(2):
                ring[m, way, s - 1].wait_recv()
                ring_buf[m][way, s - 1] = ring_buf[m][way, s - 1] + own[m][pl.ds(at(way, s + 1), piece), :]
                ring[m, way, s] = remote(ring_buf[m].at[way, s - 1], ring_buf[m].at[way, s], rs_send.at[m, way, s], rs_recv.at[m, way, s], nexts[way])
    for way in range(2):
        r = pl.ds(way * rows, rows)
        hop2[way].wait_recv()
        relays.append(remote(block(way, 2, r), block(way, 2, r), ds_send.at[5 + way], ds_recv.at[5 + way], sibling))

    def place(way, hops):
        return pl.ds(pl.multiple_of(core * half + at(way, hops), piece), piece)

    last = n_chip - 2
    gather = {}
    for m in range(n_mat):
        for way in range(2):
            ring[m, way, last].wait_recv()
            here = place(way, 0)
            out[m][here, :] = ring_buf[m][way, last] + own[m][pl.ds(at(way, 0), piece), :]
            gather[m, way, 0] = remote(out[m].at[here, :], out[m].at[here, :], ag_send.at[m, way, 0], ag_recv.at[m, way, 0], nexts[way])
            relays.append(remote(out[m].at[here, :], out[m].at[here, :], dd_send.at[m, way, 0], dd_recv.at[m, way, 0], sibling))
    for s in range(1, n_chip):
        for m in range(n_mat):
            for way in range(2):
                gather[m, way, s - 1].wait_recv()
                here = place(way, s)
                if s < n_chip - 1:
                    gather[m, way, s] = remote(out[m].at[here, :], out[m].at[here, :], ag_send.at[m, way, s], ag_recv.at[m, way, s], nexts[way])
                relays.append(remote(out[m].at[here, :], out[m].at[here, :], dd_send.at[m, way, s], dd_recv.at[m, way, s], sibling))
    for copy in relays + small:
        copy.wait()
    for copy in list(ring.values()) + list(gather.values()) + sib + list(hop1.values()) + list(hop2.values()):
        copy.wait_send()


def reduce_all(da, loss, grads, seq_size):
    n_mat = len(grads)
    n_chip = seq_size // 2
    half = grads[0].shape[0] // 2
    piece = half // (2 * n_chip)
    vmem = pl.BlockSpec(memory_space=pltpu.VMEM)
    dma = pltpu.SemaphoreType.DMA
    steps = n_chip - 1
    return pl.pallas_call(
        functools.partial(reduce_kernel, seq_size, n_mat),
        out_shape=[jax.ShapeDtypeStruct((seq_size,) + da.shape, da.dtype), jax.ShapeDtypeStruct((seq_size,) + loss.shape, F32)]
        + [jax.ShapeDtypeStruct(g.shape, F32) for g in grads],
        in_specs=[vmem] * 2 + [pl.BlockSpec(memory_space=pl.ANY)] * n_mat, out_specs=[vmem] * (2 + n_mat),
        scratch_shapes=[pltpu.VMEM((half, g.shape[1]), F32) for g in grads] * 2
        + [pltpu.VMEM((2, steps, piece, g.shape[1]), F32) for g in grads]
        + [dma((n_mat,))] * 3 + [dma((n_mat, 2, steps))] * 4 + [dma((n_mat, 2, n_chip))] * 2
        + [dma((2, 3))] * 2 + [dma((7,))] * 2 + [dma((seq_size - 1,))] * 2,
        compiler_params=pltpu.CompilerParams(collective_id=1, has_side_effects=True, vmem_limit_bytes=24 << 20),
        name="reduce_all",
    )(da, loss, *grads)


def finish_kernel(seq_size, vocab, me_ref, da_all, loss_ref, gwp_ref, gwo_ref, we_ref, *refs):
    f_refs = refs[:seq_size]
    loss_out, genc_out, gwe_out, gwp_out, gwo_out, f_all, d_all = refs[seq_size:]
    me = me_ref[0]
    n_af = da_all.shape[1]
    rows = n_af // seq_size
    gwp_out[...] = gwp_ref[...]
    gwo_out[...] = gwo_ref[:vocab, :]
    loss_out[...] = loss_ref[:, 0, :]
    for j in range(seq_size):
        owner = lax.rem(me + seq_size - j, seq_size)
        f_all[pl.ds(j * n_af, n_af), :] = f_refs[j][...]
        for src in range(seq_size):
            d_all[pl.ds(j * n_af + src * rows, rows), :] = da_all[src, pl.ds(pl.multiple_of(owner * rows, rows), rows), :]
    genc_out[...] = dot_nt(d_all[:n_af, :], we_ref[...]).astype(BF16)
    gwe_out[...] = dot_tn(f_all[...], d_all[...])


def finish(seq_idx, da_all, loss_all, gwp, gwo_t, w_enc, frames, vocab):
    seq_size, n_af, joint = da_all.shape
    vmem = pl.BlockSpec(memory_space=pltpu.VMEM)
    return pl.pallas_call(
        functools.partial(finish_kernel, seq_size, vocab),
        grid_spec=pltpu.PrefetchScalarGridSpec(
            num_scalar_prefetch=1, grid=(), in_specs=[vmem] * (5 + seq_size), out_specs=[vmem] * 5,
            scratch_shapes=[pltpu.VMEM((seq_size * n_af, frames[0].shape[1]), BF16), pltpu.VMEM((seq_size * n_af, joint), BF16)]),
        out_shape=[
            jax.ShapeDtypeStruct((seq_size, loss_all.shape[2]), F32),
            jax.ShapeDtypeStruct(frames[0].shape, BF16),
            jax.ShapeDtypeStruct(w_enc.shape, F32),
            jax.ShapeDtypeStruct(gwp.shape, F32),
            jax.ShapeDtypeStruct((vocab, joint), F32),
        ],
        compiler_params=pltpu.CompilerParams(vmem_limit_bytes=24 << 20),
        name="finish",
    )(seq_idx, da_all, loss_all, gwp, gwo_t, w_enc, *frames)


def solution(mesh):
    seq_size = mesh.shape['seq']

    def local_fn(enc_out, pred_out, w_enc, w_pred, w_out, labels, frame_len, label_len):
        seq_idx = jnp.reshape(lax.axis_index('seq'), (1,)).astype(jnp.int32)
        n_all, n_loc, enc_dim = enc_out.shape
        n_utt = n_all // seq_size
        n_frames = n_loc * seq_size
        vocab = w_out.shape[1]
        enc_local = enc_out.reshape(n_all * n_loc, enc_dim)
        enc_local, enc_rows = lax.optimization_barrier((enc_local, spread_frames(enc_local, seq_size)))
        frames = [enc_local] + [lax.ppermute(enc_local, 'seq', [(i, (i + j) % seq_size) for i in range(seq_size)]) for j in range(1, seq_size)]
        loss, da, *grads = local_grads(
            seq_idx, enc_rows, pred_out.reshape(-1, pred_out.shape[2]), w_enc, w_pred, w_out.T,
            labels, frame_len, label_len, n_utt, n_frames, n_loc, vocab)
        da_all, loss_all, gwp, gwo_t = reduce_all(da, loss, grads, seq_size)
        loss, genc, gwe, gwp, gwo_t = finish(seq_idx, da_all, loss_all, gwp, gwo_t, w_enc, frames, vocab)
        return loss[:, :n_utt].reshape(n_all), genc.reshape(n_all, n_loc, enc_dim), gwe, gwp, gwo_t.T

    in_specs = (P('dp', 'seq', None), P('dp', None, None), P(None, None), P(None, None), P(None, None), P('dp', None), P('dp'), P('dp'))
    out_specs = (P('dp'), P('dp', 'seq', None), P('dp', None), P('dp', None), P('dp', None))
    return jax.shard_map(local_fn, mesh=mesh, in_specs=in_specs, out_specs=out_specs, check_vma=False)
```

```python
import functools

import jax
import jax.numpy as jnp
from jax import lax
from jax.experimental import pallas as pl
from jax.experimental.pallas import tpu as pltpu
from jax.sharding import PartitionSpec as P

NEG_FILL = -1.0e30
CHUNK = 16
LANES = 128
TILE_CHUNKS = 16
TILE = CHUNK * TILE_CHUNKS
SUBS = 2
BODY_CHUNKS = SUBS * TILE_CHUNKS
SAFE_LOGIT = 60.0
F32 = jnp.float32
BF16 = jnp.bfloat16


def logadd(x, y):
    return jnp.maximum(x, y) + jnp.log(1.0 + jnp.exp(-jnp.abs(x - y)))


def dot_nn(x, y):
    return jnp.dot(x, y, preferred_element_type=F32)


def dot_tn(x, y):
    return lax.dot_general(x, y, (((0,), (0,)), ((), ())), preferred_element_type=F32)


def dot_nt(x, y):
    return lax.dot_general(x, y, (((1,), (1,)), ((), ())), preferred_element_type=F32)


def local_kernel(n_utt, n_frames, n_loc, n_pos, vocab,
                 seq_ref, tlen_ref, ulen_ref,
                 enc_ref, pred_hbm, wenc_hbm, wpred_hbm, wout_t_hbm, labels_ref,
                 loss_ref, da_ref, gwp_ref, gwo_ref,
                 g_v, we_v, wp_v, wraw_v, wo_v, wt_v, act_f, act_g, lab_v, lab_scr,
                 hid, ex, sums, skew, cb_s, cl_s, ce_s, al, xb_s, xl_s, occ, dz_0, dz_1, z_0, z_1,
                 acc_o, dc, da8, lrow, arow, drow, sbase, gbase, utt_of, uid, sems):
    me = seq_ref[0]
    dz_v, z_v = (dz_0, dz_1), (z_0, z_1)
    n_diag = n_frames + n_pos - 1
    pitch = n_frames + 1
    skew_rows = (n_frames + n_pos) * pitch
    n_rows = n_utt * n_pos
    vocab_pad = wt_v.shape[0]
    n_grp = vocab_pad // LANES
    pad_rows = occ.shape[0] - skew_rows

    n_all = n_utt * (n_frames // n_loc)
    for b in range(n_utt):
        uid[b] = me * n_utt + b
    copies = [
        pltpu.make_async_copy(pred_hbm.at[pl.ds(pl.multiple_of(uid[b] * n_pos, n_pos), n_pos), :], g_v.at[pl.ds(b * n_pos, n_pos), :], sems.at[3 + b])
        for b in range(n_utt)] + [
        pltpu.make_async_copy(wenc_hbm, we_v, sems.at[0]),
        pltpu.make_async_copy(wpred_hbm, wp_v, sems.at[1]),
        pltpu.make_async_copy(wout_t_hbm, wraw_v, sems.at[2]),
    ]
    for cp in copies:
        cp.start()

    def add_utt(b, pos):
        t_len = tlen_ref[uid[b]]
        n_chunk = (ulen_ref[uid[b]] + CHUNK) // CHUNK

        def add_frame(t, pos):
            def add_chunk(q, pos):
                lrow[pos] = b * n_pos + q * CHUNK
                arow[pos] = t // n_loc * (n_all * n_loc) + uid[b] * n_loc + t % n_loc
                drow[pos] = t // n_loc * (n_utt * n_loc) + b * n_loc + t % n_loc
                skew = (pitch + 1) * t + pitch * CHUNK * q
                sbase[pos] = b * skew_rows + skew
                gbase[pos] = skew
                utt_of[pos] = b
                return pos + 1
            return lax.fori_loop(0, n_chunk, add_chunk, pos)
        return lax.fori_loop(0, t_len, add_frame, pos)

    n_chunks = lax.fori_loop(0, n_utt, add_utt, 0)
    n_tiles = (n_chunks + BODY_CHUNKS - 1) // BODY_CHUNKS

    def add_dummy(pos, carry):
        lrow[pos] = n_rows
        arow[pos] = n_all * n_frames
        drow[pos] = n_utt * n_frames
        sbase[pos] = n_utt * skew_rows
        gbase[pos] = skew_rows
        utt_of[pos] = 0
        return carry
    lax.fori_loop(n_chunks, n_tiles * BODY_CHUNKS, add_dummy, 0)

    dc[...] = jnp.zeros_like(dc)
    da8[...] = jnp.zeros_like(da8)
    acc_o[...] = jnp.zeros_like(acc_o)
    occ[pl.ds(skew_rows, pad_rows), :] = jnp.zeros((pad_rows, LANES), F32)
    act_f[pl.ds(n_all * n_frames, 8), :] = jnp.zeros((8, act_f.shape[1]), F32)
    act_g[pl.ds(n_rows, CHUNK), :] = jnp.zeros((CHUNK, act_g.shape[1]), BF16)
    lab_v[pl.ds(n_rows, CHUNK), :] = jnp.full((CHUNK, LANES), -1, jnp.int32)

    lab_scr[...] = jnp.full_like(lab_scr, -1.0)
    for b in range(n_utt):
        lab_scr[b:b + 1, :n_pos - 1] = labels_ref[pl.ds(uid[b], 1), :].astype(F32)
    lab_t = jnp.transpose(lab_scr[...])
    for b in range(n_utt):
        lab_v[pl.ds(b * n_pos, n_pos), :] = jnp.broadcast_to(lab_t[:n_pos, b:b + 1], (n_pos, LANES)).astype(jnp.int32)

    for cp in copies:
        cp.wait()
    for blk in range(enc_ref.shape[0]):
        n_blk = enc_ref.shape[1]
        act_f[blk * n_blk:(blk + 1) * n_blk, :] = dot_nn(enc_ref[blk], we_v[...]).astype(BF16).astype(F32)
    act_g[pl.ds(0, n_rows), :] = dot_nn(g_v[...], wp_v[...]).astype(BF16)
    wt_v[vocab:, :] = jnp.zeros((vocab_pad - vocab, wt_v.shape[1]), BF16)
    wt_v[:vocab, :] = wraw_v[...]
    wo_v[...] = jnp.transpose(wt_v[...])

    lane = lax.broadcasted_iota(jnp.int32, (CHUNK, LANES), 1)
    left = lane < LANES // 2
    last_ok = lane < vocab - (n_grp - 1) * LANES

    def fwd_body(shifted, i, carry):
        r0 = pl.multiple_of(i * (SUBS * TILE), SUBS * TILE)
        c0 = i * BODY_CHUNKS
        for k in range(BODY_CHUNKS):
            lr = pl.multiple_of(lrow[c0 + k], CHUNK)
            pre = act_g[pl.ds(lr, CHUNK), :].astype(F32) + act_f[pl.ds(arow[c0 + k], 1), :]
            hid[pl.ds(r0 + k * CHUNK, CHUNK), :] = jnp.tanh(pre).astype(BF16)
        for sub in range(SUBS):
            z_v[sub][...] = dot_nn(hid[pl.ds(r0 + sub * TILE, TILE), :], wo_v[...])
        for k in range(BODY_CHUNKS):
            z_ref = z_v[k // TILE_CHUNKS]
            rows = pl.ds(r0 + k * CHUNK, CHUNK)
            z_rows = pl.ds(k % TILE_CHUNKS * CHUNK, CHUNK)
            ids = lab_v[pl.ds(pl.multiple_of(lrow[c0 + k], CHUNK), CHUNK), :]
            sb = sbase[c0 + k]
            zs = [z_ref[z_rows, j * LANES:(j + 1) * LANES] for j in range(n_grp)]
            picked = functools.reduce(jnp.add, [jnp.where(lane + j * LANES == ids, zs[j], 0.0) for j in range(n_grp)])
            picked = jnp.sum(picked, axis=1, keepdims=True)
            if shifted:
                top = functools.reduce(jnp.maximum, zs[:-1] + [jnp.where(last_ok, zs[-1], NEG_FILL)])
                top = jnp.max(top, axis=1, keepdims=True)
                es = [jnp.exp(z - top) for z in zs]
            else:
                es = [jnp.exp(z) for z in zs]
            es[-1] = jnp.where(last_ok, es[-1], 0.0)
            for j in range(n_grp):
                ex[rows, j * LANES:(j + 1) * LANES] = es[j]
            tot = jnp.sum(functools.reduce(jnp.add, es), axis=1, keepdims=True)
            tot_b = jnp.broadcast_to(tot, (CHUNK, LANES))
            sums[rows, :] = tot_b
            log_norm = jnp.log(tot_b)
            if shifted:
                log_norm = log_norm + top
            skew[pl.ds(sb, CHUNK, stride=pitch), :] = jnp.where(left, zs[0][:, 0:1], picked) - log_norm
        return carry

    bound = jnp.max(jnp.sum(jnp.abs(wo_v[...].astype(F32)), axis=0))

    @pl.when(bound < SAFE_LOGIT)
    def _():
        lax.fori_loop(0, n_tiles, functools.partial(fwd_body, False), 0)

    @pl.when(jnp.logical_not(bound < SAFE_LOGIT))
    def _():
        lax.fori_loop(0, n_tiles, functools.partial(fwd_body, True), 0)

    lane_s = lax.broadcasted_iota(jnp.int32, (n_frames, LANES), 1)
    sub_s = lax.broadcasted_iota(jnp.int32, (n_frames, LANES), 0)
    t_lens = jnp.zeros((n_frames, LANES), jnp.int32)
    u_lens = jnp.zeros((n_frames, LANES), jnp.int32)
    for b in range(n_utt):
        t_lens = jnp.where(lane_s == b, tlen_ref[uid[b]], t_lens)
        u_lens = jnp.where(lane_s == b, ulen_ref[uid[b]], u_lens)
    slot_s = lane_s % (LANES // 2)
    live_t = sub_s < t_lens
    last_t = sub_s == t_lens - 1

    def merge_diag(d):
        base = d * pitch
        both = skew[pl.ds(base, n_frames), :]
        for b in range(1, n_utt):
            both = jnp.where(slot_s == b, skew[pl.ds(base + b * skew_rows, n_frames), :], both)
        bl = both
        lb = pltpu.roll(both, LANES // 2, 1)
        u = d - sub_s
        live = live_t & (u >= 0)
        here = pl.ds(pl.multiple_of(d * n_frames, n_frames), n_frames)
        cb_s[here, :] = jnp.where(live & (u <= u_lens), bl, NEG_FILL)
        cl_s[here, :] = jnp.where(live & (u < u_lens), lb, NEG_FILL)
        ce_s[here, :] = jnp.where(last_t & (u == u_lens), 1.0, 0.0)

    def merge_step(i, carry):
        for k in range(4):
            merge_diag(i * 4 + k)
        return carry
    lax.fori_loop(0, (n_frames + n_pos) // 4, merge_step, 0)

    def lattice_step(i, carry):
        a, be = carry
        fwd = pl.ds(pl.multiple_of(i * n_frames, n_frames), n_frames)
        bwd = pl.ds(pl.multiple_of((n_diag - 1 - i) * n_frames, n_frames), n_frames)
        back = (n_diag - 1 - i) * pitch
        al[pl.ds(i * pitch, n_frames), :] = a
        moved = jnp.where(sub_s == 0, NEG_FILL, pltpu.roll(a + cb_s[fwd, :], 1, 0))
        a = logadd(moved, a + cl_s[fwd, :])
        up = jnp.where(sub_s == n_frames - 1, NEG_FILL, pltpu.roll(be, n_frames - 1, 0))
        bl = cb_s[bwd, :]
        x_b = jnp.where(ce_s[bwd, :] > 0.0, bl, up + bl)
        x_l = be + cl_s[bwd, :]
        xb_s[pl.ds(back, n_frames), :] = x_b
        xl_s[pl.ds(back, n_frames), :] = x_l
        return a, logadd(x_b, x_l)

    def lattice_pair(i, carry):
        return lattice_step(2 * i + 1, lattice_step(2 * i, carry))

    neg = jnp.full((n_frames, LANES), NEG_FILL, F32)
    state = lax.fori_loop(0, n_diag // 2, lattice_pair, (jnp.where(sub_s == 0, 0.0, neg), neg))
    for i in range(n_diag // 2 * 2, n_diag):
        state = lattice_step(i, state)
    be0 = state[1]
    log_prob = be0[0:1, :]
    lane_8 = lax.broadcasted_iota(jnp.int32, loss_ref.shape, 1)
    loss_ref[...] = functools.reduce(jnp.add, [
        jnp.where(lane_8 == uid[b], -log_prob[:, b:b + 1], 0.0) for b in range(n_utt)])

    n_live = n_diag * pitch
    n_blk = CHUNK
    left_8 = left
    for r in range(0, pl.cdiv(n_live, n_blk) * n_blk, n_blk):
        rows = pl.ds(r, n_blk)
        a = al[rows, :] - log_prob
        x = jnp.where(left_8, a + xb_s[rows, :], pltpu.roll(a + xl_s[rows, :], LANES // 2, 1))
        occ[rows, :] = jnp.exp(jnp.minimum(x, 0.0))

    def bwd_tile(i, carry):
        r0 = pl.multiple_of(i * (SUBS * TILE), SUBS * TILE)
        c0 = i * BODY_CHUNKS
        for sub in range(SUBS):
            for kk in range(TILE_CHUNKS):
                k = sub * TILE_CHUNKS + kk
                rows = pl.ds(r0 + k * CHUNK, CHUNK)
                gb0 = gbase[c0 + k]
                both = occ[pl.ds(gb0, CHUNK, stride=pitch), :]
                ids = lab_v[pl.ds(pl.multiple_of(lrow[c0 + k], CHUNK), CHUNK), :]
                ob = jnp.sum(jnp.where(lane == utt_of[c0 + k], both, 0.0), axis=1, keepdims=True)
                ol = jnp.sum(jnp.where(lane == utt_of[c0 + k] + LANES // 2, both, 0.0), axis=1, keepdims=True)
                scale = (ob + ol) / sums[rows, :]
                for j in range(n_grp):
                    dz = ex[rows, j * LANES:(j + 1) * LANES] * scale
                    if j == 0:
                        dz = dz - jnp.where(lane == 0, ob, 0.0)
                    dz = dz - jnp.where(lane + j * LANES == ids, ol, 0.0)
                    dz_v[sub][kk * CHUNK:(kk + 1) * CHUNK, j * LANES:(j + 1) * LANES] = dz.astype(BF16)
        for sub in range(SUBS):
            z_v[sub][...] = dot_nn(dz_v[sub][...], wt_v[...])
        for sub in range(SUBS):
            for kk in range(TILE_CHUNKS):
                k = sub * TILE_CHUNKS + kk
                lr = pl.multiple_of(lrow[c0 + k], CHUNK)
                ar = pl.multiple_of(drow[c0 + k] * 8, 8)
                h = hid[pl.ds(r0 + k * CHUNK, CHUNK), :].astype(F32)
                dp = (z_v[sub][kk * CHUNK:(kk + 1) * CHUNK, :] * (1.0 - h * h)).astype(BF16).astype(F32)
                dc[pl.ds(lr, CHUNK), :] += dp
                da8[pl.ds(ar, 8), :] += dp[:8, :] + dp[8:, :]
        dz_all = jnp.concatenate([dz_v[sub][...] for sub in range(SUBS)], axis=0)
        acc_o[...] += dot_tn(dz_all, hid[pl.ds(r0, SUBS * TILE), :])
        return carry
    lax.fori_loop(0, n_tiles, bwd_tile, 0)

    n_af = n_utt * n_frames
    d_act_f = jnp.sum(da8[pl.ds(0, n_af * 8), :].reshape(n_af, 8, da8.shape[1]), axis=1).astype(BF16)
    da_ref[...] = d_act_f
    gwo_ref[...] = acc_o[...]
    gwp_ref[...] = dot_tn(g_v[...], dc[pl.ds(0, n_rows), :].astype(BF16))


def local_grads(seq_idx, enc_all, pred_out, w_enc, w_pred, w_out_t, labels, frame_len, label_len, n_utt, n_frames, n_loc, vocab):
    n_pos = labels.shape[1] + 1
    enc_dim, joint = w_enc.shape
    vocab_pad = pl.cdiv(vocab, LANES) * LANES
    n_rows = n_utt * n_pos
    n_af = n_utt * n_frames
    max_rows = n_utt * n_frames * n_pos
    skew_rows = (n_frames + n_pos) * (n_frames + 1)
    n_chunks = max_rows // CHUNK + BODY_CHUNKS
    any_spec = pl.BlockSpec(memory_space=pl.ANY)
    vmem = pl.BlockSpec(memory_space=pltpu.VMEM)
    grid_spec = pltpu.PrefetchScalarGridSpec(
        num_scalar_prefetch=3, grid=(),
        in_specs=[vmem] + [any_spec] * 4 + [vmem],
        out_specs=[vmem] * 4,
        scratch_shapes=[
            pltpu.VMEM((n_rows, w_pred.shape[0]), BF16),
            pltpu.VMEM(w_enc.shape, BF16),
            pltpu.VMEM(w_pred.shape, BF16),
            pltpu.VMEM(w_out_t.shape, BF16),
            pltpu.VMEM((joint, vocab_pad), BF16),
            pltpu.VMEM((vocab_pad, joint), BF16),
            pltpu.VMEM((enc_all.shape[0] * enc_all.shape[1] + 8, joint), F32),
            pltpu.VMEM((n_rows + CHUNK, joint), BF16),
            pltpu.VMEM((n_rows + CHUNK, LANES), jnp.int32),
            pltpu.VMEM((n_utt, LANES), F32),
            pltpu.VMEM((max_rows, joint), BF16),
            pltpu.VMEM((max_rows, vocab_pad), F32),
            pltpu.VMEM((max_rows, LANES), F32),
            pltpu.VMEM((n_utt * skew_rows + CHUNK * (n_frames + 1), LANES), F32),
            pltpu.VMEM(((n_frames + n_pos) * n_frames, LANES), F32),
            pltpu.VMEM(((n_frames + n_pos) * n_frames, LANES), F32),
            pltpu.VMEM(((n_frames + n_pos) * n_frames, LANES), F32),
            pltpu.VMEM((skew_rows, LANES), F32),
            pltpu.VMEM((skew_rows, LANES), F32),
            pltpu.VMEM((skew_rows, LANES), F32),
            pltpu.VMEM((skew_rows + CHUNK * (n_frames + 1), LANES), F32),
            pltpu.VMEM((TILE, vocab_pad), BF16),
            pltpu.VMEM((TILE, vocab_pad), BF16),
            pltpu.VMEM((TILE, max(joint, vocab_pad)), F32),
            pltpu.VMEM((TILE, max(joint, vocab_pad)), F32),
            pltpu.VMEM((vocab_pad, joint), F32),
            pltpu.VMEM((n_rows + CHUNK, joint), F32),
            pltpu.VMEM((n_af * 8 + 8, joint), F32),
            pltpu.SMEM((n_chunks,), jnp.int32),
            pltpu.SMEM((n_chunks,), jnp.int32),
            pltpu.SMEM((n_chunks,), jnp.int32),
            pltpu.SMEM((n_chunks,), jnp.int32),
            pltpu.SMEM((n_chunks,), jnp.int32),
            pltpu.SMEM((n_chunks,), jnp.int32),
            pltpu.SMEM((n_utt,), jnp.int32),
            pltpu.SemaphoreType.DMA((3 + n_utt,)),
        ])
    return pl.pallas_call(
        functools.partial(local_kernel, n_utt, n_frames, n_loc, n_pos, vocab),
        grid_spec=grid_spec,
        out_shape=[
            pltpu.VMEM((8, LANES), F32),
            pltpu.VMEM((n_af, joint), BF16),
            pltpu.VMEM((w_pred.shape[0], joint), F32),
            pltpu.VMEM((vocab_pad, joint), F32),
        ],
        compiler_params=pltpu.CompilerParams(vmem_limit_bytes=56 << 20),
        cost_estimate=pl.CostEstimate(flops=6 * max_rows * joint * vocab_pad, bytes_accessed=4 * max_rows * joint, transcendentals=2 * max_rows * joint),
        name="rnnt_local",
    )(seq_idx, frame_len, label_len, enc_all, pred_out, w_enc, w_pred, w_out_t, labels)


def greet(seq_size, me):
    barrier = pltpu.get_barrier_semaphore()
    for j in range(1, seq_size):
        pl.semaphore_signal(barrier, inc=1, device_id={'seq': lax.rem(me + j, seq_size)}, device_id_type=pl.DeviceIdType.MESH)
    pl.semaphore_wait(barrier, seq_size - 1)


class Ring:
    def __init__(self, seq_size):
        self.me = lax.axis_index('seq')
        self.n_chip = seq_size // 2
        self.chip, self.core = lax.div(self.me, 2), lax.rem(self.me, 2)
        self.sibling = self.chip * 2 + 1 - self.core
        self.nexts = (self.behind(1, 1) * 2 + self.core, self.behind(0, 1) * 2 + self.core)
        self.copies = []

    def behind(self, way, hops):
        return lax.rem(self.chip + self.n_chip - hops, self.n_chip) if way == 0 else lax.rem(self.chip + hops, self.n_chip)

    def send(self, src, dst, sems, idx, peer):
        copy = pltpu.make_async_remote_copy(src_ref=src, dst_ref=dst, send_sem=sems[0].at[idx], recv_sem=sems[1].at[idx],
                                            device_id={'seq': peer}, device_id_type=pl.DeviceIdType.MESH)
        copy.start()
        self.copies.append(copy)
        return copy


def gather_stages(ring, blocks, ring_sems, sib_sems):
    rows = blocks.shape[1] // 2
    relays = []

    def relay(dev, r, idx):
        relays.append(ring.send(blocks.at[dev, r, :], blocks.at[dev, r, :], sib_sems, idx, ring.sibling))

    hop1 = {}
    for part in range(2):
        for way in range(2):
            r = pl.ds((way if part == 0 else 1 - way) * rows, rows)
            hop1[way, part] = ring.send(blocks.at[ring.me, r, :], blocks.at[ring.me, r, :], ring_sems, (way, part), ring.nexts[way])
    relay(ring.me, pl.ds(0, 2 * rows), 0)
    yield
    hop2 = {}
    for way in range(2):
        r = pl.ds(way * rows, rows)
        dev = ring.behind(way, 1) * 2 + ring.core
        hop1[way, 0].wait_recv()
        hop2[way] = ring.send(blocks.at[dev, r, :], blocks.at[dev, r, :], ring_sems, (way, 2), ring.nexts[way])
        relay(dev, r, 1 + way)
    yield
    for way in range(2):
        hop1[way, 1].wait_recv()
        relay(ring.behind(way, 1) * 2 + ring.core, pl.ds((1 - way) * rows, rows), 3 + way)
    yield
    for way in range(2):
        hop2[way].wait_recv()
        relay(ring.behind(way, 2) * 2 + ring.core, pl.ds(way * rows, rows), 5 + way)
    yield
    for copy in relays:
        copy.wait_recv()
    yield


def spread_kernel(seq_size, enc_ref, out_ref, a_send, a_recv, s_send, s_recv):
    ring = Ring(seq_size)
    out_ref[pl.ds(ring.me, 1)] = enc_ref[...].reshape((1,) + out_ref.shape[1:])
    greet(seq_size, ring.me)
    for _ in gather_stages(ring, out_ref, (a_send, a_recv), (s_send, s_recv)):
        pass
    for copy in ring.copies:
        copy.wait_send()


def spread_frames(enc, seq_size):
    n_all, n_loc, enc_dim = enc.shape
    vmem = pl.BlockSpec(memory_space=pltpu.VMEM)
    dma = pltpu.SemaphoreType.DMA
    return pl.pallas_call(
        functools.partial(spread_kernel, seq_size),
        out_shape=pltpu.VMEM((seq_size, n_all * n_loc, enc_dim), enc.dtype),
        in_specs=[vmem], out_specs=vmem,
        scratch_shapes=[dma((2, 3))] * 2 + [dma((7,))] * 2,
        compiler_params=pltpu.CompilerParams(collective_id=0, has_side_effects=True, vmem_limit_bytes=24 << 20),
        name="spread_frames",
    )(enc)


def reduce_kernel(seq_size, n_mat, n_sub, da_ref, loss_ref, *refs):
    gw = refs[:n_mat]
    da_all, loss_out = refs[n_mat:n_mat + 2]
    out = refs[n_mat + 2:2 * n_mat + 2]
    rest = refs[2 * n_mat + 2:]
    sib_buf, own, ring_buf = rest[:n_mat], rest[n_mat:2 * n_mat], rest[2 * n_mat:3 * n_mat]
    (sib_send, sib_recv, rs_send, rs_recv, ag_send, ag_recv, dd_send, dd_recv,
     da_send, da_recv, ds_send, ds_recv, lo_send, lo_recv) = rest[3 * n_mat:]
    ring = Ring(seq_size)
    me, n_chip, core = ring.me, ring.n_chip, ring.core
    half = gw[0].shape[0] // 2
    chunk = half // n_chip
    piece = chunk // 2
    sub = piece // n_sub
    streams = [(m, q) for m in range(n_mat) for q in range(n_sub)]

    def at(way, hops, q):
        return pl.multiple_of((ring.behind(way, hops) * 2 + way) * piece + q * sub, sub)

    def mine(m, row, size):
        return gw[m].at[pl.ds(pl.multiple_of(core * half + row, size), size), :]

    da_all[pl.ds(me, 1)] = da_ref[...][None]
    loss_out[pl.ds(me, 1)] = loss_ref[...][None]
    greet(seq_size, me)
    da_gather = gather_stages(ring, da_all, (da_send, da_recv), (ds_send, ds_recv))
    next(da_gather)
    order = [ring.behind(0, 1), ring.behind(1, 1), ring.behind(0, 2), ring.chip]
    sib = {}
    for m in range(n_mat):
        for n, c in enumerate(order):
            row = pl.multiple_of(c * chunk, chunk)
            src = gw[m].at[pl.ds(pl.multiple_of((1 - core) * half + row, chunk), chunk), :]
            sib[m, n] = ring.send(src, sib_buf[m].at[pl.ds(row, chunk), :], (sib_send, sib_recv), (m, n), ring.sibling)
    small = [ring.send(loss_ref, loss_out.at[me], (lo_send, lo_recv), j - 1, lax.rem(me + j, seq_size)) for j in range(1, seq_size)]

    def combine(m, n):
        rows = pl.ds(pl.multiple_of(order[n] * chunk, chunk), chunk)
        sib[m, n].wait_recv()
        own[m][rows, :] = mine(m, order[n] * chunk, chunk)[...] + sib_buf[m][rows, :]

    rs = {}
    for m in range(n_mat):
        for way in range(2):
            combine(m, way)
            for q in range(n_sub):
                rs[m, q, way, 0] = ring.send(own[m].at[pl.ds(at(way, 1, q), sub), :], ring_buf[m].at[way, 0, pl.ds(q * sub, sub), :],
                                             (rs_send, rs_recv), (m, q, way, 0), ring.nexts[way])
    next(da_gather)
    for m in range(n_mat):
        combine(m, 2)
        combine(m, 3)
    next(da_gather)

    for s in range(1, n_chip - 1):
        for m, q in streams:
            for way in range(2):
                rows = pl.ds(q * sub, sub)
                rs[m, q, way, s - 1].wait_recv()
                ring_buf[m][way, s - 1, rows, :] = ring_buf[m][way, s - 1, rows, :] + own[m][pl.ds(at(way, s + 1, q), sub), :]
                rs[m, q, way, s] = ring.send(ring_buf[m].at[way, s - 1, rows, :], ring_buf[m].at[way, s, rows, :],
                                             (rs_send, rs_recv), (m, q, way, s), ring.nexts[way])
    next(da_gather)

    def place(way, hops, q):
        return pl.ds(pl.multiple_of(core * half + at(way, hops, q), sub), sub)

    last = n_chip - 2
    ag, relays = {}, []
    for m, q in streams:
        for way in range(2):
            rs[m, q, way, last].wait_recv()
            here = place(way, 0, q)
            out[m][here, :] = ring_buf[m][way, last, pl.ds(q * sub, sub), :] + own[m][pl.ds(at(way, 0, q), sub), :]
            ag[m, q, way, 0] = ring.send(out[m].at[here, :], out[m].at[here, :], (ag_send, ag_recv), (m, q, way, 0), ring.nexts[way])
            relays.append(ring.send(out[m].at[here, :], out[m].at[here, :], (dd_send, dd_recv), (m, q, way, 0), ring.sibling))
    for s in range(1, n_chip):
        for m, q in streams:
            for way in range(2):
                ag[m, q, way, s - 1].wait_recv()
                here = place(way, s, q)
                if s < n_chip - 1:
                    ag[m, q, way, s] = ring.send(out[m].at[here, :], out[m].at[here, :], (ag_send, ag_recv), (m, q, way, s), ring.nexts[way])
                relays.append(ring.send(out[m].at[here, :], out[m].at[here, :], (dd_send, dd_recv), (m, q, way, s), ring.sibling))
    next(da_gather)
    for copy in relays + small:
        copy.wait_recv()
    for copy in ring.copies:
        copy.wait_send()


def reduce_all(da, loss, grads, seq_size, n_sub=2):
    n_mat = len(grads)
    n_chip = seq_size // 2
    half = grads[0].shape[0] // 2
    piece = half // (2 * n_chip)
    vmem = pl.BlockSpec(memory_space=pltpu.VMEM)
    dma = pltpu.SemaphoreType.DMA
    steps = n_chip - 1
    return pl.pallas_call(
        functools.partial(reduce_kernel, seq_size, n_mat, n_sub),
        out_shape=[jax.ShapeDtypeStruct((seq_size,) + da.shape, da.dtype), jax.ShapeDtypeStruct((seq_size,) + loss.shape, F32)]
        + [jax.ShapeDtypeStruct(g.shape, F32) for g in grads],
        in_specs=[vmem] * (2 + n_mat), out_specs=[vmem] * (2 + n_mat),
        scratch_shapes=[pltpu.VMEM((half, g.shape[1]), F32) for g in grads] * 2
        + [pltpu.VMEM((2, steps, piece, g.shape[1]), F32) for g in grads]
        + [dma((n_mat, 4))] * 2 + [dma((n_mat, n_sub, 2, steps))] * 4 + [dma((n_mat, n_sub, 2, n_chip))] * 2
        + [dma((2, 3))] * 2 + [dma((7,))] * 2 + [dma((seq_size - 1,))] * 2,
        compiler_params=pltpu.CompilerParams(collective_id=1, has_side_effects=True, vmem_limit_bytes=24 << 20),
        name="reduce_all",
    )(da, loss, *grads)


def finish_kernel(seq_size, vocab, me_ref, da_all, loss_ref, gwp_ref, gwo_ref, we_ref, f_ref, loss_out, genc_out, gwe_out, gwp_out, gwo_out, d_all):
    me = me_ref[0]
    n_af, joint = da_all.shape[1:]
    rows = n_af // seq_size
    gwp_out[...] = gwp_ref[...]
    gwo_out[...] = gwo_ref[:vocab, :]
    loss_out[...] = jnp.sum(loss_ref[:, 0, :], axis=0, keepdims=True)[:, :loss_out.shape[1]]
    for i in range(seq_size):
        for src in range(seq_size):
            d_all[pl.ds(i * n_af + src * rows, rows), :] = da_all[src, pl.ds(i * rows, rows), :]
    here = d_all[pl.ds(pl.multiple_of(me * n_af, n_af), n_af), :]
    genc_out[...] = dot_nt(here, we_ref[...]).astype(BF16).reshape(genc_out.shape)
    gwe_out[...] = dot_tn(f_ref[...].reshape(seq_size * n_af, f_ref.shape[2]), d_all[...])


def finish(seq_idx, da_all, loss_all, gwp, gwo_t, w_enc, enc_all, vocab, n_loc):
    seq_size, n_af, joint = da_all.shape
    n_all = n_af // n_loc
    vmem = pl.BlockSpec(memory_space=pltpu.VMEM)
    return pl.pallas_call(
        functools.partial(finish_kernel, seq_size, vocab),
        grid_spec=pltpu.PrefetchScalarGridSpec(
            num_scalar_prefetch=1, grid=(), in_specs=[vmem] * 6, out_specs=[vmem] * 5,
            scratch_shapes=[pltpu.VMEM((seq_size * n_af, joint), BF16)]),
        out_shape=[
            jax.ShapeDtypeStruct((1, n_all), F32),
            jax.ShapeDtypeStruct((n_all, n_loc, enc_all.shape[2]), BF16),
            jax.ShapeDtypeStruct(w_enc.shape, F32),
            jax.ShapeDtypeStruct(gwp.shape, F32),
            jax.ShapeDtypeStruct((vocab, joint), F32),
        ],
        compiler_params=pltpu.CompilerParams(vmem_limit_bytes=24 << 20),
        name="finish",
    )(seq_idx, da_all, loss_all, gwp, gwo_t, w_enc, enc_all)


def solution(mesh):
    seq_size = mesh.shape['seq']

    def local_fn(enc_out, pred_out, w_enc, w_pred, w_out, labels, frame_len, label_len):
        seq_idx = jnp.reshape(lax.axis_index('seq'), (1,)).astype(jnp.int32)
        n_all, n_loc, _ = enc_out.shape
        n_utt = n_all // seq_size
        n_frames = n_loc * seq_size
        vocab = w_out.shape[1]
        enc_all = spread_frames(enc_out, seq_size)
        loss, da, *grads = local_grads(
            seq_idx, enc_all, pred_out.reshape(-1, pred_out.shape[2]), w_enc, w_pred, w_out.T,
            labels, frame_len, label_len, n_utt, n_frames, n_loc, vocab)
        da_all, loss_all, gwp, gwo_t = reduce_all(da, loss, grads, seq_size)
        loss, genc, gwe, gwp, gwo_t = finish(seq_idx, da_all, loss_all, gwp, gwo_t, w_enc, enc_all, vocab, n_loc)
        return loss.reshape(n_all), genc, gwe, gwp, gwo_t.T

    in_specs = (P('dp', 'seq', None), P('dp', None, None), P(None, None), P(None, None), P(None, None), P('dp', None), P('dp'), P('dp'))
    out_specs = (P('dp'), P('dp', 'seq', None), P('dp', None), P('dp', None), P('dp', None))
    return jax.shard_map(local_fn, mesh=mesh, in_specs=in_specs, out_specs=out_specs, check_vma=False)
```

```python
import functools

import jax
import jax.numpy as jnp
from jax import lax
from jax.experimental import pallas as pl
from jax.experimental.pallas import tpu as pltpu
from jax.sharding import PartitionSpec as P

NEG_FILL = -1.0e30
CHUNK = 16
LANES = 128
TILE_CHUNKS = 16
TILE = CHUNK * TILE_CHUNKS
SUBS = 2
BODY_CHUNKS = SUBS * TILE_CHUNKS
SAFE_LOGIT = 60.0
F32 = jnp.float32
BF16 = jnp.bfloat16


def logadd(x, y):
    return jnp.maximum(x, y) + jnp.log(1.0 + jnp.exp(-jnp.abs(x - y)))


def dot_nn(x, y):
    return jnp.dot(x, y, preferred_element_type=F32)


def dot_tn(x, y):
    return lax.dot_general(x, y, (((0,), (0,)), ((), ())), preferred_element_type=F32)


def dot_nt(x, y):
    return lax.dot_general(x, y, (((1,), (1,)), ((), ())), preferred_element_type=F32)


def placement(t_row, u_row, n_utt):
    n_all = t_row.shape[1]
    n_dev = n_all // n_utt
    work = (t_row * ((u_row + CHUNK) // CHUNK)).astype(F32)
    row = jnp.broadcast_to(work, (n_all, n_all))
    col = jnp.transpose(row)
    r_id = lax.broadcasted_iota(jnp.int32, (n_all, n_all), 1)
    c_id = lax.broadcasted_iota(jnp.int32, (n_all, n_all), 0)

    def key(rank):
        rank = rank.astype(jnp.int32)
        turn = rank // n_dev
        pos = rank % n_dev
        return jnp.where(turn % 2 == 0, pos, n_dev - 1 - pos) * n_utt + turn

    ahead = jnp.where((col > row) | ((col == row) & (c_id < r_id)), 1.0, 0.0)
    behind = jnp.where((row > col) | ((row == col) & (r_id < c_id)), 1.0, 0.0)
    return key(jnp.sum(ahead, axis=0, keepdims=True)), key(jnp.sum(behind, axis=1, keepdims=True))


def local_kernel(n_utt, n_frames, n_loc, n_pos, vocab,
                 seq_ref, tlen_ref, ulen_ref,
                 act_f, wt_v, wo_v, top_ref, pred_hbm, wpred_hbm, labels_ref, t_row, u_row,
                 loss_ref, da_ref, gwp_ref, gwo_ref,
                 g_v, wp_v, act_g, lab_v, lab_scr,
                 hid, ex, sums, skew, cb_s, cl_s, ce_s, al, xb_s, xl_s, occ, dz_0, dz_1, z_0, z_1,
                 acc_o, dc, da8, where, what, uid, sems):
    me = seq_ref[0]
    dz_v, z_v = (dz_0, dz_1), (z_0, z_1)
    n_diag = n_frames + n_pos - 1
    pitch = n_frames + 1
    skew_rows = (n_frames + n_pos) * pitch
    n_rows = n_utt * n_pos
    vocab_pad = wt_v.shape[0]
    n_grp = vocab_pad // LANES

    n_all = n_utt * (n_frames // n_loc)
    weight = pltpu.make_async_copy(wpred_hbm, wp_v, sems.at[n_utt])
    weight.start()
    key, _ = placement(t_row[...], u_row[...], n_utt)
    who = lax.broadcasted_iota(jnp.int32, key.shape, 1)
    copies = [weight]
    for b in range(n_utt):
        uid[b] = jnp.sum(jnp.where(key == me * n_utt + b, who, 0))
    uid[n_utt] = 0
    for b in range(n_utt):
        copies.append(pltpu.make_async_copy(
            pred_hbm.at[pl.ds(pl.multiple_of(uid[b] * n_pos, n_pos), n_pos), :], g_v.at[pl.ds(b * n_pos, n_pos), :], sems.at[b]))
        copies[-1].start()

    skew_bits = skew_rows.bit_length()
    lab_bits = n_rows.bit_length()
    da_bits = (n_utt * n_frames).bit_length()

    def add_utt(b, pos):
        t_len = tlen_ref[uid[b]]
        n_chunk = (ulen_ref[uid[b]] + CHUNK) // CHUNK
        one_b = (uid[b] * n_loc) << skew_bits
        two_b = b * n_pos + ((b * n_loc + (b << da_bits)) << lab_bits)

        def add_chunks(q, pos):
            one = one_b + q * (pitch * CHUNK)
            two = two_b + q * CHUNK
            for t in range(n_frames):
                hi, lo = divmod(t, n_loc)
                where[pos + t] = one + (((hi * n_all * n_loc + lo) << skew_bits) + (pitch + 1) * t)
                what[pos + t] = two + ((hi * n_utt * n_loc + lo) << lab_bits)
            return pos + t_len
        return lax.fori_loop(0, n_chunk, add_chunks, pos)

    n_chunks = lax.fori_loop(0, n_utt, add_utt, 0)
    n_tiles = (n_chunks + BODY_CHUNKS - 1) // BODY_CHUNKS
    for k in range(BODY_CHUNKS):
        where[n_chunks + k] = (n_all * n_frames) << skew_bits
        what[n_chunks + k] = n_rows + (n_utt << (lab_bits + da_bits))

    def low(x, bits):
        return x & ((1 << bits) - 1)

    def label_row(i):
        return pl.multiple_of(low(what[i], lab_bits), CHUNK)

    def grad_row(i):
        return pl.multiple_of(low(what[i] >> lab_bits, da_bits) * 8, 8)

    def slot(i):
        return what[i] >> (lab_bits + da_bits)

    def frame_row(i):
        return where[i] >> skew_bits

    def skew_row(i):
        return low(where[i], skew_bits)

    dc[...] = jnp.zeros_like(dc)
    da8[...] = jnp.zeros_like(da8)
    acc_o[...] = jnp.zeros_like(acc_o)
    act_g[pl.ds(n_rows, CHUNK), :] = jnp.zeros((CHUNK, act_g.shape[1]), BF16)
    lab_v[pl.ds(n_rows, CHUNK), :] = jnp.full((CHUNK, LANES), -1, jnp.int32)

    lab_scr[...] = jnp.full_like(lab_scr, -1.0)
    for b in range(n_utt):
        lab_scr[b:b + 1, :n_pos - 1] = labels_ref[pl.ds(uid[b], 1), :].astype(F32)
    lab_t = jnp.transpose(lab_scr[...])
    for b in range(n_utt):
        lab_v[pl.ds(b * n_pos, n_pos), :] = jnp.broadcast_to(lab_t[:n_pos, b:b + 1], (n_pos, LANES)).astype(jnp.int32)

    for cp in copies:
        cp.wait()
    act_g[pl.ds(0, n_rows), :] = dot_nn(g_v[...], wp_v[...]).astype(BF16)

    lane = lax.broadcasted_iota(jnp.int32, (CHUNK, LANES), 1)
    left = lane < LANES // 2
    last_ok = lane < vocab - (n_grp - 1) * LANES

    def fwd_body(shifted, i, carry):
        r0 = pl.multiple_of(i * (SUBS * TILE), SUBS * TILE)
        c0 = i * BODY_CHUNKS
        for k in range(BODY_CHUNKS):
            pre = act_g[pl.ds(label_row(c0 + k), CHUNK), :].astype(F32) + act_f[pl.ds(frame_row(c0 + k), 1), :]
            hid[pl.ds(r0 + k * CHUNK, CHUNK), :] = jnp.tanh(pre).astype(BF16)
        for sub in range(SUBS):
            z_v[sub][...] = dot_nn(hid[pl.ds(r0 + sub * TILE, TILE), :], wo_v[...])
        for k in range(BODY_CHUNKS):
            z_ref = z_v[k // TILE_CHUNKS]
            rows = pl.ds(r0 + k * CHUNK, CHUNK)
            z_rows = pl.ds(k % TILE_CHUNKS * CHUNK, CHUNK)
            ids = lab_v[pl.ds(label_row(c0 + k), CHUNK), :]
            sb = slot(c0 + k) * skew_rows + skew_row(c0 + k)
            zs = [z_ref[z_rows, j * LANES:(j + 1) * LANES] for j in range(n_grp)]
            picked = functools.reduce(jnp.add, [jnp.where(lane + j * LANES == ids, zs[j], 0.0) for j in range(n_grp)])
            picked = jnp.sum(picked, axis=1, keepdims=True)
            if shifted:
                top = functools.reduce(jnp.maximum, zs[:-1] + [jnp.where(last_ok, zs[-1], NEG_FILL)])
                top = jnp.max(top, axis=1, keepdims=True)
                es = [jnp.exp(z - top) for z in zs]
            else:
                es = [jnp.exp(z) for z in zs]
            es[-1] = jnp.where(last_ok, es[-1], 0.0)
            for j in range(n_grp):
                ex[rows, j * LANES:(j + 1) * LANES] = es[j]
            tot = jnp.sum(functools.reduce(jnp.add, es), axis=1, keepdims=True)
            tot_b = jnp.broadcast_to(tot, (CHUNK, LANES))
            sums[rows, :] = tot_b
            log_norm = jnp.log(tot_b)
            if shifted:
                log_norm = log_norm + top
            skew[pl.ds(sb, CHUNK, stride=pitch), :] = jnp.where(left, zs[0][:, 0:1], picked) - log_norm
        return carry

    bound = jnp.max(top_ref[...])

    @pl.when(bound < SAFE_LOGIT)
    def _():
        lax.fori_loop(0, n_tiles, functools.partial(fwd_body, False), 0)

    @pl.when(jnp.logical_not(bound < SAFE_LOGIT))
    def _():
        lax.fori_loop(0, n_tiles, functools.partial(fwd_body, True), 0)

    lane_s = lax.broadcasted_iota(jnp.int32, (n_frames, LANES), 1)
    sub_s = lax.broadcasted_iota(jnp.int32, (n_frames, LANES), 0)
    t_lens = jnp.zeros((n_frames, LANES), jnp.int32)
    u_lens = jnp.zeros((n_frames, LANES), jnp.int32)
    for b in range(n_utt):
        t_lens = jnp.where(lane_s == b, tlen_ref[uid[b]], t_lens)
        u_lens = jnp.where(lane_s == b, ulen_ref[uid[b]], u_lens)
    slot_s = lane_s % (LANES // 2)
    live_t = sub_s < t_lens
    last_t = sub_s == t_lens - 1

    def merge_diag(d):
        base = d * pitch
        both = skew[pl.ds(base, n_frames), :]
        for b in range(1, n_utt):
            both = jnp.where(slot_s == b, skew[pl.ds(base + b * skew_rows, n_frames), :], both)
        bl = both
        lb = pltpu.roll(both, LANES // 2, 1)
        u = d - sub_s
        live = live_t & (u >= 0)
        here = pl.ds(pl.multiple_of(d * n_frames, n_frames), n_frames)
        cb_s[here, :] = jnp.where(live & (u <= u_lens), bl, NEG_FILL)
        cl_s[here, :] = jnp.where(live & (u < u_lens), lb, NEG_FILL)
        ce_s[here, :] = jnp.where(last_t & (u == u_lens), 1.0, 0.0)

    def merge_step(i, carry):
        for k in range(16):
            merge_diag(i * 16 + k)
        return carry
    lax.fori_loop(0, (n_frames + n_pos) // 16, merge_step, 0)

    def lattice_step(i, carry):
        a, be = carry
        fwd = pl.ds(pl.multiple_of(i * n_frames, n_frames), n_frames)
        bwd = pl.ds(pl.multiple_of((n_diag - 1 - i) * n_frames, n_frames), n_frames)
        back = (n_diag - 1 - i) * pitch
        al[pl.ds(i * pitch, n_frames), :] = a
        moved = jnp.where(sub_s == 0, NEG_FILL, pltpu.roll(a + cb_s[fwd, :], 1, 0))
        a = logadd(moved, a + cl_s[fwd, :])
        up = jnp.where(sub_s == n_frames - 1, NEG_FILL, pltpu.roll(be, n_frames - 1, 0))
        bl = cb_s[bwd, :]
        x_b = jnp.where(ce_s[bwd, :] > 0.0, bl, up + bl)
        x_l = be + cl_s[bwd, :]
        xb_s[pl.ds(back, n_frames), :] = x_b
        xl_s[pl.ds(back, n_frames), :] = x_l
        return a, logadd(x_b, x_l)

    def lattice_pair(i, carry):
        return lattice_step(2 * i + 1, lattice_step(2 * i, carry))

    neg = jnp.full((n_frames, LANES), NEG_FILL, F32)
    state = lax.fori_loop(0, n_diag // 2, lattice_pair, (jnp.where(sub_s == 0, 0.0, neg), neg))
    for i in range(n_diag // 2 * 2, n_diag):
        state = lattice_step(i, state)
    be0 = state[1]
    log_prob = jnp.where(t_lens[0:1, :] > 0, be0[0:1, :], 0.0)
    lane_8 = lax.broadcasted_iota(jnp.int32, loss_ref.shape, 1)
    loss_ref[...] = functools.reduce(jnp.add, [
        jnp.where(lane_8 == uid[b], -log_prob[:, b:b + 1], 0.0) for b in range(n_utt)])

    n_live = n_diag * pitch
    n_blk = CHUNK
    left_8 = left
    for r in range(0, pl.cdiv(n_live, n_blk) * n_blk, n_blk):
        rows = pl.ds(r, n_blk)
        a = al[rows, :] - log_prob
        x = jnp.where(left_8, a + xb_s[rows, :], pltpu.roll(a + xl_s[rows, :], LANES // 2, 1))
        occ[rows, :] = jnp.exp(jnp.minimum(x, 0.0))

    def bwd_tile(i, carry):
        r0 = pl.multiple_of(i * (SUBS * TILE), SUBS * TILE)
        c0 = i * BODY_CHUNKS
        for sub in range(SUBS):
            for kk in range(TILE_CHUNKS):
                k = sub * TILE_CHUNKS + kk
                rows = pl.ds(r0 + k * CHUNK, CHUNK)
                both = occ[pl.ds(skew_row(c0 + k), CHUNK, stride=pitch), :]
                ids = lab_v[pl.ds(label_row(c0 + k), CHUNK), :]
                b = slot(c0 + k)
                ob = jnp.sum(jnp.where(lane == b, both, 0.0), axis=1, keepdims=True)
                ol = jnp.sum(jnp.where(lane == b + LANES // 2, both, 0.0), axis=1, keepdims=True)
                scale = (ob + ol) / sums[rows, :]
                for j in range(n_grp):
                    dz = ex[rows, j * LANES:(j + 1) * LANES] * scale
                    if j == 0:
                        dz = dz - jnp.where(lane == 0, ob, 0.0)
                    dz = dz - jnp.where(lane + j * LANES == ids, ol, 0.0)
                    dz_v[sub][kk * CHUNK:(kk + 1) * CHUNK, j * LANES:(j + 1) * LANES] = dz.astype(BF16)
        for sub in range(SUBS):
            z_v[sub][...] = dot_nn(dz_v[sub][...], wt_v[...])
        for sub in range(SUBS):
            for kk in range(TILE_CHUNKS):
                k = sub * TILE_CHUNKS + kk
                lr, ar = label_row(c0 + k), grad_row(c0 + k)
                h = hid[pl.ds(r0 + k * CHUNK, CHUNK), :].astype(F32)
                dp = (z_v[sub][kk * CHUNK:(kk + 1) * CHUNK, :] * (1.0 - h * h)).astype(BF16).astype(F32)
                dc[pl.ds(lr, CHUNK), :] += dp
                da8[pl.ds(ar, 8), :] += dp[:8, :] + dp[8:, :]
        dz_all = jnp.concatenate([dz_v[sub][...] for sub in range(SUBS)], axis=0)
        acc_o[...] += dot_tn(dz_all, hid[pl.ds(r0, SUBS * TILE), :])
        return carry
    lax.fori_loop(0, n_tiles, bwd_tile, 0)

    n_af = n_utt * n_frames
    d_act_f = jnp.sum(da8[pl.ds(0, n_af * 8), :].reshape(n_af, 8, da8.shape[1]), axis=1).astype(BF16)
    da_ref[...] = d_act_f
    gwo_ref[...] = acc_o[...]
    gwp_ref[...] = dot_tn(g_v[...], dc[pl.ds(0, n_rows), :].astype(BF16))


def local_grads(seq_idx, act_f, w_t, w_o, top, pred_out, w_pred, labels, frame_len, label_len, n_utt, n_frames, n_loc, vocab):
    n_pos = labels.shape[1] + 1
    vocab_pad, joint = w_t.shape
    n_rows = n_utt * n_pos
    n_af = n_utt * n_frames
    max_rows = n_utt * n_frames * n_pos
    skew_rows = (n_frames + n_pos) * (n_frames + 1)
    n_chunks = max_rows // CHUNK + BODY_CHUNKS
    any_spec = pl.BlockSpec(memory_space=pl.ANY)
    vmem = pl.BlockSpec(memory_space=pltpu.VMEM)
    grid_spec = pltpu.PrefetchScalarGridSpec(
        num_scalar_prefetch=3, grid=(),
        in_specs=[vmem] * 4 + [any_spec] * 2 + [vmem] * 3,
        out_specs=[vmem] * 4,
        scratch_shapes=[
            pltpu.VMEM((n_rows, w_pred.shape[0]), BF16),
            pltpu.VMEM(w_pred.shape, BF16),
            pltpu.VMEM((n_rows + CHUNK, joint), BF16),
            pltpu.VMEM((n_rows + CHUNK, LANES), jnp.int32),
            pltpu.VMEM((n_utt, LANES), F32),
            pltpu.VMEM((max_rows, joint), BF16),
            pltpu.VMEM((max_rows, vocab_pad), F32),
            pltpu.VMEM((max_rows, LANES), F32),
            pltpu.VMEM((n_utt * skew_rows + CHUNK * (n_frames + 1), LANES), F32),
            pltpu.VMEM(((n_frames + n_pos) * n_frames, LANES), F32),
            pltpu.VMEM(((n_frames + n_pos) * n_frames, LANES), F32),
            pltpu.VMEM(((n_frames + n_pos) * n_frames, LANES), F32),
            pltpu.VMEM((skew_rows, LANES), F32),
            pltpu.VMEM((skew_rows, LANES), F32),
            pltpu.VMEM((skew_rows, LANES), F32),
            pltpu.VMEM((skew_rows, LANES), F32),
            pltpu.VMEM((TILE, vocab_pad), BF16),
            pltpu.VMEM((TILE, vocab_pad), BF16),
            pltpu.VMEM((TILE, max(joint, vocab_pad)), F32),
            pltpu.VMEM((TILE, max(joint, vocab_pad)), F32),
            pltpu.VMEM((vocab_pad, joint), F32),
            pltpu.VMEM((n_rows + CHUNK, joint), F32),
            pltpu.VMEM((n_af * 8 + 8, joint), F32),
            pltpu.SMEM((n_chunks + n_frames,), jnp.int32),
            pltpu.SMEM((n_chunks + n_frames,), jnp.int32),
            pltpu.SMEM((n_utt + 1,), jnp.int32),
            pltpu.SemaphoreType.DMA((n_utt + 1,)),
        ])
    return pl.pallas_call(
        functools.partial(local_kernel, n_utt, n_frames, n_loc, n_pos, vocab),
        grid_spec=grid_spec,
        out_shape=[
            pltpu.VMEM((8, LANES), F32),
            pltpu.VMEM((n_af, joint), BF16),
            pltpu.VMEM((w_pred.shape[0], joint), F32),
            pltpu.VMEM((vocab_pad, joint), F32),
        ],
        compiler_params=pltpu.CompilerParams(vmem_limit_bytes=54 << 20),
        cost_estimate=pl.CostEstimate(flops=6 * max_rows * joint * vocab_pad, bytes_accessed=4 * max_rows * joint, transcendentals=2 * max_rows * joint),
        name="rnnt_local",
    )(seq_idx, frame_len, label_len, act_f, w_t, w_o, top, pred_out, w_pred, labels, frame_len[None], label_len[None])


def greet(seq_size, me):
    barrier = pltpu.get_barrier_semaphore()
    for j in range(1, seq_size):
        pl.semaphore_signal(barrier, inc=1, device_id={'seq': lax.rem(me + j, seq_size)}, device_id_type=pl.DeviceIdType.MESH)
    pl.semaphore_wait(barrier, seq_size - 1)


class Ring:
    def __init__(self, seq_size):
        self.me = lax.axis_index('seq')
        self.n_chip = seq_size // 2
        self.chip, self.core = lax.div(self.me, 2), lax.rem(self.me, 2)
        self.sibling = self.chip * 2 + 1 - self.core
        self.nexts = (self.behind(1, 1) * 2 + self.core, self.behind(0, 1) * 2 + self.core)
        self.copies = []

    def behind(self, way, hops):
        return lax.rem(self.chip + self.n_chip - hops, self.n_chip) if way == 0 else lax.rem(self.chip + hops, self.n_chip)

    def send(self, src, dst, sems, idx, peer):
        copy = pltpu.make_async_remote_copy(src_ref=src, dst_ref=dst, send_sem=sems[0].at[idx], recv_sem=sems[1].at[idx],
                                            device_id={'seq': peer}, device_id_type=pl.DeviceIdType.MESH)
        copy.start()
        self.copies.append(copy)
        return copy


def gather_stages(ring, blocks, ring_sems, sib_sems):
    rows = blocks.shape[1] // 2
    relays = []

    def relay(dev, r, idx):
        relays.append(ring.send(blocks.at[dev, r, :], blocks.at[dev, r, :], sib_sems, idx, ring.sibling))

    hop1 = {}
    for part in range(2):
        for way in range(2):
            r = pl.ds((way if part == 0 else 1 - way) * rows, rows)
            hop1[way, part] = ring.send(blocks.at[ring.me, r, :], blocks.at[ring.me, r, :], ring_sems, (way, part), ring.nexts[way])
    relay(ring.me, pl.ds(0, 2 * rows), 0)
    yield
    hop2 = {}
    for way in range(2):
        r = pl.ds(way * rows, rows)
        dev = ring.behind(way, 1) * 2 + ring.core
        hop1[way, 0].wait_recv()
        hop2[way] = ring.send(blocks.at[dev, r, :], blocks.at[dev, r, :], ring_sems, (way, 2), ring.nexts[way])
        relay(dev, r, 1 + way)
    yield
    for way in range(2):
        hop1[way, 1].wait_recv()
        relay(ring.behind(way, 1) * 2 + ring.core, pl.ds((1 - way) * rows, rows), 3 + way)
    yield
    for way in range(2):
        hop2[way].wait_recv()
        relay(ring.behind(way, 2) * 2 + ring.core, pl.ds(way * rows, rows), 5 + way)
    yield
    for copy in relays:
        copy.wait_recv()
    yield


def spread_kernel(seq_size, vocab, enc_ref, we_ref, wt_ref, out_ref, act_ref, wt_out, wo_out, top_out, a_send, a_recv, s_send, s_recv):
    ring = Ring(seq_size)
    rows = out_ref.shape[1]
    out_ref[pl.ds(ring.me, 1)] = enc_ref[...].reshape((1,) + out_ref.shape[1:])

    def prepare():
        wt_out[vocab:, :] = jnp.zeros((wt_out.shape[0] - vocab, wt_out.shape[1]), BF16)
        wt_out[:vocab, :] = wt_ref[...]
        wo_out[...] = jnp.transpose(wt_out[...])
        top = jnp.max(jnp.sum(jnp.abs(wo_out[...].astype(F32)), axis=0, keepdims=True), axis=1, keepdims=True)
        top_out[...] = jnp.broadcast_to(top, top_out.shape)
        act_ref[seq_size * rows:, :] = jnp.zeros((8, act_ref.shape[1]), F32)

    def project(dev):
        act_ref[pl.ds(pl.multiple_of(dev * rows, rows), rows), :] = dot_nn(out_ref[dev], we_ref[...]).astype(BF16).astype(F32)

    greet(seq_size, ring.me)
    stages = gather_stages(ring, out_ref, (a_send, a_recv), (s_send, s_recv))
    next(stages)
    prepare()
    for _ in stages:
        pass
    for dev in range(seq_size):
        project(dev)
    for copy in ring.copies:
        copy.wait_send()


def spread_frames(enc, w_enc, w_out_t, seq_size):
    n_all, n_loc, enc_dim = enc.shape
    vocab, joint = w_out_t.shape
    vocab_pad = pl.cdiv(vocab, LANES) * LANES
    vmem = pl.BlockSpec(memory_space=pltpu.VMEM)
    dma = pltpu.SemaphoreType.DMA
    return pl.pallas_call(
        functools.partial(spread_kernel, seq_size, vocab),
        out_shape=[pltpu.VMEM((seq_size, n_all * n_loc, enc_dim), enc.dtype),
                   pltpu.VMEM((seq_size * n_all * n_loc + 8, joint), F32),
                   pltpu.VMEM((vocab_pad, joint), BF16),
                   pltpu.VMEM((joint, vocab_pad), BF16),
                   pltpu.VMEM((8, LANES), F32)],
        in_specs=[vmem] * 3, out_specs=[vmem] * 5,
        scratch_shapes=[dma((2, 3))] * 2 + [dma((7,))] * 2,
        compiler_params=pltpu.CompilerParams(collective_id=0, has_side_effects=True, vmem_limit_bytes=24 << 20),
        name="spread_frames",
    )(enc, w_enc, w_out_t)


def reduce_kernel(seq_size, n_mat, n_sub, da_ref, loss_ref, *refs):
    gw = refs[:n_mat]
    da_all, loss_out = refs[n_mat:n_mat + 2]
    out = refs[n_mat + 2:2 * n_mat + 2]
    rest = refs[2 * n_mat + 2:]
    sib_buf, own, ring_buf = rest[:n_mat], rest[n_mat:2 * n_mat], rest[2 * n_mat:3 * n_mat]
    (sib_send, sib_recv, rs_send, rs_recv, ag_send, ag_recv, dd_send, dd_recv,
     da_send, da_recv, ds_send, ds_recv, lo_send, lo_recv) = rest[3 * n_mat:]
    ring = Ring(seq_size)
    me, n_chip, core = ring.me, ring.n_chip, ring.core
    half = gw[0].shape[0] // 2
    chunk = half // n_chip
    piece = chunk // 2
    sub = piece // n_sub
    streams = [(m, q) for m in range(n_mat) for q in range(n_sub)]

    def at(way, hops, q):
        return pl.multiple_of((ring.behind(way, hops) * 2 + way) * piece + q * sub, sub)

    def mine(m, row, size):
        return gw[m].at[pl.ds(pl.multiple_of(core * half + row, size), size), :]

    da_all[pl.ds(me, 1)] = da_ref[...][None]
    loss_out[pl.ds(me, 1)] = loss_ref[...][None]
    greet(seq_size, me)
    da_gather = gather_stages(ring, da_all, (da_send, da_recv), (ds_send, ds_recv))
    next(da_gather)
    order = [ring.behind(0, 1), ring.behind(1, 1), ring.behind(0, 2), ring.chip]
    sib = {}
    for m in range(n_mat):
        for n, c in enumerate(order):
            row = pl.multiple_of(c * chunk, chunk)
            src = gw[m].at[pl.ds(pl.multiple_of((1 - core) * half + row, chunk), chunk), :]
            sib[m, n] = ring.send(src, sib_buf[m].at[pl.ds(row, chunk), :], (sib_send, sib_recv), (m, n), ring.sibling)
    small = [ring.send(loss_ref, loss_out.at[me], (lo_send, lo_recv), j - 1, lax.rem(me + j, seq_size)) for j in range(1, seq_size)]

    def combine(m, n):
        rows = pl.ds(pl.multiple_of(order[n] * chunk, chunk), chunk)
        sib[m, n].wait_recv()
        own[m][rows, :] = mine(m, order[n] * chunk, chunk)[...] + sib_buf[m][rows, :]

    rs = {}
    for m in range(n_mat):
        for way in range(2):
            combine(m, way)
            for q in range(n_sub):
                rs[m, q, way, 0] = ring.send(own[m].at[pl.ds(at(way, 1, q), sub), :], ring_buf[m].at[way, 0, pl.ds(q * sub, sub), :],
                                             (rs_send, rs_recv), (m, q, way, 0), ring.nexts[way])
    next(da_gather)
    for m in range(n_mat):
        combine(m, 2)
        combine(m, 3)
    next(da_gather)

    for s in range(1, n_chip - 1):
        for m, q in streams:
            for way in range(2):
                rows = pl.ds(q * sub, sub)
                rs[m, q, way, s - 1].wait_recv()
                ring_buf[m][way, s - 1, rows, :] = ring_buf[m][way, s - 1, rows, :] + own[m][pl.ds(at(way, s + 1, q), sub), :]
                rs[m, q, way, s] = ring.send(ring_buf[m].at[way, s - 1, rows, :], ring_buf[m].at[way, s, rows, :],
                                             (rs_send, rs_recv), (m, q, way, s), ring.nexts[way])
    next(da_gather)

    def place(way, hops, q):
        return pl.ds(pl.multiple_of(core * half + at(way, hops, q), sub), sub)

    last = n_chip - 2
    ag, relays = {}, []
    for m, q in streams:
        for way in range(2):
            rs[m, q, way, last].wait_recv()
            here = place(way, 0, q)
            out[m][here, :] = ring_buf[m][way, last, pl.ds(q * sub, sub), :] + own[m][pl.ds(at(way, 0, q), sub), :]
            ag[m, q, way, 0] = ring.send(out[m].at[here, :], out[m].at[here, :], (ag_send, ag_recv), (m, q, way, 0), ring.nexts[way])
            relays.append(ring.send(out[m].at[here, :], out[m].at[here, :], (dd_send, dd_recv), (m, q, way, 0), ring.sibling))
    for s in range(1, n_chip):
        for m, q in streams:
            for way in range(2):
                ag[m, q, way, s - 1].wait_recv()
                here = place(way, s, q)
                if s < n_chip - 1:
                    ag[m, q, way, s] = ring.send(out[m].at[here, :], out[m].at[here, :], (ag_send, ag_recv), (m, q, way, s), ring.nexts[way])
                relays.append(ring.send(out[m].at[here, :], out[m].at[here, :], (dd_send, dd_recv), (m, q, way, s), ring.sibling))
    next(da_gather)
    for copy in relays + small:
        copy.wait_recv()
    for copy in ring.copies:
        copy.wait_send()


def reduce_all(da, loss, grads, seq_size, n_sub=2):
    n_mat = len(grads)
    n_chip = seq_size // 2
    half = grads[0].shape[0] // 2
    piece = half // (2 * n_chip)
    vmem = pl.BlockSpec(memory_space=pltpu.VMEM)
    dma = pltpu.SemaphoreType.DMA
    steps = n_chip - 1
    return pl.pallas_call(
        functools.partial(reduce_kernel, seq_size, n_mat, n_sub),
        out_shape=[jax.ShapeDtypeStruct((seq_size,) + da.shape, da.dtype), jax.ShapeDtypeStruct((seq_size,) + loss.shape, F32)]
        + [jax.ShapeDtypeStruct(g.shape, F32) for g in grads],
        in_specs=[vmem] * (2 + n_mat), out_specs=[vmem] * (2 + n_mat),
        scratch_shapes=[pltpu.VMEM((half, g.shape[1]), F32) for g in grads] * 2
        + [pltpu.VMEM((2, steps, piece, g.shape[1]), F32) for g in grads]
        + [dma((n_mat, 4))] * 2 + [dma((n_mat, n_sub, 2, steps))] * 4 + [dma((n_mat, n_sub, 2, n_chip))] * 2
        + [dma((2, 3))] * 2 + [dma((7,))] * 2 + [dma((seq_size - 1,))] * 2,
        compiler_params=pltpu.CompilerParams(collective_id=1, has_side_effects=True, vmem_limit_bytes=24 << 20),
        name="reduce_all",
    )(da, loss, *grads)


def finish_kernel(seq_size, vocab, n_loc, me_ref, da_all, loss_ref, gwp_ref, gwo_ref, we_ref, f_ref, t_row, u_row, loss_out, genc_out, gwe_out, gwp_out, gwo_out, d_raw, d_all):
    me = me_ref[0]
    n_af, joint = da_all.shape[1:]
    rows = n_af // seq_size
    n_all = n_af // n_loc
    gwp_out[...] = gwp_ref[...]
    gwo_out[...] = gwo_ref[:vocab, :]
    loss_out[...] = jnp.sum(loss_ref[:, 0, :], axis=0, keepdims=True)[:, :n_all]

    def ids(shape, dim):
        return lax.broadcasted_iota(jnp.int32, shape, dim)

    _, key = placement(t_row[...], u_row[...], n_all // seq_size)
    pick = jnp.where(ids((n_all, n_all), 1) == key, 1.0, 0.0).astype(BF16)
    left = jnp.where(ids((n_af, n_all), 0) // n_loc == ids((n_af, n_all), 1), 1.0, 0.0).astype(BF16)
    right = jnp.where(ids((n_all, n_af), 0) == ids((n_all, n_af), 1) // n_loc, 1.0, 0.0).astype(BF16)
    wide = dot_nn(dot_nn(left, pick).astype(BF16), right)
    same = ids((n_af, n_af), 0) % n_loc == ids((n_af, n_af), 1) % n_loc
    move = jnp.where(same, wide, 0.0).astype(BF16)
    for i in range(seq_size):
        for src in range(seq_size):
            d_raw[i, pl.ds(src * rows, rows), :] = da_all[src, pl.ds(i * rows, rows), :]
        d_all[pl.ds(i * n_af, n_af), :] = dot_nn(move, d_raw[i]).astype(BF16)
    here = d_all[pl.ds(pl.multiple_of(me * n_af, n_af), n_af), :]
    genc_out[...] = dot_nt(here, we_ref[...]).astype(BF16).reshape(genc_out.shape)
    gwe_out[...] = dot_tn(f_ref[...].reshape(seq_size * n_af, f_ref.shape[2]), d_all[...])


def finish(seq_idx, da_all, loss_all, gwp, gwo_t, w_enc, enc_all, frame_len, label_len, vocab, n_loc):
    seq_size, n_af, joint = da_all.shape
    n_all = n_af // n_loc
    vmem = pl.BlockSpec(memory_space=pltpu.VMEM)
    return pl.pallas_call(
        functools.partial(finish_kernel, seq_size, vocab, n_loc),
        grid_spec=pltpu.PrefetchScalarGridSpec(
            num_scalar_prefetch=1, grid=(), in_specs=[vmem] * 8, out_specs=[vmem] * 5,
            scratch_shapes=[pltpu.VMEM((seq_size, n_af, joint), BF16), pltpu.VMEM((seq_size * n_af, joint), BF16)]),
        out_shape=[
            jax.ShapeDtypeStruct((1, n_all), F32),
            jax.ShapeDtypeStruct((n_all, n_loc, enc_all.shape[2]), BF16),
            jax.ShapeDtypeStruct(w_enc.shape, F32),
            jax.ShapeDtypeStruct(gwp.shape, F32),
            jax.ShapeDtypeStruct((vocab, joint), F32),
        ],
        compiler_params=pltpu.CompilerParams(vmem_limit_bytes=24 << 20),
        name="finish",
    )(seq_idx, da_all, loss_all, gwp, gwo_t, w_enc, enc_all, frame_len[None], label_len[None])


def solution(mesh):
    seq_size = mesh.shape['seq']

    def local_fn(enc_out, pred_out, w_enc, w_pred, w_out, labels, frame_len, label_len):
        seq_idx = jnp.reshape(lax.axis_index('seq'), (1,)).astype(jnp.int32)
        n_all, n_loc, _ = enc_out.shape
        n_utt = n_all // seq_size
        n_frames = n_loc * seq_size
        vocab = w_out.shape[1]
        def keep(x):
            return pltpu.with_memory_space_constraint(x, pltpu.VMEM)

        enc_all, act_f, w_t, w_o, top = map(keep, spread_frames(enc_out, w_enc, w_out.T, seq_size))
        loss, da, *grads = local_grads(
            seq_idx, act_f, w_t, w_o, top, pred_out.reshape(-1, pred_out.shape[2]), w_pred,
            labels, frame_len, label_len, n_utt, n_frames, n_loc, vocab)
        da_all, loss_all, gwp, gwo_t = reduce_all(da, loss, grads, seq_size)
        loss, genc, gwe, gwp, gwo_t = finish(seq_idx, da_all, loss_all, gwp, gwo_t, w_enc, enc_all, frame_len, label_len, vocab, n_loc)
        return loss.reshape(n_all), genc, gwe, gwp, gwo_t.T

    in_specs = (P('dp', 'seq', None), P('dp', None, None), P(None, None), P(None, None), P(None, None), P('dp', None), P('dp'), P('dp'))
    out_specs = (P('dp'), P('dp', 'seq', None), P('dp', None), P('dp', None), P('dp', None))
    return jax.shard_map(local_fn, mesh=mesh, in_specs=in_specs, out_specs=out_specs, check_vma=False)
```

```python
import functools

import jax
import jax.numpy as jnp
from jax import lax
from jax.experimental import pallas as pl
from jax.experimental.pallas import tpu as pltpu
from jax.sharding import PartitionSpec as P

NEG_FILL = -1.0e30
CHUNK = 16
LANES = 128
TILE_CHUNKS = 16
TILE = CHUNK * TILE_CHUNKS
SUBS = 2
BODY_CHUNKS = SUBS * TILE_CHUNKS
SAFE_LOGIT = 60.0
F32 = jnp.float32
BF16 = jnp.bfloat16


def logadd(x, y):
    return jnp.maximum(x, y) + jnp.log(1.0 + jnp.exp(-jnp.abs(x - y)))


def dot_nn(x, y):
    return jnp.dot(x, y, preferred_element_type=F32)


def dot_tn(x, y):
    return lax.dot_general(x, y, (((0,), (0,)), ((), ())), preferred_element_type=F32)


def dot_nt(x, y):
    return lax.dot_general(x, y, (((1,), (1,)), ((), ())), preferred_element_type=F32)


def placement(t_row, u_row, n_utt):
    n_all = t_row.shape[1]
    n_dev = n_all // n_utt
    work = (t_row * ((u_row + CHUNK) // CHUNK)).astype(F32)
    row = jnp.broadcast_to(work, (n_all, n_all))
    col = jnp.transpose(row)
    r_id = lax.broadcasted_iota(jnp.int32, (n_all, n_all), 1)
    c_id = lax.broadcasted_iota(jnp.int32, (n_all, n_all), 0)

    def key(rank):
        rank = rank.astype(jnp.int32)
        turn = rank // n_dev
        pos = rank % n_dev
        return jnp.where(turn % 2 == 0, pos, n_dev - 1 - pos) * n_utt + turn

    ahead = jnp.where((col > row) | ((col == row) & (c_id < r_id)), 1.0, 0.0)
    behind = jnp.where((row > col) | ((row == col) & (r_id < c_id)), 1.0, 0.0)
    return key(jnp.sum(ahead, axis=0, keepdims=True)), key(jnp.sum(behind, axis=1, keepdims=True))


def local_kernel(n_utt, n_frames, n_loc, n_pos, vocab,
                 seq_ref, tlen_ref, ulen_ref,
                 act_f, wt_v, wo_v, top_ref, pred_hbm, wpred_hbm, labels_ref, t_row, u_row,
                 loss_ref, da_ref, gwp_ref, gwo_ref,
                 g_v, wp_v, act_g, lab_v, lab_scr,
                 hid, ex, sums, skew, cb_s, cl_s, ce_s, al, xb_s, xl_s, occ, dz_0, dz_1, z_0, z_1,
                 dc, da8, where, what, uid, sems):
    me = seq_ref[0]
    dz_v, z_v = (dz_0, dz_1), (z_0, z_1)
    n_diag = n_frames + n_pos - 1
    pitch = n_frames + 1
    skew_rows = (n_frames + n_pos) * pitch
    n_rows = n_utt * n_pos
    vocab_pad = wt_v.shape[0]
    n_grp = vocab_pad // LANES
    n_col = wt_v.shape[1] // LANES
    da_rows = n_utt * n_frames * 8

    n_all = n_utt * (n_frames // n_loc)
    weight = pltpu.make_async_copy(wpred_hbm, wp_v, sems.at[n_utt])
    weight.start()
    key, _ = placement(t_row[...], u_row[...], n_utt)
    who = lax.broadcasted_iota(jnp.int32, key.shape, 1)
    copies = [weight]
    for b in range(n_utt):
        uid[b] = jnp.sum(jnp.where(key == me * n_utt + b, who, 0))
    uid[n_utt] = 0
    for b in range(n_utt):
        copies.append(pltpu.make_async_copy(
            pred_hbm.at[pl.ds(pl.multiple_of(uid[b] * n_pos, n_pos), n_pos), :], g_v.at[pl.ds(b * n_pos, n_pos), :], sems.at[b]))
        copies[-1].start()

    skew_bits = skew_rows.bit_length()
    lab_bits = n_rows.bit_length()
    da_bits = (n_utt * n_frames).bit_length()

    def add_utt(b, pos):
        t_len = tlen_ref[uid[b]]
        n_chunk = (ulen_ref[uid[b]] + CHUNK) // CHUNK
        one_b = (uid[b] * n_loc) << skew_bits
        two_b = b * n_pos + ((b * n_loc + (b << da_bits)) << lab_bits)

        def add_chunks(q, pos):
            one = one_b + q * (pitch * CHUNK)
            two = two_b + q * CHUNK
            for t in range(n_frames):
                hi, lo = divmod(t, n_loc)
                where[pos + t] = one + (((hi * n_all * n_loc + lo) << skew_bits) + (pitch + 1) * t)
                what[pos + t] = two + ((hi * n_utt * n_loc + lo) << lab_bits)
            return pos + t_len
        return lax.fori_loop(0, n_chunk, add_chunks, pos)

    n_chunks = lax.fori_loop(0, n_utt, add_utt, 0)
    n_tiles = (n_chunks + BODY_CHUNKS - 1) // BODY_CHUNKS
    for k in range(BODY_CHUNKS):
        where[n_chunks + k] = (n_all * n_frames) << skew_bits
        what[n_chunks + k] = n_rows + (n_utt << (lab_bits + da_bits))

    def low(x, bits):
        return x & ((1 << bits) - 1)

    def label_row(i):
        return pl.multiple_of(low(what[i], lab_bits), CHUNK)

    def grad_row(i):
        return pl.multiple_of(low(what[i] >> lab_bits, da_bits) * 8, 8)

    def slot(i):
        return what[i] >> (lab_bits + da_bits)

    def frame_row(i):
        return where[i] >> skew_bits

    def skew_row(i):
        return low(where[i], skew_bits)

    dc[...] = jnp.zeros_like(dc)
    da8[...] = jnp.zeros_like(da8)
    gwo_ref[...] = jnp.zeros_like(gwo_ref)
    act_g[pl.ds(n_rows, CHUNK), :] = jnp.zeros((CHUNK, act_g.shape[1]), BF16)
    lab_v[pl.ds(n_rows, CHUNK), :] = jnp.full((CHUNK, LANES), -1, jnp.int32)

    lab_scr[...] = jnp.full_like(lab_scr, -1.0)
    for b in range(n_utt):
        lab_scr[b:b + 1, :n_pos - 1] = labels_ref[pl.ds(uid[b], 1), :].astype(F32)
    lab_t = jnp.transpose(lab_scr[...])
    for b in range(n_utt):
        lab_v[pl.ds(b * n_pos, n_pos), :] = jnp.broadcast_to(lab_t[:n_pos, b:b + 1], (n_pos, LANES)).astype(jnp.int32)

    for cp in copies:
        cp.wait()
    act_g[pl.ds(0, n_rows), :] = dot_nn(g_v[...], wp_v[...]).astype(BF16)

    lane = lax.broadcasted_iota(jnp.int32, (CHUNK, LANES), 1)
    left = lane < LANES // 2
    last_ok = lane < vocab - (n_grp - 1) * LANES

    def fwd_body(shifted, i, carry):
        r0 = pl.multiple_of(i * (SUBS * TILE), SUBS * TILE)
        c0 = i * BODY_CHUNKS
        for k in range(BODY_CHUNKS):
            pre = act_g[pl.ds(label_row(c0 + k), CHUNK), :].astype(F32) + act_f[pl.ds(frame_row(c0 + k), 1), :]
            hid[pl.ds(r0 + k * CHUNK, CHUNK), :] = jnp.tanh(pre).astype(BF16)
        for sub in range(SUBS):
            z_v[sub][...] = dot_nn(hid[pl.ds(r0 + sub * TILE, TILE), :], wo_v[...])
        for k in range(BODY_CHUNKS):
            z_ref = z_v[k // TILE_CHUNKS]
            rows = pl.ds(r0 + k * CHUNK, CHUNK)
            z_rows = pl.ds(k % TILE_CHUNKS * CHUNK, CHUNK)
            ids = lab_v[pl.ds(label_row(c0 + k), CHUNK), :]
            sb = slot(c0 + k) * skew_rows + skew_row(c0 + k)
            zs = [z_ref[z_rows, j * LANES:(j + 1) * LANES] for j in range(n_grp)]
            picked = functools.reduce(jnp.add, [jnp.where(lane + j * LANES == ids, zs[j], 0.0) for j in range(n_grp)])
            picked = jnp.sum(picked, axis=1, keepdims=True)
            if shifted:
                top = functools.reduce(jnp.maximum, zs[:-1] + [jnp.where(last_ok, zs[-1], NEG_FILL)])
                top = jnp.max(top, axis=1, keepdims=True)
                es = [jnp.exp(z - top) for z in zs]
            else:
                es = [jnp.exp(z) for z in zs]
            es[-1] = jnp.where(last_ok, es[-1], 0.0)
            for j in range(n_grp):
                ex[rows, j * LANES:(j + 1) * LANES] = es[j]
            tot = jnp.sum(functools.reduce(jnp.add, es), axis=1, keepdims=True)
            tot_b = jnp.broadcast_to(tot, (CHUNK, LANES))
            sums[rows, :] = tot_b
            log_norm = jnp.log(tot_b)
            if shifted:
                log_norm = log_norm + top
            skew[pl.ds(sb, CHUNK, stride=pitch), :] = jnp.where(left, zs[0][:, 0:1], picked) - log_norm
        return carry

    bound = jnp.max(top_ref[...])

    @pl.when(bound < SAFE_LOGIT)
    def _():
        lax.fori_loop(0, n_tiles, functools.partial(fwd_body, False), 0)

    @pl.when(jnp.logical_not(bound < SAFE_LOGIT))
    def _():
        lax.fori_loop(0, n_tiles, functools.partial(fwd_body, True), 0)

    lane_s = lax.broadcasted_iota(jnp.int32, (n_frames, LANES), 1)
    sub_s = lax.broadcasted_iota(jnp.int32, (n_frames, LANES), 0)
    t_lens = jnp.zeros((n_frames, LANES), jnp.int32)
    u_lens = jnp.zeros((n_frames, LANES), jnp.int32)
    for b in range(n_utt):
        t_lens = jnp.where(lane_s == b, tlen_ref[uid[b]], t_lens)
        u_lens = jnp.where(lane_s == b, ulen_ref[uid[b]], u_lens)
    slot_s = lane_s % (LANES // 2)
    live_t = sub_s < t_lens
    last_t = sub_s == t_lens - 1

    def merge_diag(d):
        base = d * pitch
        both = skew[pl.ds(base, n_frames), :]
        for b in range(1, n_utt):
            both = jnp.where(slot_s == b, skew[pl.ds(base + b * skew_rows, n_frames), :], both)
        bl = both
        lb = pltpu.roll(both, LANES // 2, 1)
        u = d - sub_s
        live = live_t & (u >= 0)
        here = pl.ds(pl.multiple_of(d * n_frames, n_frames), n_frames)
        cb_s[here, :] = jnp.where(live & (u <= u_lens), bl, NEG_FILL)
        cl_s[here, :] = jnp.where(live & (u < u_lens), lb, NEG_FILL)
        ce_s[here, :] = jnp.where(last_t & (u == u_lens), 1.0, 0.0)

    def merge_step(i, carry):
        for k in range(16):
            merge_diag(i * 16 + k)
        return carry
    lax.fori_loop(0, (n_frames + n_pos) // 16, merge_step, 0)

    def lattice_step(i, carry):
        a, be = carry
        fwd = pl.ds(pl.multiple_of(i * n_frames, n_frames), n_frames)
        bwd = pl.ds(pl.multiple_of((n_diag - 1 - i) * n_frames, n_frames), n_frames)
        back = (n_diag - 1 - i) * pitch
        al[pl.ds(i * pitch, n_frames), :] = a
        moved = jnp.where(sub_s == 0, NEG_FILL, pltpu.roll(a + cb_s[fwd, :], 1, 0))
        a = logadd(moved, a + cl_s[fwd, :])
        up = jnp.where(sub_s == n_frames - 1, NEG_FILL, pltpu.roll(be, n_frames - 1, 0))
        bl = cb_s[bwd, :]
        x_b = jnp.where(ce_s[bwd, :] > 0.0, bl, up + bl)
        x_l = be + cl_s[bwd, :]
        xb_s[pl.ds(back, n_frames), :] = x_b
        xl_s[pl.ds(back, n_frames), :] = x_l
        return a, logadd(x_b, x_l)

    def lattice_pair(i, carry):
        return lattice_step(2 * i + 1, lattice_step(2 * i, carry))

    neg = jnp.full((n_frames, LANES), NEG_FILL, F32)
    state = lax.fori_loop(0, n_diag // 2, lattice_pair, (jnp.where(sub_s == 0, 0.0, neg), neg))
    for i in range(n_diag // 2 * 2, n_diag):
        state = lattice_step(i, state)
    be0 = state[1]
    log_prob = jnp.where(t_lens[0:1, :] > 0, be0[0:1, :], 0.0)
    lane_8 = lax.broadcasted_iota(jnp.int32, loss_ref.shape, 1)
    loss_ref[...] = functools.reduce(jnp.add, [
        jnp.where(lane_8 == uid[b], -log_prob[:, b:b + 1], 0.0) for b in range(n_utt)])

    n_live = n_diag * pitch
    n_blk = CHUNK
    left_8 = left
    for r in range(0, pl.cdiv(n_live, n_blk) * n_blk, n_blk):
        rows = pl.ds(r, n_blk)
        a = al[rows, :] - log_prob
        x = jnp.where(left_8, a + xb_s[rows, :], pltpu.roll(a + xl_s[rows, :], LANES // 2, 1))
        occ[rows, :] = jnp.exp(jnp.minimum(x, 0.0))

    def bwd_tile(i, carry):
        r0 = pl.multiple_of(i * (SUBS * TILE), SUBS * TILE)
        c0 = i * BODY_CHUNKS
        for sub in range(SUBS):
            for kk in range(TILE_CHUNKS):
                k = sub * TILE_CHUNKS + kk
                rows = pl.ds(r0 + k * CHUNK, CHUNK)
                both = occ[pl.ds(skew_row(c0 + k), CHUNK, stride=pitch), :]
                ids = lab_v[pl.ds(label_row(c0 + k), CHUNK), :]
                b = slot(c0 + k)
                ob = jnp.sum(jnp.where(lane == b, both, 0.0), axis=1, keepdims=True)
                ol = jnp.sum(jnp.where(lane == b + LANES // 2, both, 0.0), axis=1, keepdims=True)
                scale = (ob + ol) / sums[rows, :]
                for j in range(n_grp):
                    dz = ex[rows, j * LANES:(j + 1) * LANES] * scale
                    if j == 0:
                        dz = dz - jnp.where(lane == 0, ob, 0.0)
                    dz = dz - jnp.where(lane + j * LANES == ids, ol, 0.0)
                    dz_v[sub][kk * CHUNK:(kk + 1) * CHUNK, j * LANES:(j + 1) * LANES] = dz.astype(BF16)
        for sub in range(SUBS):
            z_v[sub][...] = dot_nn(dz_v[sub][...], wt_v[...])
        for sub in range(SUBS):
            for kk in range(TILE_CHUNKS):
                k = sub * TILE_CHUNKS + kk
                lr, ar = label_row(c0 + k), grad_row(c0 + k)
                h = hid[pl.ds(r0 + k * CHUNK, CHUNK), :].astype(F32)
                dp = (z_v[sub][kk * CHUNK:(kk + 1) * CHUNK, :] * (1.0 - h * h)).astype(BF16).astype(F32)
                dc[pl.ds(lr, CHUNK), :] += dp
                for j in range(n_col):
                    da8[pl.ds(ar + j * da_rows, 8), :] += dp[:8, j * LANES:(j + 1) * LANES] + dp[8:, j * LANES:(j + 1) * LANES]
        dz_all = jnp.concatenate([dz_v[sub][...] for sub in range(SUBS)], axis=0)
        gwo_ref[...] += dot_tn(dz_all, hid[pl.ds(r0, SUBS * TILE), :])
        return carry
    lax.fori_loop(0, n_tiles, bwd_tile, 0)

    n_af = n_utt * n_frames
    for j in range(n_col):
        parts = [da8[pl.ds(j * da_rows + r, n_af, stride=8), :] for r in range(8)]
        da_ref[:, j * LANES:(j + 1) * LANES] = functools.reduce(jnp.add, parts).astype(BF16)
    gwp_ref[...] = dot_tn(g_v[...], dc[pl.ds(0, n_rows), :].astype(BF16))


def local_grads(seq_idx, act_f, w_t, w_o, top, pred_out, w_pred, labels, frame_len, label_len, n_utt, n_frames, n_loc, vocab):
    n_pos = labels.shape[1] + 1
    vocab_pad, joint = w_t.shape
    n_rows = n_utt * n_pos
    n_af = n_utt * n_frames
    max_rows = n_utt * n_frames * n_pos
    skew_rows = (n_frames + n_pos) * (n_frames + 1)
    n_chunks = max_rows // CHUNK + BODY_CHUNKS
    any_spec = pl.BlockSpec(memory_space=pl.ANY)
    vmem = pl.BlockSpec(memory_space=pltpu.VMEM)
    grid_spec = pltpu.PrefetchScalarGridSpec(
        num_scalar_prefetch=3, grid=(),
        in_specs=[vmem] * 4 + [any_spec] * 2 + [vmem] * 3,
        out_specs=[vmem] * 4,
        scratch_shapes=[
            pltpu.VMEM((n_rows, w_pred.shape[0]), BF16),
            pltpu.VMEM(w_pred.shape, BF16),
            pltpu.VMEM((n_rows + CHUNK, joint), BF16),
            pltpu.VMEM((n_rows + CHUNK, LANES), jnp.int32),
            pltpu.VMEM((n_utt, LANES), F32),
            pltpu.VMEM((max_rows, joint), BF16),
            pltpu.VMEM((max_rows, vocab_pad), F32),
            pltpu.VMEM((max_rows, LANES), F32),
            pltpu.VMEM((n_utt * skew_rows + CHUNK * (n_frames + 1), LANES), F32),
            pltpu.VMEM(((n_frames + n_pos) * n_frames, LANES), F32),
            pltpu.VMEM(((n_frames + n_pos) * n_frames, LANES), F32),
            pltpu.VMEM(((n_frames + n_pos) * n_frames, LANES), F32),
            pltpu.VMEM((skew_rows, LANES), F32),
            pltpu.VMEM((skew_rows, LANES), F32),
            pltpu.VMEM((skew_rows, LANES), F32),
            pltpu.VMEM((skew_rows, LANES), F32),
            pltpu.VMEM((TILE, vocab_pad), BF16),
            pltpu.VMEM((TILE, vocab_pad), BF16),
            pltpu.VMEM((TILE, max(joint, vocab_pad)), F32),
            pltpu.VMEM((TILE, max(joint, vocab_pad)), F32),
            pltpu.VMEM((n_rows + CHUNK, joint), F32),
            pltpu.VMEM((joint // LANES * n_af * 8, LANES), F32),
            pltpu.SMEM((n_chunks + n_frames,), jnp.int32),
            pltpu.SMEM((n_chunks + n_frames,), jnp.int32),
            pltpu.SMEM((n_utt + 1,), jnp.int32),
            pltpu.SemaphoreType.DMA((n_utt + 1,)),
        ])
    return pl.pallas_call(
        functools.partial(local_kernel, n_utt, n_frames, n_loc, n_pos, vocab),
        grid_spec=grid_spec,
        out_shape=[
            pltpu.VMEM((8, LANES), F32),
            pltpu.VMEM((n_af, joint), BF16),
            pltpu.VMEM((w_pred.shape[0], joint), F32),
            pltpu.VMEM((vocab_pad, joint), F32),
        ],
        compiler_params=pltpu.CompilerParams(vmem_limit_bytes=54 << 20),
        cost_estimate=pl.CostEstimate(flops=6 * max_rows * joint * vocab_pad, bytes_accessed=4 * max_rows * joint, transcendentals=2 * max_rows * joint),
        name="rnnt_local",
    )(seq_idx, frame_len, label_len, act_f, w_t, w_o, top, pred_out, w_pred, labels, frame_len[None], label_len[None])


def greet_all(seq_size, me):
    barrier = pltpu.get_barrier_semaphore()
    for j in range(1, seq_size):
        pl.semaphore_signal(barrier, inc=1, device_id={'seq': lax.rem(me + j, seq_size)}, device_id_type=pl.DeviceIdType.MESH)


def await_all(seq_size):
    pl.semaphore_wait(pltpu.get_barrier_semaphore(), seq_size - 1)


class Ring:
    def __init__(self, seq_size):
        self.me = lax.axis_index('seq')
        self.n_chip = seq_size // 2
        self.chip, self.core = lax.div(self.me, 2), lax.rem(self.me, 2)
        self.sibling = self.chip * 2 + 1 - self.core
        self.nexts = (self.behind(1, 1) * 2 + self.core, self.behind(0, 1) * 2 + self.core)
        self.copies = []

    def behind(self, way, hops):
        return lax.rem(self.chip + self.n_chip - hops, self.n_chip) if way == 0 else lax.rem(self.chip + hops, self.n_chip)

    def send(self, src, dst, sems, idx, peer):
        copy = pltpu.make_async_remote_copy(src_ref=src, dst_ref=dst, send_sem=sems[0].at[idx], recv_sem=sems[1].at[idx],
                                            device_id={'seq': peer}, device_id_type=pl.DeviceIdType.MESH)
        copy.start()
        self.copies.append(copy)
        return copy


def gather_stages(ring, blocks, ring_sems, sib_sems):
    rows = blocks.shape[1] // 2
    relays = []

    def relay(dev, r, idx):
        relays.append(ring.send(blocks.at[dev, r, :], blocks.at[dev, r, :], sib_sems, idx, ring.sibling))

    hop1 = {}
    for part in range(2):
        for way in range(2):
            r = pl.ds((way if part == 0 else 1 - way) * rows, rows)
            hop1[way, part] = ring.send(blocks.at[ring.me, r, :], blocks.at[ring.me, r, :], ring_sems, (way, part), ring.nexts[way])
    relay(ring.me, pl.ds(0, 2 * rows), 0)
    yield
    hop2 = {}
    for way in range(2):
        r = pl.ds(way * rows, rows)
        dev = ring.behind(way, 1) * 2 + ring.core
        hop1[way, 0].wait_recv()
        hop2[way] = ring.send(blocks.at[dev, r, :], blocks.at[dev, r, :], ring_sems, (way, 2), ring.nexts[way])
        relay(dev, r, 1 + way)
    yield
    for way in range(2):
        hop1[way, 1].wait_recv()
        relay(ring.behind(way, 1) * 2 + ring.core, pl.ds((1 - way) * rows, rows), 3 + way)
    yield
    for way in range(2):
        hop2[way].wait_recv()
        relay(ring.behind(way, 2) * 2 + ring.core, pl.ds(way * rows, rows), 5 + way)
    yield
    for copy in relays:
        copy.wait_recv()
    yield


def spread_kernel(seq_size, vocab, enc_hbm, we_hbm, wt_hbm, out_ref, act_ref, wt_out, wo_out, top_out,
                  enc_ref, we_ref, wt_ref, load_sem, a_send, a_recv, s_send, s_recv):
    ring = Ring(seq_size)
    rows = out_ref.shape[1]
    loads = [pltpu.make_async_copy(src, dst, load_sem.at[n]) for n, (src, dst) in enumerate(
        ((enc_hbm, enc_ref), (wt_hbm, wt_ref), (we_hbm, we_ref)))]
    for load in loads:
        load.start()

    def prepare():
        wt_out[vocab:, :] = jnp.zeros((wt_out.shape[0] - vocab, wt_out.shape[1]), BF16)
        wt_out[:vocab, :] = wt_ref[...]
        wo_out[...] = jnp.transpose(wt_out[...])
        top = jnp.max(jnp.sum(jnp.abs(wo_out[...].astype(F32)), axis=0, keepdims=True), axis=1, keepdims=True)
        top_out[...] = jnp.broadcast_to(top, top_out.shape)
        act_ref[seq_size * rows:, :] = jnp.zeros((8, act_ref.shape[1]), F32)

    def project(dev):
        act_ref[pl.ds(pl.multiple_of(dev * rows, rows), rows), :] = dot_nn(out_ref[dev], we_ref[...]).astype(BF16).astype(F32)

    greet_all(seq_size, ring.me)
    loads[0].wait()
    out_ref[pl.ds(ring.me, 1)] = enc_ref[...].reshape((1,) + out_ref.shape[1:])
    await_all(seq_size)
    stages = gather_stages(ring, out_ref, (a_send, a_recv), (s_send, s_recv))
    next(stages)
    loads[1].wait()
    prepare()
    loads[2].wait()
    for _ in stages:
        pass
    for dev in range(seq_size):
        project(dev)
    for copy in ring.copies:
        copy.wait_send()


def spread_frames(enc, w_enc, w_out_t, seq_size):
    n_all, n_loc, enc_dim = enc.shape
    vocab, joint = w_out_t.shape
    vocab_pad = pl.cdiv(vocab, LANES) * LANES
    vmem = pl.BlockSpec(memory_space=pltpu.VMEM)
    dma = pltpu.SemaphoreType.DMA
    return pl.pallas_call(
        functools.partial(spread_kernel, seq_size, vocab),
        out_shape=[pltpu.VMEM((seq_size, n_all * n_loc, enc_dim), enc.dtype),
                   pltpu.VMEM((seq_size * n_all * n_loc + 8, joint), F32),
                   pltpu.VMEM((vocab_pad, joint), BF16),
                   pltpu.VMEM((joint, vocab_pad), BF16),
                   pltpu.VMEM((8, LANES), F32)],
        in_specs=[pl.BlockSpec(memory_space=pltpu.HBM)] * 3, out_specs=[vmem] * 5,
        scratch_shapes=[pltpu.VMEM(enc.shape, enc.dtype), pltpu.VMEM(w_enc.shape, BF16), pltpu.VMEM(w_out_t.shape, BF16),
                        dma((3,))] + [dma((2, 3))] * 2 + [dma((7,))] * 2,
        compiler_params=pltpu.CompilerParams(collective_id=0, has_side_effects=True, vmem_limit_bytes=24 << 20),
        name="spread_frames",
    )(*(pltpu.with_memory_space_constraint(x, pltpu.HBM) for x in (enc, w_enc, w_out_t)))


def reduce_kernel(seq_size, n_mat, n_sub, da_ref, loss_ref, *refs):
    gw = refs[:n_mat]
    da_all, loss_out = refs[n_mat:n_mat + 2]
    out = refs[n_mat + 2:2 * n_mat + 2]
    rest = refs[2 * n_mat + 2:]
    sib_buf, own, ring_buf = rest[:n_mat], rest[n_mat:2 * n_mat], rest[2 * n_mat:3 * n_mat]
    (sib_send, sib_recv, rs_send, rs_recv, ag_send, ag_recv, dd_send, dd_recv,
     da_send, da_recv, ds_send, ds_recv, lo_send, lo_recv) = rest[3 * n_mat:]
    ring = Ring(seq_size)
    me, n_chip, core = ring.me, ring.n_chip, ring.core
    half = gw[0].shape[0] // 2
    chunk = half // n_chip
    piece = chunk // 2
    sub = piece // n_sub
    streams = [(m, q) for m in range(n_mat) for q in range(n_sub)]

    def at(way, hops, q):
        return pl.multiple_of((ring.behind(way, hops) * 2 + way) * piece + q * sub, sub)

    def mine(m, row, size):
        return gw[m].at[pl.ds(pl.multiple_of(core * half + row, size), size), :]

    greet_all(seq_size, me)
    da_all[pl.ds(me, 1)] = da_ref[...][None]
    loss_out[pl.ds(me, 1)] = loss_ref[...][None]
    await_all(seq_size)
    da_gather = gather_stages(ring, da_all, (da_send, da_recv), (ds_send, ds_recv))
    next(da_gather)
    order = [ring.behind(0, 1), ring.behind(1, 1), ring.behind(0, 2), ring.chip]
    sib = {}
    for m in range(n_mat):
        for n, c in enumerate(order):
            row = pl.multiple_of(c * chunk, chunk)
            src = gw[m].at[pl.ds(pl.multiple_of((1 - core) * half + row, chunk), chunk), :]
            sib[m, n] = ring.send(src, sib_buf[m].at[pl.ds(row, chunk), :], (sib_send, sib_recv), (m, n), ring.sibling)
    small = [ring.send(loss_ref, loss_out.at[me], (lo_send, lo_recv), j - 1, lax.rem(me + j, seq_size)) for j in range(1, seq_size)]

    def combine(m, n):
        rows = pl.ds(pl.multiple_of(order[n] * chunk, chunk), chunk)
        sib[m, n].wait_recv()
        own[m][rows, :] = mine(m, order[n] * chunk, chunk)[...] + sib_buf[m][rows, :]

    rs = {}
    for m in range(n_mat):
        for way in range(2):
            combine(m, way)
            for q in range(n_sub):
                rs[m, q, way, 0] = ring.send(own[m].at[pl.ds(at(way, 1, q), sub), :], ring_buf[m].at[way, 0, pl.ds(q * sub, sub), :],
                                             (rs_send, rs_recv), (m, q, way, 0), ring.nexts[way])
    next(da_gather)
    for m in range(n_mat):
        combine(m, 2)
        combine(m, 3)
    next(da_gather)

    for s in range(1, n_chip - 1):
        for m, q in streams:
            for way in range(2):
                rows = pl.ds(q * sub, sub)
                rs[m, q, way, s - 1].wait_recv()
                ring_buf[m][way, s - 1, rows, :] = ring_buf[m][way, s - 1, rows, :] + own[m][pl.ds(at(way, s + 1, q), sub), :]
                rs[m, q, way, s] = ring.send(ring_buf[m].at[way, s - 1, rows, :], ring_buf[m].at[way, s, rows, :],
                                             (rs_send, rs_recv), (m, q, way, s), ring.nexts[way])
    next(da_gather)

    def place(way, hops, q):
        return pl.ds(pl.multiple_of(core * half + at(way, hops, q), sub), sub)

    last = n_chip - 2
    ag, relays = {}, []
    for m, q in streams:
        for way in range(2):
            rs[m, q, way, last].wait_recv()
            here = place(way, 0, q)
            out[m][here, :] = ring_buf[m][way, last, pl.ds(q * sub, sub), :] + own[m][pl.ds(at(way, 0, q), sub), :]
            ag[m, q, way, 0] = ring.send(out[m].at[here, :], out[m].at[here, :], (ag_send, ag_recv), (m, q, way, 0), ring.nexts[way])
            relays.append(ring.send(out[m].at[here, :], out[m].at[here, :], (dd_send, dd_recv), (m, q, way, 0), ring.sibling))
    for s in range(1, n_chip):
        for m, q in streams:
            for way in range(2):
                ag[m, q, way, s - 1].wait_recv()
                here = place(way, s, q)
                if s < n_chip - 1:
                    ag[m, q, way, s] = ring.send(out[m].at[here, :], out[m].at[here, :], (ag_send, ag_recv), (m, q, way, s), ring.nexts[way])
                relays.append(ring.send(out[m].at[here, :], out[m].at[here, :], (dd_send, dd_recv), (m, q, way, s), ring.sibling))
    next(da_gather)
    for copy in relays + small:
        copy.wait_recv()
    for copy in ring.copies:
        copy.wait_send()


def reduce_all(da, loss, grads, seq_size, n_sub=2):
    n_mat = len(grads)
    n_chip = seq_size // 2
    half = grads[0].shape[0] // 2
    piece = half // (2 * n_chip)
    vmem = pl.BlockSpec(memory_space=pltpu.VMEM)
    dma = pltpu.SemaphoreType.DMA
    steps = n_chip - 1
    return pl.pallas_call(
        functools.partial(reduce_kernel, seq_size, n_mat, n_sub),
        out_shape=[jax.ShapeDtypeStruct((seq_size,) + da.shape, da.dtype), jax.ShapeDtypeStruct((seq_size,) + loss.shape, F32)]
        + [jax.ShapeDtypeStruct(g.shape, F32) for g in grads],
        in_specs=[vmem] * (2 + n_mat), out_specs=[vmem] * (2 + n_mat),
        scratch_shapes=[pltpu.VMEM((half, g.shape[1]), F32) for g in grads] * 2
        + [pltpu.VMEM((2, steps, piece, g.shape[1]), F32) for g in grads]
        + [dma((n_mat, 4))] * 2 + [dma((n_mat, n_sub, 2, steps))] * 4 + [dma((n_mat, n_sub, 2, n_chip))] * 2
        + [dma((2, 3))] * 2 + [dma((7,))] * 2 + [dma((seq_size - 1,))] * 2,
        compiler_params=pltpu.CompilerParams(collective_id=1, has_side_effects=True, vmem_limit_bytes=24 << 20),
        name="reduce_all",
    )(da, loss, *grads)


def finish_kernel(seq_size, vocab, n_loc, me_ref, da_all, loss_ref, gwp_ref, gwo_ref, we_ref, f_ref, t_row, u_row, loss_out, genc_out, gwe_out, gwp_out, gwo_out, gwo_v, d_raw, d_all, sems):
    me = me_ref[0]
    n_af, joint = da_all.shape[1:]
    rows = n_af // seq_size
    n_all = n_af // n_loc
    put_p = pltpu.make_async_copy(gwp_ref, gwp_out, sems.at[0])
    put_p.start()
    gwo_v[...] = gwo_ref[:vocab, :]
    put_o = pltpu.make_async_copy(gwo_v, gwo_out, sems.at[1])
    put_o.start()
    loss_out[...] = jnp.sum(loss_ref[:, 0, :], axis=0, keepdims=True)[:, :n_all]

    def ids(shape, dim):
        return lax.broadcasted_iota(jnp.int32, shape, dim)

    _, key = placement(t_row[...], u_row[...], n_all // seq_size)
    pick = jnp.where(ids((n_all, n_all), 1) == key, 1.0, 0.0).astype(BF16)
    left = jnp.where(ids((n_af, n_all), 0) // n_loc == ids((n_af, n_all), 1), 1.0, 0.0).astype(BF16)
    right = jnp.where(ids((n_all, n_af), 0) == ids((n_all, n_af), 1) // n_loc, 1.0, 0.0).astype(BF16)
    wide = dot_nn(dot_nn(left, pick).astype(BF16), right)
    same = ids((n_af, n_af), 0) % n_loc == ids((n_af, n_af), 1) % n_loc
    move = jnp.where(same, wide, 0.0).astype(BF16)
    for i in range(seq_size):
        for src in range(seq_size):
            d_raw[i, pl.ds(src * rows, rows), :] = da_all[src, pl.ds(i * rows, rows), :]
        d_all[pl.ds(i * n_af, n_af), :] = dot_nn(move, d_raw[i]).astype(BF16)
    here = d_all[pl.ds(pl.multiple_of(me * n_af, n_af), n_af), :]
    genc_out[...] = dot_nt(here, we_ref[...]).astype(BF16).reshape(genc_out.shape)
    gwe_out[...] = dot_tn(f_ref[...].reshape(seq_size * n_af, f_ref.shape[2]), d_all[...])
    put_p.wait()
    put_o.wait()


def finish(seq_idx, da_all, loss_all, gwp, gwo_t, w_enc, enc_all, frame_len, label_len, vocab, n_loc):
    seq_size, n_af, joint = da_all.shape
    n_all = n_af // n_loc
    vmem = pl.BlockSpec(memory_space=pltpu.VMEM)
    return pl.pallas_call(
        functools.partial(finish_kernel, seq_size, vocab, n_loc),
        grid_spec=pltpu.PrefetchScalarGridSpec(
            num_scalar_prefetch=1, grid=(), in_specs=[vmem] * 8, out_specs=[vmem] * 3 + [pl.BlockSpec(memory_space=pltpu.HBM)] * 2,
            scratch_shapes=[pltpu.VMEM((vocab, joint), F32), pltpu.VMEM((seq_size, n_af, joint), BF16), pltpu.VMEM((seq_size * n_af, joint), BF16), pltpu.SemaphoreType.DMA((2,))]),
        out_shape=[
            jax.ShapeDtypeStruct((1, n_all), F32),
            jax.ShapeDtypeStruct((n_all, n_loc, enc_all.shape[2]), BF16),
            jax.ShapeDtypeStruct(w_enc.shape, F32),
            jax.ShapeDtypeStruct(gwp.shape, F32),
            jax.ShapeDtypeStruct((vocab, joint), F32),
        ],
        compiler_params=pltpu.CompilerParams(vmem_limit_bytes=24 << 20),
        name="finish",
    )(seq_idx, da_all, loss_all, gwp, gwo_t, w_enc, enc_all, frame_len[None], label_len[None])


def solution(mesh):
    seq_size = mesh.shape['seq']

    def local_fn(enc_out, pred_out, w_enc, w_pred, w_out, labels, frame_len, label_len):
        seq_idx = jnp.reshape(lax.axis_index('seq'), (1,)).astype(jnp.int32)
        n_all, n_loc, _ = enc_out.shape
        n_utt = n_all // seq_size
        n_frames = n_loc * seq_size
        vocab = w_out.shape[1]
        def keep(x):
            return pltpu.with_memory_space_constraint(x, pltpu.VMEM)

        enc_all, act_f, w_t, w_o, top = map(keep, spread_frames(enc_out, w_enc, w_out.T, seq_size))
        loss, da, *grads = local_grads(
            seq_idx, act_f, w_t, w_o, top, pred_out.reshape(-1, pred_out.shape[2]), w_pred,
            labels, frame_len, label_len, n_utt, n_frames, n_loc, vocab)
        da_all, loss_all, gwp, gwo_t = reduce_all(da, loss, grads, seq_size)
        loss, genc, gwe, gwp, gwo_t = finish(seq_idx, da_all, loss_all, gwp, gwo_t, w_enc, enc_all, frame_len, label_len, vocab, n_loc)
        return loss.reshape(n_all), genc, gwe, gwp, gwo_t.T

    in_specs = (P('dp', 'seq', None), P('dp', None, None), P(None, None), P(None, None), P(None, None), P('dp', None), P('dp'), P('dp'))
    out_specs = (P('dp'), P('dp', 'seq', None), P('dp', None), P('dp', None), P('dp', None))
    return jax.shard_map(local_fn, mesh=mesh, in_specs=in_specs, out_specs=out_specs, check_vma=False)
```

```python
import functools

import jax
import jax.numpy as jnp
from jax import lax
from jax.experimental import pallas as pl
from jax.experimental.pallas import tpu as pltpu
from jax.sharding import PartitionSpec as P

NEG_FILL = -1.0e30
CHUNK = 16
LANES = 128
TILE_CHUNKS = 16
TILE = CHUNK * TILE_CHUNKS
SUBS = 2
BODY_CHUNKS = SUBS * TILE_CHUNKS
SAFE_LOGIT = 60.0
F32 = jnp.float32
BF16 = jnp.bfloat16


def logadd(x, y):
    return jnp.maximum(x, y) + jnp.log(1.0 + jnp.exp(-jnp.abs(x - y)))


def dot_nn(x, y):
    return jnp.dot(x, y, preferred_element_type=F32)


def dot_tn(x, y):
    return lax.dot_general(x, y, (((0,), (0,)), ((), ())), preferred_element_type=F32)


def dot_nt(x, y):
    return lax.dot_general(x, y, (((1,), (1,)), ((), ())), preferred_element_type=F32)


def placement(t_row, u_row, n_utt):
    n_all = t_row.shape[1]
    n_dev = n_all // n_utt
    work = (t_row * ((u_row + CHUNK) // CHUNK)).astype(F32)
    row = jnp.broadcast_to(work, (n_all, n_all))
    col = jnp.transpose(row)
    r_id = lax.broadcasted_iota(jnp.int32, (n_all, n_all), 1)
    c_id = lax.broadcasted_iota(jnp.int32, (n_all, n_all), 0)

    def key(rank):
        rank = rank.astype(jnp.int32)
        turn = rank // n_dev
        pos = rank % n_dev
        return jnp.where(turn % 2 == 0, pos, n_dev - 1 - pos) * n_utt + turn

    ahead = jnp.where((col > row) | ((col == row) & (c_id < r_id)), 1.0, 0.0)
    behind = jnp.where((row > col) | ((row == col) & (r_id < c_id)), 1.0, 0.0)
    return key(jnp.sum(ahead, axis=0, keepdims=True)), key(jnp.sum(behind, axis=1, keepdims=True))


def local_kernel(n_utt, n_frames, n_loc, n_pos, vocab,
                 seq_ref, tlen_ref, ulen_ref,
                 act_f, wt_v, wo_v, top_ref, pred_hbm, wpred_hbm, labels_ref, t_row, u_row,
                 loss_ref, da_ref, gwp_ref, gwo_ref,
                 g_v, wp_v, act_g, lab_v, lab_scr,
                 hid, ex, sums, skew, cb_s, cl_s, ce_s, al, xb_s, xl_s, occ, dz_0, dz_1, z_0, z_1,
                 dc, da8, where, what, uid, sems):
    me = seq_ref[0]
    dz_v, z_v = (dz_0, dz_1), (z_0, z_1)
    n_diag = n_frames + n_pos - 1
    pitch = n_frames + 1
    skew_rows = (n_frames + n_pos) * pitch
    n_rows = n_utt * n_pos
    vocab_pad = wt_v.shape[0]
    n_grp = vocab_pad // LANES
    n_col = wt_v.shape[1] // LANES
    da_rows = n_utt * n_frames * 8

    n_all = n_utt * (n_frames // n_loc)
    weight = pltpu.make_async_copy(wpred_hbm, wp_v, sems.at[n_utt])
    weight.start()
    key, _ = placement(t_row[...], u_row[...], n_utt)
    who = lax.broadcasted_iota(jnp.int32, key.shape, 1)
    copies = [weight]
    for b in range(n_utt):
        uid[b] = jnp.sum(jnp.where(key == me * n_utt + b, who, 0))
    uid[n_utt] = 0
    for b in range(n_utt):
        copies.append(pltpu.make_async_copy(
            pred_hbm.at[pl.ds(pl.multiple_of(uid[b] * n_pos, n_pos), n_pos), :], g_v.at[pl.ds(b * n_pos, n_pos), :], sems.at[b]))
        copies[-1].start()

    skew_bits = skew_rows.bit_length()
    lab_bits = n_rows.bit_length()
    da_bits = (n_utt * n_frames).bit_length()

    def add_utt(b, pos):
        t_len = tlen_ref[uid[b]]
        n_chunk = (ulen_ref[uid[b]] + CHUNK) // CHUNK
        one_b = (uid[b] * n_loc) << skew_bits
        two_b = b * n_pos + ((b * n_loc + (b << da_bits)) << lab_bits)

        def add_chunks(q, pos):
            one = one_b + q * (pitch * CHUNK)
            two = two_b + q * CHUNK
            for t in range(n_frames):
                hi, lo = divmod(t, n_loc)
                where[pos + t] = one + (((hi * n_all * n_loc + lo) << skew_bits) + (pitch + 1) * t)
                what[pos + t] = two + ((hi * n_utt * n_loc + lo) << lab_bits)
            return pos + t_len
        return lax.fori_loop(0, n_chunk, add_chunks, pos)

    n_chunks = lax.fori_loop(0, n_utt, add_utt, 0)
    n_tiles = (n_chunks + BODY_CHUNKS - 1) // BODY_CHUNKS
    for k in range(BODY_CHUNKS):
        where[n_chunks + k] = (n_all * n_frames) << skew_bits
        what[n_chunks + k] = n_rows + (n_utt << (lab_bits + da_bits))

    def low(x, bits):
        return x & ((1 << bits) - 1)

    def label_row(i):
        return pl.multiple_of(low(what[i], lab_bits), CHUNK)

    def grad_row(i):
        return pl.multiple_of(low(what[i] >> lab_bits, da_bits) * 8, 8)

    def slot(i):
        return what[i] >> (lab_bits + da_bits)

    def frame_row(i):
        return where[i] >> skew_bits

    def skew_row(i):
        return low(where[i], skew_bits)

    dc[...] = jnp.zeros_like(dc)
    da8[...] = jnp.zeros_like(da8)
    gwo_ref[...] = jnp.zeros_like(gwo_ref)
    act_g[pl.ds(n_rows, CHUNK), :] = jnp.zeros((CHUNK, act_g.shape[1]), BF16)
    lab_v[pl.ds(n_rows, CHUNK), :] = jnp.full((CHUNK, LANES), -1, jnp.int32)

    lab_scr[...] = jnp.full_like(lab_scr, -1.0)
    for b in range(n_utt):
        lab_scr[b:b + 1, :n_pos - 1] = labels_ref[pl.ds(uid[b], 1), :].astype(F32)
    lab_t = jnp.transpose(lab_scr[...])
    for b in range(n_utt):
        lab_v[pl.ds(b * n_pos, n_pos), :] = jnp.broadcast_to(lab_t[:n_pos, b:b + 1], (n_pos, LANES)).astype(jnp.int32)

    for cp in copies:
        cp.wait()
    act_g[pl.ds(0, n_rows), :] = dot_nn(g_v[...], wp_v[...]).astype(BF16)

    lane = lax.broadcasted_iota(jnp.int32, (CHUNK, LANES), 1)
    left = lane < LANES // 2
    last_ok = lane < vocab - (n_grp - 1) * LANES

    def fwd_body(shifted, i, carry):
        r0 = pl.multiple_of(i * (SUBS * TILE), SUBS * TILE)
        c0 = i * BODY_CHUNKS
        for k in range(BODY_CHUNKS):
            pre = act_g[pl.ds(label_row(c0 + k), CHUNK), :].astype(F32) + act_f[pl.ds(frame_row(c0 + k), 1), :]
            hid[pl.ds(r0 + k * CHUNK, CHUNK), :] = jnp.tanh(pre).astype(BF16)
        for sub in range(SUBS):
            z_v[sub][...] = dot_nn(hid[pl.ds(r0 + sub * TILE, TILE), :], wo_v[...])
        for k in range(BODY_CHUNKS):
            z_ref = z_v[k // TILE_CHUNKS]
            rows = pl.ds(r0 + k * CHUNK, CHUNK)
            z_rows = pl.ds(k % TILE_CHUNKS * CHUNK, CHUNK)
            ids = lab_v[pl.ds(label_row(c0 + k), CHUNK), :]
            sb = slot(c0 + k) * skew_rows + skew_row(c0 + k)
            zs = [z_ref[z_rows, j * LANES:(j + 1) * LANES] for j in range(n_grp)]
            picked = functools.reduce(jnp.add, [jnp.where(lane + j * LANES == ids, zs[j], 0.0) for j in range(n_grp)])
            picked = jnp.sum(picked, axis=1, keepdims=True)
            if shifted:
                top = functools.reduce(jnp.maximum, zs[:-1] + [jnp.where(last_ok, zs[-1], NEG_FILL)])
                top = jnp.max(top, axis=1, keepdims=True)
                es = [jnp.exp(z - top) for z in zs]
            else:
                es = [jnp.exp(z) for z in zs]
            es[-1] = jnp.where(last_ok, es[-1], 0.0)
            for j in range(n_grp):
                ex[rows, j * LANES:(j + 1) * LANES] = es[j]
            tot = jnp.sum(functools.reduce(jnp.add, es), axis=1, keepdims=True)
            tot_b = jnp.broadcast_to(tot, (CHUNK, LANES))
            sums[rows, :] = tot_b
            log_norm = jnp.log(tot_b)
            if shifted:
                log_norm = log_norm + top
            skew[pl.ds(sb, CHUNK, stride=pitch), :] = jnp.where(left, zs[0][:, 0:1], picked) - log_norm
        return carry

    bound = jnp.max(top_ref[...])

    @pl.when(bound < SAFE_LOGIT)
    def _():
        lax.fori_loop(0, n_tiles, functools.partial(fwd_body, False), 0)

    @pl.when(jnp.logical_not(bound < SAFE_LOGIT))
    def _():
        lax.fori_loop(0, n_tiles, functools.partial(fwd_body, True), 0)

    lane_s = lax.broadcasted_iota(jnp.int32, (n_frames, LANES), 1)
    sub_s = lax.broadcasted_iota(jnp.int32, (n_frames, LANES), 0)
    t_lens = jnp.zeros((n_frames, LANES), jnp.int32)
    u_lens = jnp.zeros((n_frames, LANES), jnp.int32)
    for b in range(n_utt):
        t_lens = jnp.where(lane_s == b, tlen_ref[uid[b]], t_lens)
        u_lens = jnp.where(lane_s == b, ulen_ref[uid[b]], u_lens)
    slot_s = lane_s % (LANES // 2)
    live_t = sub_s < t_lens
    last_t = sub_s == t_lens - 1

    def merge_diag(d):
        base = d * pitch
        both = skew[pl.ds(base, n_frames), :]
        for b in range(1, n_utt):
            both = jnp.where(slot_s == b, skew[pl.ds(base + b * skew_rows, n_frames), :], both)
        bl = both
        lb = pltpu.roll(both, LANES // 2, 1)
        u = d - sub_s
        live = live_t & (u >= 0)
        here = pl.ds(pl.multiple_of(d * n_frames, n_frames), n_frames)
        cb_s[here, :] = jnp.where(live & (u <= u_lens), bl, NEG_FILL)
        cl_s[here, :] = jnp.where(live & (u < u_lens), lb, NEG_FILL)
        ce_s[here, :] = jnp.where(last_t & (u == u_lens), 1.0, 0.0)

    def merge_step(i, carry):
        for k in range(16):
            merge_diag(i * 16 + k)
        return carry
    lax.fori_loop(0, (n_frames + n_pos) // 16, merge_step, 0)

    def lattice_step(i, carry):
        a, be = carry
        fwd = pl.ds(pl.multiple_of(i * n_frames, n_frames), n_frames)
        bwd = pl.ds(pl.multiple_of((n_diag - 1 - i) * n_frames, n_frames), n_frames)
        back = (n_diag - 1 - i) * pitch
        al[pl.ds(i * pitch, n_frames), :] = a
        moved = jnp.where(sub_s == 0, NEG_FILL, pltpu.roll(a + cb_s[fwd, :], 1, 0))
        a = logadd(moved, a + cl_s[fwd, :])
        up = jnp.where(sub_s == n_frames - 1, NEG_FILL, pltpu.roll(be, n_frames - 1, 0))
        bl = cb_s[bwd, :]
        x_b = jnp.where(ce_s[bwd, :] > 0.0, bl, up + bl)
        x_l = be + cl_s[bwd, :]
        xb_s[pl.ds(back, n_frames), :] = x_b
        xl_s[pl.ds(back, n_frames), :] = x_l
        return a, logadd(x_b, x_l)

    def lattice_pair(i, carry):
        return lattice_step(2 * i + 1, lattice_step(2 * i, carry))

    neg = jnp.full((n_frames, LANES), NEG_FILL, F32)
    state = lax.fori_loop(0, n_diag // 2, lattice_pair, (jnp.where(sub_s == 0, 0.0, neg), neg))
    for i in range(n_diag // 2 * 2, n_diag):
        state = lattice_step(i, state)
    be0 = state[1]
    log_prob = jnp.where(t_lens[0:1, :] > 0, be0[0:1, :], 0.0)
    lane_8 = lax.broadcasted_iota(jnp.int32, loss_ref.shape, 1)
    loss_ref[...] = functools.reduce(jnp.add, [
        jnp.where(lane_8 == uid[b], -log_prob[:, b:b + 1], 0.0) for b in range(n_utt)])

    n_live = n_diag * pitch
    n_blk = CHUNK
    left_8 = left
    for r in range(0, pl.cdiv(n_live, n_blk) * n_blk, n_blk):
        rows = pl.ds(r, n_blk)
        a = al[rows, :] - log_prob
        x = jnp.where(left_8, a + xb_s[rows, :], pltpu.roll(a + xl_s[rows, :], LANES // 2, 1))
        occ[rows, :] = jnp.exp(jnp.minimum(x, 0.0))

    def bwd_tile(i, carry):
        r0 = pl.multiple_of(i * (SUBS * TILE), SUBS * TILE)
        c0 = i * BODY_CHUNKS
        for sub in range(SUBS):
            for kk in range(TILE_CHUNKS):
                k = sub * TILE_CHUNKS + kk
                rows = pl.ds(r0 + k * CHUNK, CHUNK)
                both = occ[pl.ds(skew_row(c0 + k), CHUNK, stride=pitch), :]
                ids = lab_v[pl.ds(label_row(c0 + k), CHUNK), :]
                b = slot(c0 + k)
                ob = jnp.sum(jnp.where(lane == b, both, 0.0), axis=1, keepdims=True)
                ol = jnp.sum(jnp.where(lane == b + LANES // 2, both, 0.0), axis=1, keepdims=True)
                scale = (ob + ol) / sums[rows, :]
                for j in range(n_grp):
                    dz = ex[rows, j * LANES:(j + 1) * LANES] * scale
                    if j == 0:
                        dz = dz - jnp.where(lane == 0, ob, 0.0)
                    dz = dz - jnp.where(lane + j * LANES == ids, ol, 0.0)
                    dz_v[sub][kk * CHUNK:(kk + 1) * CHUNK, j * LANES:(j + 1) * LANES] = dz.astype(BF16)
        for sub in range(SUBS):
            z_v[sub][...] = dot_nn(dz_v[sub][...], wt_v[...])
        for sub in range(SUBS):
            for kk in range(TILE_CHUNKS):
                k = sub * TILE_CHUNKS + kk
                lr, ar = label_row(c0 + k), grad_row(c0 + k)
                h = hid[pl.ds(r0 + k * CHUNK, CHUNK), :].astype(F32)
                dp = (z_v[sub][kk * CHUNK:(kk + 1) * CHUNK, :] * (1.0 - h * h)).astype(BF16).astype(F32)
                dc[pl.ds(lr, CHUNK), :] += dp
                for j in range(n_col):
                    da8[pl.ds(ar + j * da_rows, 8), :] += dp[:8, j * LANES:(j + 1) * LANES] + dp[8:, j * LANES:(j + 1) * LANES]
        dz_all = jnp.concatenate([dz_v[sub][...] for sub in range(SUBS)], axis=0)
        gwo_ref[...] += dot_tn(dz_all, hid[pl.ds(r0, SUBS * TILE), :])
        return carry
    lax.fori_loop(0, n_tiles, bwd_tile, 0)

    n_af = n_utt * n_frames
    for j in range(n_col):
        parts = [da8[pl.ds(j * da_rows + r, n_af, stride=8), :] for r in range(8)]
        da_ref[:, j * LANES:(j + 1) * LANES] = functools.reduce(jnp.add, parts).astype(BF16)
    gwp_ref[...] = dot_tn(g_v[...], dc[pl.ds(0, n_rows), :].astype(BF16))


def local_grads(seq_idx, act_f, w_t, w_o, top, pred_out, w_pred, labels, frame_len, label_len, n_utt, n_frames, n_loc, vocab):
    n_pos = labels.shape[1] + 1
    vocab_pad, joint = w_t.shape
    n_rows = n_utt * n_pos
    n_af = n_utt * n_frames
    max_rows = n_utt * n_frames * n_pos
    skew_rows = (n_frames + n_pos) * (n_frames + 1)
    n_chunks = max_rows // CHUNK + BODY_CHUNKS
    any_spec = pl.BlockSpec(memory_space=pl.ANY)
    vmem = pl.BlockSpec(memory_space=pltpu.VMEM)
    grid_spec = pltpu.PrefetchScalarGridSpec(
        num_scalar_prefetch=3, grid=(),
        in_specs=[vmem] * 4 + [any_spec] * 2 + [vmem] * 3,
        out_specs=[vmem] * 4,
        scratch_shapes=[
            pltpu.VMEM((n_rows, w_pred.shape[0]), BF16),
            pltpu.VMEM(w_pred.shape, BF16),
            pltpu.VMEM((n_rows + CHUNK, joint), BF16),
            pltpu.VMEM((n_rows + CHUNK, LANES), jnp.int32),
            pltpu.VMEM((n_utt, LANES), F32),
            pltpu.VMEM((max_rows, joint), BF16),
            pltpu.VMEM((max_rows, vocab_pad), F32),
            pltpu.VMEM((max_rows, LANES), F32),
            pltpu.VMEM((n_utt * skew_rows + CHUNK * (n_frames + 1), LANES), F32),
            pltpu.VMEM(((n_frames + n_pos) * n_frames, LANES), F32),
            pltpu.VMEM(((n_frames + n_pos) * n_frames, LANES), F32),
            pltpu.VMEM(((n_frames + n_pos) * n_frames, LANES), F32),
            pltpu.VMEM((skew_rows, LANES), F32),
            pltpu.VMEM((skew_rows, LANES), F32),
            pltpu.VMEM((skew_rows, LANES), F32),
            pltpu.VMEM((skew_rows, LANES), F32),
            pltpu.VMEM((TILE, vocab_pad), BF16),
            pltpu.VMEM((TILE, vocab_pad), BF16),
            pltpu.VMEM((TILE, max(joint, vocab_pad)), F32),
            pltpu.VMEM((TILE, max(joint, vocab_pad)), F32),
            pltpu.VMEM((n_rows + CHUNK, joint), F32),
            pltpu.VMEM((joint // LANES * n_af * 8, LANES), F32),
            pltpu.SMEM((n_chunks + n_frames,), jnp.int32),
            pltpu.SMEM((n_chunks + n_frames,), jnp.int32),
            pltpu.SMEM((n_utt + 1,), jnp.int32),
            pltpu.SemaphoreType.DMA((n_utt + 1,)),
        ])
    return pl.pallas_call(
        functools.partial(local_kernel, n_utt, n_frames, n_loc, n_pos, vocab),
        grid_spec=grid_spec,
        out_shape=[
            pltpu.VMEM((8, LANES), F32),
            pltpu.VMEM((n_af, joint), BF16),
            pltpu.VMEM((w_pred.shape[0], joint), F32),
            pltpu.VMEM((vocab_pad, joint), F32),
        ],
        compiler_params=pltpu.CompilerParams(vmem_limit_bytes=54 << 20),
        cost_estimate=pl.CostEstimate(flops=6 * max_rows * joint * vocab_pad, bytes_accessed=4 * max_rows * joint, transcendentals=2 * max_rows * joint),
        name="rnnt_local",
    )(seq_idx, frame_len, label_len, act_f, w_t, w_o, top, pred_out, w_pred, labels, frame_len[None], label_len[None])


def greet_all(seq_size, me):
    barrier = pltpu.get_barrier_semaphore()
    for j in range(1, seq_size):
        pl.semaphore_signal(barrier, inc=1, device_id={'seq': lax.rem(me + j, seq_size)}, device_id_type=pl.DeviceIdType.MESH)


def await_all(seq_size):
    pl.semaphore_wait(pltpu.get_barrier_semaphore(), seq_size - 1)


class Ring:
    def __init__(self, seq_size):
        self.me = lax.axis_index('seq')
        self.n_chip = seq_size // 2
        self.chip, self.core = lax.div(self.me, 2), lax.rem(self.me, 2)
        self.sibling = self.chip * 2 + 1 - self.core
        self.nexts = (self.behind(1, 1) * 2 + self.core, self.behind(0, 1) * 2 + self.core)
        self.copies = []

    def behind(self, way, hops):
        return lax.rem(self.chip + self.n_chip - hops, self.n_chip) if way == 0 else lax.rem(self.chip + hops, self.n_chip)

    def send(self, src, dst, sems, idx, peer):
        copy = pltpu.make_async_remote_copy(src_ref=src, dst_ref=dst, send_sem=sems[0].at[idx], recv_sem=sems[1].at[idx],
                                            device_id={'seq': peer}, device_id_type=pl.DeviceIdType.MESH)
        copy.start()
        self.copies.append(copy)
        return copy


def gather_stages(ring, blocks, ring_sems, sib_sems):
    rows = blocks.shape[1] // 2
    relays = []

    def relay(dev, r, idx):
        relays.append(ring.send(blocks.at[dev, r, :], blocks.at[dev, r, :], sib_sems, idx, ring.sibling))

    hop1 = {}
    for part in range(2):
        for way in range(2):
            r = pl.ds((way if part == 0 else 1 - way) * rows, rows)
            hop1[way, part] = ring.send(blocks.at[ring.me, r, :], blocks.at[ring.me, r, :], ring_sems, (way, part), ring.nexts[way])
        yield
    relay(ring.me, pl.ds(0, 2 * rows), 0)
    hop2 = {}
    for way in range(2):
        r = pl.ds(way * rows, rows)
        dev = ring.behind(way, 1) * 2 + ring.core
        hop1[way, 0].wait_recv()
        hop2[way] = ring.send(blocks.at[dev, r, :], blocks.at[dev, r, :], ring_sems, (way, 2), ring.nexts[way])
        relay(dev, r, 1 + way)
    yield
    for way in range(2):
        hop1[way, 1].wait_recv()
        relay(ring.behind(way, 1) * 2 + ring.core, pl.ds((1 - way) * rows, rows), 3 + way)
    yield
    for way in range(2):
        hop2[way].wait_recv()
        relay(ring.behind(way, 2) * 2 + ring.core, pl.ds(way * rows, rows), 5 + way)
    yield
    for copy in relays:
        copy.wait_recv()
    yield


def spread_kernel(seq_size, vocab, enc_hbm, we_hbm, wt_hbm, out_ref, act_ref, wt_out, wo_out, top_out,
                  enc_ref, we_ref, wt_ref, load_sem, a_send, a_recv, s_send, s_recv):
    ring = Ring(seq_size)
    rows = out_ref.shape[1]
    loads = [pltpu.make_async_copy(src, dst, load_sem.at[n]) for n, (src, dst) in enumerate(
        ((enc_hbm, enc_ref), (wt_hbm, wt_ref), (we_hbm, we_ref)))]
    for load in loads:
        load.start()

    def prepare():
        wt_out[vocab:, :] = jnp.zeros((wt_out.shape[0] - vocab, wt_out.shape[1]), BF16)
        wt_out[:vocab, :] = wt_ref[...]
        wo_out[...] = jnp.transpose(wt_out[...])
        top = jnp.max(jnp.sum(jnp.abs(wo_out[...].astype(F32)), axis=0, keepdims=True), axis=1, keepdims=True)
        top_out[...] = jnp.broadcast_to(top, top_out.shape)
        act_ref[seq_size * rows:, :] = jnp.zeros((8, act_ref.shape[1]), F32)

    def project(dev):
        act_ref[pl.ds(pl.multiple_of(dev * rows, rows), rows), :] = dot_nn(out_ref[dev], we_ref[...]).astype(BF16).astype(F32)

    greet_all(seq_size, ring.me)
    loads[0].wait()
    out_ref[pl.ds(ring.me, 1)] = enc_ref[...].reshape((1,) + out_ref.shape[1:])
    await_all(seq_size)
    stages = gather_stages(ring, out_ref, (a_send, a_recv), (s_send, s_recv))
    next(stages)
    next(stages)
    loads[1].wait()
    prepare()
    loads[2].wait()
    for _ in stages:
        pass
    for dev in range(seq_size):
        project(dev)
    for copy in ring.copies:
        copy.wait_send()


def spread_frames(enc, w_enc, w_out_t, seq_size):
    n_all, n_loc, enc_dim = enc.shape
    vocab, joint = w_out_t.shape
    vocab_pad = pl.cdiv(vocab, LANES) * LANES
    vmem = pl.BlockSpec(memory_space=pltpu.VMEM)
    dma = pltpu.SemaphoreType.DMA
    return pl.pallas_call(
        functools.partial(spread_kernel, seq_size, vocab),
        out_shape=[pltpu.VMEM((seq_size, n_all * n_loc, enc_dim), enc.dtype),
                   pltpu.VMEM((seq_size * n_all * n_loc + 8, joint), F32),
                   pltpu.VMEM((vocab_pad, joint), BF16),
                   pltpu.VMEM((joint, vocab_pad), BF16),
                   pltpu.VMEM((8, LANES), F32)],
        in_specs=[pl.BlockSpec(memory_space=pltpu.HBM)] * 3, out_specs=[vmem] * 5,
        scratch_shapes=[pltpu.VMEM(enc.shape, enc.dtype), pltpu.VMEM(w_enc.shape, BF16), pltpu.VMEM(w_out_t.shape, BF16),
                        dma((3,))] + [dma((2, 3))] * 2 + [dma((7,))] * 2,
        compiler_params=pltpu.CompilerParams(collective_id=0, has_side_effects=True, vmem_limit_bytes=24 << 20),
        name="spread_frames",
    )(*(pltpu.with_memory_space_constraint(x, pltpu.HBM) for x in (enc, w_enc, w_out_t)))


def reduce_kernel(seq_size, n_mat, n_sub, da_ref, loss_ref, *refs):
    gw = refs[:n_mat]
    da_all, loss_out = refs[n_mat:n_mat + 2]
    out = refs[n_mat + 2:2 * n_mat + 2]
    rest = refs[2 * n_mat + 2:]
    sib_buf, own, ring_buf = rest[:n_mat], rest[n_mat:2 * n_mat], rest[2 * n_mat:3 * n_mat]
    (sib_send, sib_recv, rs_send, rs_recv, ag_send, ag_recv, dd_send, dd_recv,
     da_send, da_recv, ds_send, ds_recv, lo_send, lo_recv) = rest[3 * n_mat:]
    ring = Ring(seq_size)
    me, n_chip, core = ring.me, ring.n_chip, ring.core
    half = gw[0].shape[0] // 2
    chunk = half // n_chip
    piece = chunk // 2
    sub = piece // n_sub
    streams = [(m, q) for m in range(n_mat) for q in range(n_sub)]
    front = (ring.behind(1, 1), ring.behind(0, 1))
    far = ring.behind(0, 2)

    def at(c, part, q):
        return pl.multiple_of((c * 2 + part) * piece + q * sub, sub)

    def mine(m, row, size):
        return gw[m].at[pl.ds(pl.multiple_of(core * half + row, size), size), :]

    greet_all(seq_size, me)
    da_all[pl.ds(me, 1)] = da_ref[...][None]
    loss_out[pl.ds(me, 1)] = loss_ref[...][None]
    await_all(seq_size)
    da_gather = gather_stages(ring, da_all, (da_send, da_recv), (ds_send, ds_recv))
    next(da_gather)
    order = [far, front[0], front[1], ring.chip]
    sib = {}
    for m in range(n_mat):
        for n, c in enumerate(order):
            row = pl.multiple_of(c * chunk, chunk)
            src = gw[m].at[pl.ds(pl.multiple_of((1 - core) * half + row, chunk), chunk), :]
            sib[m, n] = ring.send(src, sib_buf[m].at[pl.ds(row, chunk), :], (sib_send, sib_recv), (m, n), ring.sibling)

    def combine(m, n):
        rows = pl.ds(pl.multiple_of(order[n] * chunk, chunk), chunk)
        sib[m, n].wait_recv()
        own[m][rows, :] = mine(m, order[n] * chunk, chunk)[...] + sib_buf[m][rows, :]

    rs = {}

    def push(m, q, way, kind, src):
        rs[m, q, way, kind] = ring.send(src, ring_buf[m].at[way, kind, pl.ds(q * sub, sub), :],
                                        (rs_send, rs_recv), (m, q, way, kind), ring.nexts[way])

    for m in range(n_mat):
        combine(m, 0)
        for q in range(n_sub):
            for way in range(2):
                push(m, q, way, 0, own[m].at[pl.ds(at(far, way, q), sub), :])
    for m in range(n_mat):
        combine(m, 1)
        combine(m, 2)
        for q in range(n_sub):
            for way in range(2):
                push(m, q, way, 1, own[m].at[pl.ds(at(front[way], 1 - way, q), sub), :])
    next(da_gather)
    small = [ring.send(loss_ref, loss_out.at[me], (lo_send, lo_recv), j - 1, lax.rem(me + j, seq_size)) for j in range(1, seq_size)]
    for m in range(n_mat):
        combine(m, 3)
    for m, q in streams:
        for way in range(2):
            rows = pl.ds(q * sub, sub)
            rs[m, q, way, 0].wait_recv()
            ring_buf[m][way, 0, rows, :] = ring_buf[m][way, 0, rows, :] + own[m][pl.ds(at(front[way], way, q), sub), :]
            push(m, q, way, 2, ring_buf[m].at[way, 0, rows, :])
    next(da_gather)
    next(da_gather)

    def place(c, part, q):
        return pl.ds(pl.multiple_of(core * half + at(c, part, q), sub), sub)

    ag, relays = {}, []

    def pass_on(m, q, way, kind, c, part):
        here = place(c, part, q)
        ag[m, q, way, kind] = ring.send(out[m].at[here, :], out[m].at[here, :], (ag_send, ag_recv), (m, q, way, kind), ring.nexts[way])

    def relay(m, c, idx):
        r = pl.ds(pl.multiple_of(core * half + c * chunk, chunk), chunk)
        relays.append(ring.send(out[m].at[r, :], out[m].at[r, :], (dd_send, dd_recv), (m, idx), ring.sibling))

    for m, q in streams:
        rows = pl.ds(q * sub, sub)
        for way in range(2):
            rs[m, q, 1 - way, 1].wait_recv()
            rs[m, q, way, 2].wait_recv()
            out[m][place(ring.chip, way, q), :] = (ring_buf[m][way, 2, rows, :] + ring_buf[m][1 - way, 1, rows, :]) + own[m][pl.ds(at(ring.chip, way, q), sub), :]
            pass_on(m, q, way, 0, ring.chip, way)
    for m, q in streams:
        for way in range(2):
            pass_on(m, q, way, 1, ring.chip, 1 - way)
    for m in range(n_mat):
        relay(m, ring.chip, 0)
    for m, q in streams:
        for way in range(2):
            ag[m, q, way, 0].wait_recv()
            pass_on(m, q, way, 2, ring.behind(way, 1), way)
    next(da_gather)
    for m in range(n_mat):
        for way in range(2):
            for q in range(n_sub):
                ag[m, q, way, 1].wait_recv()
            relay(m, ring.behind(way, 1), 1 + way)
    for m in range(n_mat):
        for way in range(2):
            for q in range(n_sub):
                ag[m, q, way, 2].wait_recv()
        relay(m, far, 3)
    next(da_gather)
    for copy in relays + small:
        copy.wait_recv()
    for copy in ring.copies:
        copy.wait_send()


def reduce_all(da, loss, grads, seq_size, n_sub=1):
    n_mat = len(grads)
    n_chip = seq_size // 2
    half = grads[0].shape[0] // 2
    piece = half // (2 * n_chip)
    vmem = pl.BlockSpec(memory_space=pltpu.VMEM)
    dma = pltpu.SemaphoreType.DMA
    return pl.pallas_call(
        functools.partial(reduce_kernel, seq_size, n_mat, n_sub),
        out_shape=[jax.ShapeDtypeStruct((seq_size,) + da.shape, da.dtype), jax.ShapeDtypeStruct((seq_size,) + loss.shape, F32)]
        + [jax.ShapeDtypeStruct(g.shape, F32) for g in grads],
        in_specs=[vmem] * (2 + n_mat), out_specs=[vmem] * (2 + n_mat),
        scratch_shapes=[pltpu.VMEM((half, g.shape[1]), F32) for g in grads] * 2
        + [pltpu.VMEM((2, 3, piece, g.shape[1]), F32) for g in grads]
        + [dma((n_mat, 4))] * 2 + [dma((n_mat, n_sub, 2, 3))] * 4 + [dma((n_mat, 4))] * 2
        + [dma((2, 3))] * 2 + [dma((7,))] * 2 + [dma((seq_size - 1,))] * 2,
        compiler_params=pltpu.CompilerParams(collective_id=1, has_side_effects=True, vmem_limit_bytes=24 << 20),
        name="reduce_all",
    )(da, loss, *grads)


def finish_kernel(seq_size, vocab, n_loc, me_ref, da_all, loss_ref, gwp_ref, gwo_ref, we_ref, f_ref, t_row, u_row, loss_out, genc_out, gwe_out, gwp_out, gwo_out, gwo_v, d_raw, d_all, sems):
    me = me_ref[0]
    n_af, joint = da_all.shape[1:]
    rows = n_af // seq_size
    n_all = n_af // n_loc
    put_p = pltpu.make_async_copy(gwp_ref, gwp_out, sems.at[0])
    put_p.start()
    gwo_v[...] = gwo_ref[:vocab, :]
    put_o = pltpu.make_async_copy(gwo_v, gwo_out, sems.at[1])
    put_o.start()
    loss_out[...] = jnp.sum(loss_ref[:, 0, :], axis=0, keepdims=True)[:, :n_all]

    def ids(shape, dim):
        return lax.broadcasted_iota(jnp.int32, shape, dim)

    _, key = placement(t_row[...], u_row[...], n_all // seq_size)
    pick = jnp.where(ids((n_all, n_all), 1) == key, 1.0, 0.0).astype(BF16)
    left = jnp.where(ids((n_af, n_all), 0) // n_loc == ids((n_af, n_all), 1), 1.0, 0.0).astype(BF16)
    right = jnp.where(ids((n_all, n_af), 0) == ids((n_all, n_af), 1) // n_loc, 1.0, 0.0).astype(BF16)
    wide = dot_nn(dot_nn(left, pick).astype(BF16), right)
    same = ids((n_af, n_af), 0) % n_loc == ids((n_af, n_af), 1) % n_loc
    move = jnp.where(same, wide, 0.0).astype(BF16)
    for i in range(seq_size):
        for src in range(seq_size):
            d_raw[i, pl.ds(src * rows, rows), :] = da_all[src, pl.ds(i * rows, rows), :]
        d_all[pl.ds(i * n_af, n_af), :] = dot_nn(move, d_raw[i]).astype(BF16)
    here = d_all[pl.ds(pl.multiple_of(me * n_af, n_af), n_af), :]
    genc_out[...] = dot_nt(here, we_ref[...]).astype(BF16).reshape(genc_out.shape)
    gwe_out[...] = dot_tn(f_ref[...].reshape(seq_size * n_af, f_ref.shape[2]), d_all[...])
    put_p.wait()
    put_o.wait()


def finish(seq_idx, da_all, loss_all, gwp, gwo_t, w_enc, enc_all, frame_len, label_len, vocab, n_loc):
    seq_size, n_af, joint = da_all.shape
    n_all = n_af // n_loc
    vmem = pl.BlockSpec(memory_space=pltpu.VMEM)
    return pl.pallas_call(
        functools.partial(finish_kernel, seq_size, vocab, n_loc),
        grid_spec=pltpu.PrefetchScalarGridSpec(
            num_scalar_prefetch=1, grid=(), in_specs=[vmem] * 8, out_specs=[vmem] * 3 + [pl.BlockSpec(memory_space=pltpu.HBM)] * 2,
            scratch_shapes=[pltpu.VMEM((vocab, joint), F32), pltpu.VMEM((seq_size, n_af, joint), BF16), pltpu.VMEM((seq_size * n_af, joint), BF16), pltpu.SemaphoreType.DMA((2,))]),
        out_shape=[
            jax.ShapeDtypeStruct((1, n_all), F32),
            jax.ShapeDtypeStruct((n_all, n_loc, enc_all.shape[2]), BF16),
            jax.ShapeDtypeStruct(w_enc.shape, F32),
            jax.ShapeDtypeStruct(gwp.shape, F32),
            jax.ShapeDtypeStruct((vocab, joint), F32),
        ],
        compiler_params=pltpu.CompilerParams(vmem_limit_bytes=24 << 20),
        name="finish",
    )(seq_idx, da_all, loss_all, gwp, gwo_t, w_enc, enc_all, frame_len[None], label_len[None])


def solution(mesh):
    seq_size = mesh.shape['seq']

    def local_fn(enc_out, pred_out, w_enc, w_pred, w_out, labels, frame_len, label_len):
        seq_idx = jnp.reshape(lax.axis_index('seq'), (1,)).astype(jnp.int32)
        n_all, n_loc, _ = enc_out.shape
        n_utt = n_all // seq_size
        n_frames = n_loc * seq_size
        vocab = w_out.shape[1]
        def keep(x):
            return pltpu.with_memory_space_constraint(x, pltpu.VMEM)

        enc_all, act_f, w_t, w_o, top = map(keep, spread_frames(enc_out, w_enc, w_out.T, seq_size))
        loss, da, *grads = local_grads(
            seq_idx, act_f, w_t, w_o, top, pred_out.reshape(-1, pred_out.shape[2]), w_pred,
            labels, frame_len, label_len, n_utt, n_frames, n_loc, vocab)
        da_all, loss_all, gwp, gwo_t = reduce_all(da, loss, grads, seq_size)
        loss, genc, gwe, gwp, gwo_t = finish(seq_idx, da_all, loss_all, gwp, gwo_t, w_enc, enc_all, frame_len, label_len, vocab, n_loc)
        return loss.reshape(n_all), genc, gwe, gwp, gwo_t.T

    in_specs = (P('dp', 'seq', None), P('dp', None, None), P(None, None), P(None, None), P(None, None), P('dp', None), P('dp'), P('dp'))
    out_specs = (P('dp'), P('dp', 'seq', None), P('dp', None), P('dp', None), P('dp', None))
    return jax.shard_map(local_fn, mesh=mesh, in_specs=in_specs, out_specs=out_specs, check_vma=False)
```
